512 devices in a mesh: slab: 16 (over z, core), blk: 32 (over x, y).
Axes of the slice: x: 4, y: 8, z: 8, core: 2. Of those that a mesh axis runs over, the one named last changes fastest.
Arguments:
- voltage: float32 [64, 256, 512], P('slab', 'blk'), may hold values from -1 to 1.2
- voltage_lag: float32 [64, 256, 512], P('slab', 'blk'), may hold values from -1 to 1.2
- tissue: int32 [64, 256, 512], P('slab', 'blk'), may hold values from 0 to 1, as said below
- fiber: int32 [64, 256, 512], P('slab', 'blk'), may hold values from 0 to 15
- conductivity: float32 [6, 16], replicated, may hold values from -0.036 to 0.12, as said below
- worker: int32 [64, 256], P('slab', 'blk'), may hold values from -1 to 511, as said below
- gates: float32 [12, 8192, 512], P(None, ('slab', 'blk')), may hold values from 0.02 to 0.98
- gate_half: float32 [12], replicated, may hold values from -0.6 to 0.6
- gate_steep: float32 [12], replicated, may hold values from -8 to 8
- gate_tmin: float32 [12], replicated, may hold values from 0.1 to 0.5
- gate_tspan: float32 [12], replicated, may hold values from 0.2 to 3
- channel: float32 [6], replicated, may hold values from 0.5 to 3
Outputs:
- voltage_out: float32 [64, 256, 512], P('slab', 'blk')
- gates_out: float32 [12, 8192, 512], P(None, ('slab', 'blk'))
- charge: float32 [3, 64, 256, 512], P(None, 'slab', 'blk')
The draws below stay inside these ranges and needn't reach their ends.
Inputs may be any that keep to these rules, and one draw needn't show every extreme that they name: `worker`: -1 marks a tile with no tissue. Otherwise the entry is w * 16 + k: the tile's gating variables are row k of the 16 rows of gates held by the device with blk index w in the same slab group. Every such row is named by exactly one tile of its slab group. The tiles of one device name one blk index at most 1 times, and some device does so exactly 1 times. `tissue`: 1 only in tiles whose worker entry is not -1; every such tile holds some tissue. `conductivity`: the first three rows are positive; each class's tensor is positive definite.
All inputs are finite; a program needn't handle non-finite values.
Results may differ from the reference program's by a relative error of at most 0.000088.
Values sent between devices are 32-bit elements; how exact they have to be, the bound alone decides.
No kernel may reach another device: no remote copies, remote signals or barrier semaphores. Data moves between devices by JAX's collectives and lax.ppermute only.
A program may use at most 64 MiB of HBM per device.

```python
import math
import jax
import jax.numpy as jnp
from jax import lax

CX = 4
CY = 8
CZ = 512
NG = 12
FIB = 16
STEPS = 3
RCAP = 16
NX = 64
NY = 256
ROWS = 8192
N_SLAB = 16
N_BLK = 32


def tissue_layout(key):
    keys = jax.random.split(jax.random.fold_in(key, 11), 5)
    tiles = CX * CY
    group = N_BLK * tiles
    weighting = jax.random.randint(keys[0], (N_SLAB, N_BLK), 0, 4)
    favoured = jax.random.randint(keys[1], (N_SLAB,), 0, N_BLK)
    weighting = jnp.where(jnp.arange(N_BLK)[None, :] == favoured[:, None], 9, weighting)
    noise = jax.random.randint(keys[2], (N_SLAB, group), 0, 4096)
    ranks = jnp.arange(group, dtype=jnp.int32)
    scores = jnp.repeat(weighting, tiles, axis=1) * 67108864 + noise * 16384 + ranks[None, :]
    chosen = lax.top_k(scores, RCAP * N_BLK)[1]
    picked = jnp.zeros((N_SLAB, group), jnp.int32).at[jnp.arange(N_SLAB)[:, None], chosen].set(1)
    order = jnp.cumsum(picked, axis=1) - 1
    targets = jnp.where(picked == 1, order % N_BLK * RCAP + order // N_BLK, -1)
    starts = jax.random.randint(keys[3], (N_SLAB, group), 0, CZ // 4)
    spans = jax.random.randint(keys[4], (N_SLAB, group), CZ // 2, CZ - CZ // 4 + 1)
    depth = jnp.arange(CZ, dtype=jnp.int32)
    inside = (depth >= starts[..., None]) & (depth < starts[..., None] + spans[..., None]) & (picked[..., None] == 1)
    targets = targets.reshape(N_SLAB, N_BLK, CX, CY).transpose(0, 2, 1, 3).reshape(N_SLAB * CX, N_BLK * CY)
    inside = inside.reshape(N_SLAB, N_BLK, CX, CY, CZ).transpose(0, 2, 1, 3, 4).reshape(N_SLAB * CX, N_BLK * CY, CZ)
    return (targets.astype(jnp.int32), inside.astype(jnp.int32))


def draw_worker(key, part):
    return tissue_layout(key)[0]


def draw_tissue(key, part):
    return tissue_layout(key)[1]


def draw_conductivity(key, part):
    keys = jax.random.split(jax.random.fold_in(key, 5), 2)
    lowest, highest, reach = (0.03, 0.1, 0.25)
    diagonal = jnp.exp(jax.random.uniform(keys[0], (3, FIB), jnp.float32, math.log(lowest), math.log(highest)))
    mixing = jax.random.uniform(keys[1], (3, FIB), jnp.float32, -reach, reach)
    products = jnp.stack([diagonal[0] * diagonal[1], diagonal[0] * diagonal[2], diagonal[1] * diagonal[2]])
    return jnp.concatenate([diagonal, mixing * jnp.sqrt(products)], axis=0)


def with_ends(drawn, own_key, low, high):
    place = [jax.random.randint(jax.random.fold_in(own_key, axis), (), 0, length) for axis, length in enumerate(drawn.shape)]
    longest = drawn.shape.index(max(drawn.shape))
    next_to = place[:longest] + [(place[longest] + 1) % drawn.shape[longest]] + place[longest + 1:]
    return drawn.at[tuple(place)].set(low).at[tuple(next_to)].set(high)


def block_scale(own_key, dims, cuts, least, high):
    def one(axis_at, shards_of):
        heights = jax.random.uniform(jax.random.fold_in(jax.random.fold_in(own_key, 6), axis_at), (shards_of,), jnp.float32, least / len(cuts), high / len(cuts))
        return jnp.repeat(jnp.exp(heights), dims[axis_at] // shards_of).reshape((-1,) + (1,) * (len(dims) - axis_at - 1))

    level = one(*cuts[0])
    for cut in cuts[1:]:
        level = level * one(*cut)
    return level


def setup_inputs(seed: int = 0) -> dict:
    seeds = jax.random.split(jax.random.key(seed), 13)
    return {
        "voltage": jnp.clip(-1.0 + 2.2 * jax.random.uniform(seeds[0], (NX, NY, CZ), jnp.float32) ** block_scale(seeds[0], (NX, NY, CZ), ((0, 16), (1, 32)), -0.2, 0.2), -1.0, 1.2),
        "voltage_lag": jnp.clip(-1.0 + 2.2 * jax.random.uniform(seeds[1], (NX, NY, CZ), jnp.float32) ** block_scale(seeds[1], (NX, NY, CZ), ((0, 16), (1, 32)), -0.2, 0.2), -1.0, 1.2),
        "tissue": draw_tissue(jax.random.fold_in(seeds[12], 71), 0),
        "fiber": with_ends(jax.random.randint(seeds[3], (NX, NY, CZ), 0, FIB), jax.random.fold_in(seeds[3], 1), 0, FIB - 1).astype(jnp.int32),
        "conductivity": draw_conductivity(jax.random.fold_in(seeds[12], 71), 0),
        "worker": draw_worker(jax.random.fold_in(seeds[12], 71), 0),
        "gates": jnp.clip(0.02 + 0.96000002 * jax.random.uniform(seeds[6], (NG, ROWS, CZ), jnp.float32) ** block_scale(seeds[6], (NG, ROWS, CZ), ((1, 512),), -0.2, 0.2), 0.02, 0.98),
        "gate_half": jnp.clip(jax.random.uniform(seeds[7], (NG,), jnp.float32, -0.6, 0.6), -0.6, 0.6),
        "gate_steep": jnp.clip(jax.random.uniform(seeds[8], (NG,), jnp.float32, -8.0, 8.0), -8.0, 8.0),
        "gate_tmin": jnp.clip(jnp.exp(jax.random.uniform(seeds[9], (NG,), jnp.float32, math.log(0.1), math.log(0.5))), 0.1, 0.5),
        "gate_tspan": jnp.clip(jnp.exp(jax.random.uniform(seeds[10], (NG,), jnp.float32, math.log(0.2), math.log(3.0))), 0.2, 3.0),
        "channel": jnp.clip(jnp.exp(jax.random.uniform(seeds[11], (6,), jnp.float32, math.log(0.5), math.log(3.0))), 0.5, 3.0),
    }


STEP_DT = 0.1
PHASE_REF = -0.2
PHASE_SOFT = 0.5
COMPONENT = ((1, 4, 5), (4, 2, 6), (5, 6, 3))

def basis(direction, amount):
    return tuple((amount if position == direction else 0 for position in range(3)))

def combine(first, second):
    return tuple((left_part + right_part for left_part, right_part in zip(first, second)))

def window(array, starts, extent):
    leading = array.ndim - 3
    begin = (0,) * leading + tuple(starts)
    finish = tuple(array.shape[:leading]) + tuple((first + count for first, count in zip(starts, extent)))
    return lax.slice(array, begin, finish)

def shifted(array, direction, offset, extent):
    starts = tuple(((0 if position == direction else 1) + offset[position] for position in range(3)))
    sizes = tuple((extent[position] + 1 if position == direction else extent[position] for position in range(3)))
    return window(array, starts, sizes)

def coefficient_stack(weights, fiber, conductivity):
    classes = (fiber[None] == jnp.arange(FIB, dtype=jnp.int32)[:, None, None, None]).astype(jnp.float32)
    sigma = jnp.tensordot(conductivity, classes, axes=(1, 0), precision=lax.Precision.HIGHEST)
    return jnp.concatenate([weights[None], weights[None] * sigma], axis=0)

def face_terms(padded_stack, extent):
    result = []
    for direction in range(3):
        lower = shifted(padded_stack, direction, (0, 0, 0), extent)
        upper = shifted(padded_stack, direction, basis(direction, 1), extent)
        face_mask = lower[0] * upper[0]
        result.append([0.5 * (lower[COMPONENT[direction][other]] + upper[COMPONENT[direction][other]]) * face_mask for other in range(3)])
    return result

def diffuse(padded_field, faces, extent):
    total = jnp.zeros(extent, jnp.float32)
    for direction in range(3):
        along = basis(direction, 1)
        flux = faces[direction][direction] * (shifted(padded_field, direction, along, extent) - shifted(padded_field, direction, (0, 0, 0), extent))
        for other in range(3):
            if other != direction:
                upward = basis(other, 1)
                downward = basis(other, -1)
                slope = (shifted(padded_field, direction, upward, extent) + shifted(padded_field, direction, combine(along, upward), extent) - shifted(padded_field, direction, downward, extent) - shifted(padded_field, direction, combine(along, downward), extent)) * 0.25
                flux = flux + faces[direction][other] * slope
        total = total + jnp.diff(flux, axis=direction)
    return total

def react(potential, states, params):
    gate_half, gate_steep, gate_tmin, gate_tspan, channel = params
    level = potential[None]
    centre = gate_half[:, None, None]
    target = jax.nn.sigmoid(gate_steep[:, None, None] * (level - centre))
    relax = gate_tmin[:, None, None] + gate_tspan[:, None, None] / (1.0 + 4.0 * (level - centre) * (level - centre))
    fresh = target + (states - target) * jnp.exp(-STEP_DT / relax)
    sodium = channel[0] * states[0] * states[0] * states[0] * states[1] * states[2] * (potential - 1.2)
    calcium = channel[1] * states[3] * states[4] * states[5] * states[6] * (potential - 1.0)
    transient = channel[2] * states[7] * states[8] * (potential + 0.9)
    rapid_delayed = channel[3] * states[9] * states[10] * (potential + 0.9)
    slow_delayed = channel[4] * states[11] * states[11] * (potential + 0.8)
    inward_rect = channel[5] * (potential + 0.9) / (1.0 + jnp.exp(4.0 * (potential + 0.6)))
    return (fresh, sodium + calcium + transient + rapid_delayed + slow_delayed + inward_rect)

def edge_term(first, second):
    cross = first[0] * second[1] - first[1] * second[0]
    inner = first[0] * second[0] + first[1] * second[1]
    norm_value = jnp.sqrt((first[0] * first[0] + first[1] * first[1]) * (second[0] * second[0] + second[1] * second[1]))
    return 2.0 * jnp.arctan(cross / (norm_value + inner + PHASE_SOFT))

def charges(padded_phase, extent):
    results = []
    for first_dim, second_dim in ((0, 1), (1, 2), (0, 2)):
        corners = [basis(first_dim, 1), basis(second_dim, 1), basis(first_dim, -1), basis(second_dim, -1)]
        points = [window(padded_phase, tuple((1 + value for value in corner)), extent) for corner in corners]
        circulation = jnp.zeros(extent, jnp.float32)
        for position in range(4):
            circulation = circulation + edge_term(points[position], points[(position + 1) % 4])
        results.append(circulation)
    return jnp.stack(results)

def pad_space(array):
    return jnp.pad(array, [(0, 0)] * (array.ndim - 3) + [(1, 1)] * 3)

def reference(voltage, voltage_lag, tissue, fiber, conductivity, worker, gates, gate_half, gate_steep, gate_tmin, gate_tspan, channel):
    extent = voltage.shape
    params = (gate_half, gate_steep, gate_tmin, gate_tspan, channel)
    weights = tissue.astype(jnp.float32)
    faces = face_terms(pad_space(coefficient_stack(weights, fiber, conductivity)), extent)
    total_rows = N_SLAB * N_BLK * RCAP
    targets = worker.reshape(-1)
    live = targets >= 0
    slab_base = jnp.broadcast_to((jnp.arange(NX, dtype=jnp.int32) // CX * (N_BLK * RCAP))[:, None], (NX, NY)).reshape(-1)
    owned_rows = jnp.where(live, slab_base + targets, total_rows)
    tile_ids = jnp.arange(NX * NY, dtype=jnp.int32)
    tile_of_row = jnp.zeros((total_rows + 1,), jnp.int32).at[owned_rows].set(tile_ids)[:total_rows]
    safe_rows = jnp.minimum(owned_rows, total_rows - 1)
    states = gates
    potential = voltage
    for timestep in range(STEPS):
        tile_volts = potential.reshape(NX * NY, CZ)
        states, row_current = react(tile_volts[tile_of_row], states, params)
        current = jnp.where(live[:, None], row_current[safe_rows], 0.0).reshape(extent)
        spread = diffuse(pad_space(weights * potential), faces, extent)
        potential = potential + weights * (spread - STEP_DT * current)
    phase = jnp.stack([weights * (potential - PHASE_REF), weights * (voltage_lag - PHASE_REF)])
    return (potential, states, charges(pad_space(phase), extent))
```

```python
import jax
import jax.numpy as jnp
from jax import lax
from jax.sharding import PartitionSpec as P

FIB = 16
STEPS = 3


STEP_DT = 0.1
PHASE_REF = -0.2
PHASE_SOFT = 0.5
COMPONENT = ((1, 4, 5), (4, 2, 6), (5, 6, 3))


def basis(direction, amount):
    return tuple((amount if position == direction else 0 for position in range(3)))


def combine(first, second):
    return tuple((left_part + right_part for left_part, right_part in zip(first, second)))


def window(array, starts, extent):
    leading = array.ndim - 3
    begin = (0,) * leading + tuple(starts)
    finish = tuple(array.shape[:leading]) + tuple(
        (first + count for first, count in zip(starts, extent))
    )
    return lax.slice(array, begin, finish)


def shifted(array, direction, offset, extent):
    starts = tuple(
        ((0 if position == direction else 1) + offset[position] for position in range(3))
    )
    sizes = tuple(
        (
            extent[position] + 1 if position == direction else extent[position]
            for position in range(3)
        )
    )
    return window(array, starts, sizes)


def coefficient_stack(weights, fiber, conductivity):
    classes = (fiber[None] == jnp.arange(FIB, dtype=jnp.int32)[:, None, None, None]).astype(
        jnp.float32
    )
    sigma = jnp.tensordot(conductivity, classes, axes=(1, 0), precision=lax.Precision.HIGHEST)
    return jnp.concatenate([weights[None], weights[None] * sigma], axis=0)


def face_terms(padded_stack, extent):
    result = []
    for direction in range(3):
        lower = shifted(padded_stack, direction, (0, 0, 0), extent)
        upper = shifted(padded_stack, direction, basis(direction, 1), extent)
        face_mask = lower[0] * upper[0]
        result.append(
            [
                0.5
                * (lower[COMPONENT[direction][other]] + upper[COMPONENT[direction][other]])
                * face_mask
                for other in range(3)
            ]
        )
    return result


def diffuse(padded_field, faces, extent):
    total = jnp.zeros(extent, jnp.float32)
    for direction in range(3):
        along = basis(direction, 1)
        flux = faces[direction][direction] * (
            shifted(padded_field, direction, along, extent)
            - shifted(padded_field, direction, (0, 0, 0), extent)
        )
        for other in range(3):
            if other != direction:
                upward = basis(other, 1)
                downward = basis(other, -1)
                slope = (
                    shifted(padded_field, direction, upward, extent)
                    + shifted(padded_field, direction, combine(along, upward), extent)
                    - shifted(padded_field, direction, downward, extent)
                    - shifted(padded_field, direction, combine(along, downward), extent)
                ) * 0.25
                flux = flux + faces[direction][other] * slope
        total = total + jnp.diff(flux, axis=direction)
    return total


def edge_term(first, second):
    cross = first[0] * second[1] - first[1] * second[0]
    inner = first[0] * second[0] + first[1] * second[1]
    norm_value = jnp.sqrt(
        (first[0] * first[0] + first[1] * first[1])
        * (second[0] * second[0] + second[1] * second[1])
    )
    return 2.0 * jnp.arctan(cross / (norm_value + inner + PHASE_SOFT))


def charges(padded_phase, extent):
    results = []
    for first_dim, second_dim in ((0, 1), (1, 2), (0, 2)):
        corners = [
            basis(first_dim, 1),
            basis(second_dim, 1),
            basis(first_dim, -1),
            basis(second_dim, -1),
        ]
        points = [
            window(padded_phase, tuple((1 + value for value in corner)), extent)
            for corner in corners
        ]
        circulation = jnp.zeros(extent, jnp.float32)
        for position in range(4):
            circulation = circulation + edge_term(points[position], points[(position + 1) % 4])
        results.append(circulation)
    return jnp.stack(results)


def pad_depth(array):
    return jnp.pad(array, [(0, 0)] * (array.ndim - 1) + [(1, 1)])


def shift_pair(axis, last, first):
    size = lax.axis_size(axis)
    up = [(i, i + 1) for i in range(size - 1)]
    return (lax.ppermute(last, axis, up), lax.ppermute(first, axis, [(b, a) for a, b in up]))


def gate_update(level, states, params):
    gate_half, gate_steep, gate_tmin, gate_tspan, _ = params
    offset = level[None] - gate_half[:, None, None]
    target = jax.nn.sigmoid(gate_steep[:, None, None] * offset)
    relax = gate_tmin[:, None, None] + gate_tspan[:, None, None] / (1.0 + 4.0 * offset * offset)
    return target + (states - target) * jnp.exp(-STEP_DT / relax)


def ionic_current(level, states, channel):
    sodium = channel[0] * states[0] * states[0] * states[0] * states[1] * states[2] * (level - 1.2)
    calcium = channel[1] * states[3] * states[4] * states[5] * states[6] * (level - 1.0)
    transient = channel[2] * states[7] * states[8] * (level + 0.9)
    rapid_delayed = channel[3] * states[9] * states[10] * (level + 0.9)
    slow_delayed = channel[4] * states[11] * states[11] * (level + 0.8)
    inward_rect = channel[5] * (level + 0.9) / (1.0 + jnp.exp(4.0 * (level + 0.6)))
    return sodium + calcium + transient + rapid_delayed + slow_delayed + inward_rect


def swap_blocks(x):
    return lax.all_to_all(x, "blk", split_axis=0, concat_axis=0, tiled=True)


def inner_faces(faces):
    return [
        [lax.slice_in_dim(lax.slice_in_dim(f, 1, f.shape[0] - 1, axis=0), 1, f.shape[1] - 1, axis=1) for f in row]
        for row in faces
    ]


def on_device(
    voltage,
    voltage_lag,
    tissue,
    fiber,
    conductivity,
    worker,
    gates,
    gate_half,
    gate_steep,
    gate_tmin,
    gate_tspan,
    channel,
):
    extent = voltage.shape
    planes, rows, depth = extent
    gate_count, capacity, _ = gates.shape
    params = (gate_half, gate_steep, gate_tmin, gate_tspan, channel)
    blocks = lax.axis_size("blk")
    lanes = 128
    chunks = depth // lanes
    weights = tissue.astype(jnp.float32)

    targets = worker.reshape(-1)
    tile_count = targets.shape[0]
    live = targets >= 0
    holder = jnp.where(live, targets // capacity, -1)
    claimed = holder[None, :] == jnp.arange(blocks, dtype=jnp.int32)[:, None]
    claims = jnp.sum(jnp.where(claimed, targets % capacity + 1, 0), axis=1) - 1
    tile_of = jnp.sum(jnp.where(claimed, jnp.arange(tile_count, dtype=jnp.int32)[None, :], 0), axis=1)
    arrived = swap_blocks(jnp.broadcast_to(claims[:, None, None], (blocks, 1, lanes)))[:, 0, 0]

    by_row = gates.transpose(1, 0, 2).reshape(capacity, gate_count * chunks, lanes)
    leaving = by_row[jnp.maximum(arrived, 0)]
    coming = swap_blocks(leaving)
    states = (
        coming[jnp.maximum(holder, 0)].reshape(tile_count, gate_count, depth).transpose(1, 0, 2)
    )

    field = weights * voltage
    lag = weights * (voltage_lag - PHASE_REF)
    fiber_f = fiber.astype(jnp.float32)
    low, high = shift_pair(
        "slab",
        jnp.concatenate([field[-1:], lag[-1:], fiber_f[-2:], weights[-2:]]),
        jnp.concatenate([field[:1], lag[:1], fiber_f[:2], weights[:2]]),
    )
    field_s = jnp.concatenate([low[0:1], field, high[0:1]])
    lag_s = jnp.concatenate([low[1:2], lag, high[1:2]])
    fiber_s = jnp.concatenate([low[2:4], fiber_f, high[2:4]])
    weights_s = jnp.concatenate([low[4:6], weights, high[4:6]])
    low, high = shift_pair(
        "blk",
        jnp.concatenate([field_s[:, -1], lag_s[1:-1, -1], fiber_s[:, -2], fiber_s[:, -1], weights_s[:, -2], weights_s[:, -1]]),
        jnp.concatenate([field_s[:, 0], lag_s[1:-1, 0], fiber_s[:, 0], fiber_s[:, 1], weights_s[:, 0], weights_s[:, 1]]),
    )
    n1, n2 = planes + 2, planes + 4

    def column(part, start, count):
        return part[start : start + count, None]

    def two(part, start):
        return jnp.concatenate([column(part, start, n2), column(part, start + n2, n2)], axis=1)

    field_e = jnp.concatenate([column(low, 0, n1), field_s, column(high, 0, n1)], axis=1)
    lag_rim = (column(low, n1, planes), column(high, n1, planes))
    at = n1 + planes
    fiber_e = jnp.concatenate([two(low, at), fiber_s, two(high, at)], axis=1)
    at = at + 2 * n2
    weights_e = jnp.concatenate([two(low, at), weights_s, two(high, at)], axis=1)
    stack_e = coefficient_stack(weights_e, fiber_e.astype(jnp.int32), conductivity)
    ring = (planes + 2, rows + 2, depth)
    faces_ring = face_terms(pad_depth(stack_e), ring)
    faces = inner_faces(faces_ring)
    weights_ring = weights_e[1:-1, 1:-1]

    def current_of(potential, states):
        found = ionic_current(potential.reshape(tile_count, depth), states, channel)
        return jnp.where(live[:, None], found, 0.0).reshape(extent)

    spread = diffuse(pad_depth(field_e), faces, extent)
    v0 = voltage
    v1 = v0 + weights * (spread - STEP_DT * current_of(v0, states))
    states = gate_update(v0.reshape(tile_count, depth), states, params)
    current = current_of(v1, states)
    low, high = shift_pair(
        "slab",
        jnp.concatenate([v1[-2:], current[-1:]]),
        jnp.concatenate([v1[:2], current[:1]]),
    )
    v1_s = jnp.concatenate([low[:2], v1, high[:2]])
    current_s = jnp.concatenate([low[2:], current, high[2:]])
    low, high = shift_pair(
        "blk",
        jnp.concatenate([v1_s[:, -2], v1_s[:, -1], current_s[:, -1]]),
        jnp.concatenate([v1_s[:, 0], v1_s[:, 1], current_s[:, 0]]),
    )
    v1_e = jnp.concatenate([two(low, 0), v1_s, two(high, 0)], axis=1)
    current_e = jnp.concatenate([column(low, 2 * n2, n1), current_s, column(high, 2 * n2, n1)], axis=1)
    states = gate_update(v1.reshape(tile_count, depth), states, params)
    spread = diffuse(pad_depth(weights_e * v1_e), faces_ring, ring)
    v2_e = v1_e[1:-1, 1:-1] + weights_ring * (spread - STEP_DT * current_e)
    v2 = v2_e[1:-1, 1:-1]

    used = jnp.stack([v.reshape(tile_count, chunks, lanes) for v in (v0, v1, v2)], axis=1)
    used = used.reshape(tile_count, 3 * chunks, lanes)[tile_of]
    returned = swap_blocks(used)

    spread = diffuse(pad_depth(weights_ring * v2_e), faces, extent)
    v3 = v2 + weights * (spread - STEP_DT * current_of(v2, states))

    ours = weights * (v3 - PHASE_REF)
    below, above = shift_pair("slab", ours[-1:], ours[:1])
    left, right = shift_pair("blk", ours[:, -1:], ours[:, :1])

    def plus(array, low0, high0, low1, high1):
        tall = jnp.concatenate([low0, array, high0], axis=0)
        around = [(1, 1), (0, 0), (0, 0)]
        return jnp.concatenate([jnp.pad(low1, around), tall, jnp.pad(high1, around)], axis=1)

    phase = jnp.stack(
        [
            plus(ours, below, above, left, right),
            plus(lag, lag_s[:1], lag_s[-1:], *lag_rim),
        ]
    )
    charge = charges(pad_depth(phase), extent)

    mine = arrived[None, :] == jnp.arange(capacity, dtype=jnp.int32)[:, None]
    source = jnp.sum(jnp.where(mine, jnp.arange(blocks, dtype=jnp.int32)[None, :], 0), axis=1)
    seen = returned[source].reshape(capacity, 3, depth)
    gates_out = gates
    for step in range(STEPS):
        gates_out = gate_update(seen[:, step], gates_out, params)
    return (v3, gates_out, charge)

def solution(mesh):
    in_specs = (
        P("slab", "blk", None),
        P("slab", "blk", None),
        P("slab", "blk", None),
        P("slab", "blk", None),
        P(),
        P("slab", "blk"),
        P(None, ("slab", "blk"), None),
        P(),
        P(),
        P(),
        P(),
        P(),
    )
    out_specs = (
        P("slab", "blk", None),
        P(None, ("slab", "blk"), None),
        P(None, "slab", "blk", None),
    )
    return jax.shard_map(
        on_device, mesh=mesh, in_specs=in_specs, out_specs=out_specs, check_vma=False
    )
```

```python
import functools

import jax
import jax.numpy as jnp
from jax import lax
from jax.experimental import pallas as pl
from jax.experimental.pallas import tpu as pltpu
from jax.sharding import PartitionSpec as P

FIB = 16
STEPS = 3
GATES = 12
CX, CY, CZ = 4, 8, 512
TILES = CX * CY
LANES = 128
CHUNKS = CZ // LANES
CAP = 16
NI, NJ = CX + 4, 16


STEP_DT = 0.1
PHASE_REF = -0.2
PHASE_SOFT = 0.5
COMPONENT = ((0, 3, 4), (3, 1, 5), (4, 5, 2))
HALF, STEEP, TMIN, TSPAN, CHANNEL = 0, 12, 24, 36, 48

f32 = jnp.float32
VM = pl.BlockSpec(memory_space=pltpu.VMEM)
SM = pl.BlockSpec(memory_space=pltpu.SMEM)


def kernel_call(body, outs, ins, scratch=(), flops=1_000_000):
    return pl.pallas_call(
        body,
        out_shape=[jax.ShapeDtypeStruct(shape, f32) for shape in outs],
        in_specs=ins,
        out_specs=[VM] * len(outs),
        scratch_shapes=[pltpu.VMEM(shape, f32) for shape in scratch],
        cost_estimate=pl.CostEstimate(flops=flops, bytes_accessed=1_000_000, transcendentals=0),
        compiler_params=pltpu.CompilerParams(vmem_limit_bytes=40 * 1024 * 1024),
    )


def chunk(c):
    return pl.ds(c * LANES, LANES)


def to_dense(dense_ref, plane, i):
    for c in range(CHUNKS):
        dense_ref[pl.ds(i * CY * CHUNKS + c, CY, stride=CHUNKS), :] = plane[:, c * LANES : (c + 1) * LANES]


def from_dense(dense_ref, i, c):
    return dense_ref[pl.ds(i * CY * CHUNKS + c, CY, stride=CHUNKS), :]


def updated(level, state, par_ref, g):
    offset = level - par_ref[HALF + g]
    target = 1.0 / (1.0 + jnp.exp(-par_ref[STEEP + g] * offset))
    bell = 1.0 + 4.0 * (offset * offset)
    decay = jnp.exp((-STEP_DT * bell) / (par_ref[TMIN + g] * bell + par_ref[TSPAN + g]))
    return target + (state - target) * decay


def factors(s, par_ref):
    return (
        par_ref[CHANNEL] * s[0] * s[0] * s[0] * s[1] * s[2],
        par_ref[CHANNEL + 1] * s[3] * s[4] * s[5] * s[6],
        par_ref[CHANNEL + 2] * s[7] * s[8] + par_ref[CHANNEL + 3] * s[9] * s[10],
        par_ref[CHANNEL + 4] * s[11] * s[11],
    )


def current_from(level, parts, par_ref):
    inward = par_ref[CHANNEL + 5] * (level + 0.9) / (1.0 + jnp.exp(4.0 * (level + 0.6)))
    return (
        parts[0] * (level - 1.2)
        + parts[1] * (level - 1.0)
        + parts[2] * (level + 0.9)
        + parts[3] * (level + 0.8)
        + inward
    )


def start_body(voltage, lag, tissue, fiber, up_ref, down_ref):
    for ref, outer, pair in ((up_ref, CX - 1, (CX - 2, CX - 1)), (down_ref, 0, (0, 1))):
        w = tissue[outer].astype(f32)
        ref[0] = w * voltage[outer]
        ref[1] = w * (lag[outer] - PHASE_REF)
        for n, i in enumerate(pair):
            ref[2 + n] = fiber[i].astype(f32)
            ref[4 + n] = tissue[i].astype(f32)


def columns_body(voltage, lag, tissue, fiber, low, high, up_ref, down_ref):
    for ref, outer, pair in ((up_ref, CY - 1, (CY - 2, CY - 1)), (down_ref, 0, (0, 1))):
        one = slice(outer, outer + 1)
        ref[0:1] = low[0, one]
        ref[CX + 1 : CX + 2] = high[0, one]
        for i in range(CX):
            w = tissue[i, one].astype(f32)
            ref[1 + i : 2 + i] = w * voltage[i, one]
            ref[CX + 2 + i : CX + 3 + i] = w * (lag[i, one] - PHASE_REF)
        at = 2 * CX + 2
        for n, j in enumerate(pair):
            one = slice(j, j + 1)
            for m in range(2):
                for kind, base in ((2, at + n * NI), (4, at + (2 + n) * NI)):
                    ref[base + m : base + m + 1] = low[kind + m, one]
                    ref[base + CX + 2 + m : base + CX + 3 + m] = high[kind + m, one]
            for i in range(CX):
                ref[at + n * NI + 2 + i : at + n * NI + 3 + i] = fiber[i, one].astype(f32)
                ref[at + (2 + n) * NI + 2 + i : at + (2 + n) * NI + 3 + i] = tissue[i, one].astype(f32)


def by_row_body(gates, out_ref):
    for g in range(GATES):
        for c in range(CHUNKS):
            for k in range(0, CAP, 8):
                out_ref[pl.ds(k * GATES * CHUNKS + g * CHUNKS + c, 8, stride=GATES * CHUNKS), :] = gates[g, k : k + 8, chunk(c)]


def pack_body(slots, arrived, by_row, out_ref):
    for d in range(slots):
        k = jnp.maximum(arrived[d], 0)
        out_ref[d] = by_row[pl.ds(pl.multiple_of(k * GATES * CHUNKS, 8), GATES * CHUNKS), :]


def up_j(x):
    return pltpu.roll(x, NJ - 1, 0)


def down_j(x):
    return pltpu.roll(x, 1, 0)


def up_z(x):
    return pltpu.roll(x, CZ - 1, 1)


def down_z(x):
    return pltpu.roll(x, 1, 1)


def spread_of(f, face, first, last):
    z = lax.broadcasted_iota(jnp.int32, (NJ, CZ), 1)
    dy, dz = {}, {}
    for i in range(first - 1, last + 2):
        dy[i] = up_j(f[i]) - down_j(f[i])
        dz[i] = jnp.where(z == CZ - 1, 0.0, up_z(f[i])) - jnp.where(z == 0, 0.0, down_z(f[i]))
    along = {}
    for i in range(first - 1, last + 1):
        along[i] = (
            face(0, i) * (f[i + 1] - f[i])
            + face(1, i) * (0.25 * (dy[i] + dy[i + 1]))
            + face(2, i) * (0.25 * (dz[i] + dz[i + 1]))
        )
    total = {}
    for i in range(first, last + 1):
        dx = f[i + 1] - f[i - 1]
        flux_y = (
            face(4, i) * (up_j(f[i]) - f[i])
            + face(3, i) * (0.25 * (dx + up_j(dx)))
            + face(5, i) * (0.25 * (dz[i] + up_j(dz[i])))
        )
        flux_z = (
            face(8, i) * (up_z(f[i]) - f[i])
            + face(6, i) * (0.25 * (dx + up_z(dx)))
            + face(7, i) * (0.25 * (dy[i] + up_z(dy[i])))
        )
        total[i] = along[i] - along[i - 1] + flux_y - down_j(flux_y) + flux_z - down_z(flux_z)
    return total


def faces_body(voltage, tissue, fiber, low, high, left, right, cond, faces_ref, weights_ref, base_ref, field_ref, fib_ref, stack_ref):
    zero = jnp.zeros((NI, NJ, CZ), f32)
    field_ref[...] = zero
    fib_ref[...] = zero
    weights_ref[...] = zero
    own = slice(2, 2 + CY)
    for i in range(CX):
        w = tissue[i].astype(f32)
        field_ref[2 + i, own, :] = w * voltage[i]
        weights_ref[2 + i, own, :] = w
        fib_ref[2 + i, own, :] = fiber[i].astype(f32)
    for ref, base, at in ((low, 0, 1), (high, CX + 2, CX + 2)):
        field_ref[at, own, :] = ref[0]
        for m in range(2):
            fib_ref[base + m, own, :] = ref[2 + m]
            weights_ref[base + m, own, :] = ref[4 + m]
    at = 2 * CX + 2
    for ref, outer, cols in ((left, 1, (0, 1)), (right, 2 + CY, (2 + CY, 3 + CY))):
        for i in range(CX + 2):
            field_ref[1 + i, outer : outer + 1, :] = ref[i : i + 1, :]
        for n, j in enumerate(cols):
            for i in range(NI):
                fib_ref[i, j : j + 1, :] = ref[at + n * NI + i : at + n * NI + i + 1, :]
                weights_ref[i, j : j + 1, :] = ref[at + (2 + n) * NI + i : at + (2 + n) * NI + i + 1, :]

    def classes(i, carry):
        for c in range(CHUNKS):
            fib = fib_ref[i, :, chunk(c)]
            w = weights_ref[i, :, chunk(c)]
            found = [jnp.full((NJ, LANES), cond[n * FIB]) for n in range(6)]
            for k in range(1, FIB):
                here = fib == float(k)
                found = [jnp.where(here, cond[n * FIB + k], old) for n, old in enumerate(found)]
            for n in range(6):
                stack_ref[n, i, :, chunk(c)] = 0.5 * (w * found[n])
        return carry

    lax.fori_loop(0, NI, classes, 0)
    z = lax.broadcasted_iota(jnp.int32, (NJ, CZ), 1)
    for i in range(NI - 1):
        w = weights_ref[i]
        both = w * weights_ref[i + 1]
        for n, comp in enumerate(COMPONENT[0]):
            faces_ref[n, i] = (stack_ref[comp, i] + stack_ref[comp, i + 1]) * both
        if i == 0:
            continue
        both = w * up_j(w)
        for n, comp in enumerate(COMPONENT[1]):
            here = stack_ref[comp, i]
            faces_ref[3 + n, i] = (here + up_j(here)) * both
        both = w * jnp.where(z == CZ - 1, 0.0, up_z(w))
        for n, comp in enumerate(COMPONENT[2]):
            here = stack_ref[comp, i]
            faces_ref[6 + n, i] = (here + up_z(here)) * both
    field = {i: field_ref[i] for i in range(1, NI - 1)}
    spread = spread_of(field, lambda n, i: faces_ref[n, i], 2, CX + 1)
    for i in range(CX):
        base_ref[i] = voltage[i] + tissue[i].astype(f32) * spread[2 + i][2 : 2 + CY]


def react_body(holder, par, coming, voltage, base, tissue, live, v1_ref, current_ref, states_ref, v_d, base_d, w_d, live_d, out_d, cur_d):
    for i in range(CX):
        mask = jnp.concatenate([live[i]] * CHUNKS, axis=1)
        to_dense(v_d, voltage[i], i)
        to_dense(base_d, base[i], i)
        to_dense(w_d, tissue[i].astype(f32) * mask, i)
        to_dense(live_d, mask, i)

    def pair(p, carry):
        rows = pl.ds(pl.multiple_of(p * 8, 8), 8)
        first, second = holder[2 * p], holder[2 * p + 1]
        level = v_d[rows, :]
        states = [
            jnp.concatenate([coming[first, pl.ds(g * CHUNKS, CHUNKS), :], coming[second, pl.ds(g * CHUNKS, CHUNKS), :]], axis=0)
            for g in range(GATES)
        ]
        after = base_d[rows, :] - w_d[rows, :] * (STEP_DT * current_from(level, factors(states, par), par))
        states = [updated(level, s, par, g) for g, s in enumerate(states)]
        for g in range(GATES):
            states_ref[g, rows, :] = states[g]
        out_d[rows, :] = after
        cur_d[rows, :] = live_d[rows, :] * current_from(after, factors(states, par), par)
        return carry

    lax.fori_loop(0, TILES // 2, pair, 0)
    for i in range(CX):
        for c in range(CHUNKS):
            v1_ref[i, :, chunk(c)] = from_dense(out_d, i, c)
            current_ref[i, :, chunk(c)] = from_dense(cur_d, i, c)


def second_body(par, states_in, v1, parts_ref, v_d, parts_d):
    for i in range(CX):
        to_dense(v_d, v1[i], i)

    def pair(p, carry):
        rows = pl.ds(pl.multiple_of(p * 8, 8), 8)
        level = v_d[rows, :]
        states = [updated(level, states_in[g, rows, :], par, g) for g in range(GATES)]
        for n, part in enumerate(factors(states, par)):
            parts_d[n, rows, :] = part
        return carry

    lax.fori_loop(0, TILES // 2, pair, 0)
    for n in range(4):
        for i in range(CX):
            for c in range(CHUNKS):
                parts_ref[n, i, :, chunk(c)] = from_dense(parts_d.at[n], i, c)


def columns2_body(v1, current, low, high, up_ref, down_ref):
    for ref, pair in ((up_ref, (CY - 2, CY - 1)), (down_ref, (0, 1))):
        outer = CY - 1 if ref is up_ref else 0
        for n, j in enumerate(pair):
            one = slice(j, j + 1)
            for m in range(2):
                ref[n * NI + m : n * NI + m + 1] = low[m, one]
                ref[n * NI + CX + 2 + m : n * NI + CX + 3 + m] = high[m, one]
            for i in range(CX):
                ref[n * NI + 2 + i : n * NI + 3 + i] = v1[i, one]
        one = slice(outer, outer + 1)
        at = 2 * NI
        ref[at : at + 1] = low[2, one]
        ref[at + CX + 1 : at + CX + 2] = high[2, one]
        for i in range(CX):
            ref[at + 1 + i : at + 2 + i] = current[i, one]


def steps_body(slots, tile_of, par, v0, v1, current, low, high, left, right, weights, faces, parts, live, v3_ref, ours_ref, used_ref, v_ref, cur_ref, next_ref, rows_ref):
    v_ref[...] = jnp.zeros((NI, NJ, CZ), f32)
    cur_ref[...] = jnp.zeros((NI, NJ, CZ), f32)
    own = slice(2, 2 + CY)
    for i in range(CX):
        v_ref[2 + i, own, :] = v1[i]
        cur_ref[2 + i, own, :] = current[i]
    for m in range(2):
        v_ref[m, own, :] = low[m]
        v_ref[CX + 2 + m, own, :] = high[m]
    cur_ref[1, own, :] = low[2]
    cur_ref[CX + 2, own, :] = high[2]
    for ref, cols, outer in ((left, (0, 1), 1), (right, (2 + CY, 3 + CY), 2 + CY)):
        for n, j in enumerate(cols):
            for i in range(NI):
                v_ref[i, j : j + 1, :] = ref[n * NI + i : n * NI + i + 1, :]
        for i in range(CX + 2):
            cur_ref[1 + i, outer : outer + 1, :] = ref[2 * NI + i : 2 * NI + i + 1, :]
    face = lambda n, i: faces[n, i]
    field = {i: weights[i] * v_ref[i] for i in range(NI)}
    spread = spread_of(field, face, 1, NI - 2)
    for i in range(1, NI - 1):
        next_ref[i] = v_ref[i] + weights[i] * (spread[i] - STEP_DT * cur_ref[i])
    field = {i: weights[i] * next_ref[i] for i in range(1, NI - 1)}
    spread = spread_of(field, face, 2, CX + 1)
    for i in range(CX):
        v2 = next_ref[2 + i, own, :]
        w = weights[2 + i, own, :]
        mask = jnp.concatenate([live[i]] * CHUNKS, axis=1)
        found = mask * current_from(v2, [parts[n, i] for n in range(4)], par)
        v3 = v2 + w * (spread[2 + i][own] - STEP_DT * found)
        v3_ref[i] = v3
        ours_ref[i] = w * (v3 - PHASE_REF)
        for n, v in enumerate((v0[i], v1[i], v2)):
            for c in range(CHUNKS):
                rows_ref[pl.ds(i * CY * 16 + n * CHUNKS + c, CY, stride=16), :] = v[:, c * LANES : (c + 1) * LANES]
        for c in range(CHUNKS):
            rows_ref[pl.ds(i * CY * 16 + 3 * CHUNKS + c, CY, stride=16), :] = jnp.zeros((CY, LANES), f32)
    for d in range(slots):
        used_ref[d] = rows_ref[pl.ds(pl.multiple_of(tile_of[d] * 16, 16), 16), :]


def last_body(slots, arrived, par, returned, gates, out_ref, rows_ref):
    for d in range(slots):
        k = arrived[d]
        row = jnp.where(k >= 0, k, CAP)
        rows_ref[pl.ds(pl.multiple_of(row * 16, 16), 16), :] = returned[d]

    def one(g, carry):
        for k in range(0, CAP, 8):
            for c in range(CHUNKS):
                state = gates[g, k : k + 8, chunk(c)]
                for n in range(STEPS):
                    state = updated(rows_ref[pl.ds(k * 16 + n * CHUNKS + c, 8, stride=16), :], state, par, g)
                out_ref[g, k : k + 8, chunk(c)] = state
        return carry

    lax.fori_loop(0, GATES, one, 0)


def shift_pair(axis, last, first):
    size = lax.axis_size(axis)
    up = [(i, i + 1) for i in range(size - 1)]
    return (lax.ppermute(last, axis, up), lax.ppermute(first, axis, [(b, a) for a, b in up]))


def swap_blocks(x):
    return lax.all_to_all(x, "blk", split_axis=0, concat_axis=0, tiled=True)


def basis(direction, amount):
    return tuple((amount if position == direction else 0 for position in range(3)))


def window(array, starts, extent):
    leading = array.ndim - 3
    begin = (0,) * leading + tuple(starts)
    finish = tuple(array.shape[:leading]) + tuple(
        (first + count for first, count in zip(starts, extent))
    )
    return lax.slice(array, begin, finish)


def edge_term(first, second):
    cross = first[0] * second[1] - first[1] * second[0]
    inner = first[0] * second[0] + first[1] * second[1]
    norm_value = jnp.sqrt(
        (first[0] * first[0] + first[1] * first[1])
        * (second[0] * second[0] + second[1] * second[1])
    )
    return 2.0 * jnp.arctan(cross / (norm_value + inner + PHASE_SOFT))


def charges(padded_phase, extent):
    results = []
    for first_dim, second_dim in ((0, 1), (1, 2), (0, 2)):
        corners = [
            basis(first_dim, 1),
            basis(second_dim, 1),
            basis(first_dim, -1),
            basis(second_dim, -1),
        ]
        points = [
            window(padded_phase, tuple((1 + value for value in corner)), extent)
            for corner in corners
        ]
        circulation = jnp.zeros(extent, jnp.float32)
        for position in range(4):
            circulation = circulation + edge_term(points[position], points[(position + 1) % 4])
        results.append(circulation)
    return jnp.stack(results)


def pad_depth(array):
    return jnp.pad(array, [(0, 0)] * (array.ndim - 1) + [(1, 1)])


def on_device(
    voltage,
    voltage_lag,
    tissue,
    fiber,
    conductivity,
    worker,
    gates,
    gate_half,
    gate_steep,
    gate_tmin,
    gate_tspan,
    channel,
):
    block = voltage.shape
    slots = lax.axis_size("blk")
    par = jnp.concatenate([gate_half, gate_steep, gate_tmin, gate_tspan, channel])
    cond = conductivity.reshape(-1)

    targets = worker.reshape(-1)
    live = targets >= 0
    holder = jnp.where(live, targets // CAP, -1)
    claimed = holder[None, :] == jnp.arange(slots, dtype=jnp.int32)[:, None]
    claims = jnp.sum(jnp.where(claimed, targets % CAP + 1, 0), axis=1) - 1
    tile_of = jnp.sum(jnp.where(claimed, jnp.arange(TILES, dtype=jnp.int32)[None, :], 0), axis=1)
    arrived = swap_blocks(jnp.broadcast_to(claims[:, None, None], (slots, 1, LANES)))[:, 0, 0]
    mask = jnp.broadcast_to((worker >= 0).astype(f32)[:, :, None], (CX, CY, LANES))

    rim = (6, CY, CZ)
    up, down = kernel_call(start_body, [rim, rim], [VM] * 4)(voltage, voltage_lag, tissue, fiber)
    low, high = shift_pair("slab", up, down)
    (by_row,) = kernel_call(by_row_body, [(CAP * GATES * CHUNKS, LANES)], [VM])(gates)

    run = (slots, GATES * CHUNKS, LANES)
    (leaving,) = kernel_call(functools.partial(pack_body, slots), [run], [SM, VM])(arrived, by_row)
    coming = swap_blocks(leaving)

    side = (2 * CX + 2 + 4 * NI, CZ)
    up, down = kernel_call(columns_body, [side, side], [VM] * 6)(voltage, voltage_lag, tissue, fiber, low, high)
    left, right = shift_pair("blk", up, down)
    wide = (NI, NJ, CZ)
    faces, weights_e, base = kernel_call(
        faces_body, [(9, *wide), wide, block], [VM] * 7 + [SM], [wide, wide, (6, *wide)]
    )(voltage, tissue, fiber, low, high, left, right, cond)
    lag_low, lag_high = low[1:2], high[1:2]
    lag_left, lag_right = (x[CX + 2 : 2 * CX + 2, None] for x in (left, right))

    dense = (TILES * CHUNKS, LANES)
    v1, current, states = kernel_call(
        react_body, [block, block, (GATES, *dense)], [SM, SM] + [VM] * 5, [dense] * 6
    )(jnp.maximum(holder, 0), par, coming, voltage, base, tissue, mask)

    low, high = shift_pair(
        "slab", jnp.concatenate([v1[-2:], current[-1:]]), jnp.concatenate([v1[:2], current[:1]])
    )
    (parts,) = kernel_call(second_body, [(4, *block)], [SM, VM, VM], [dense, (4, *dense)])(par, states, v1)
    side = (2 * NI + CX + 2, CZ)
    up, down = kernel_call(columns2_body, [side, side], [VM] * 4)(v1, current, low, high)
    left, right = shift_pair("blk", up, down)

    v3, ours, used = kernel_call(
        functools.partial(steps_body, slots),
        [block, block, (slots, 16, LANES)],
        [SM, SM] + [VM] * 11,
        [wide, wide, wide, (TILES * 16, LANES)],
    )(tile_of, par, voltage, v1, current, low, high, left, right, weights_e, faces, parts, mask)
    returned = swap_blocks(used)

    below, above = shift_pair("slab", ours[-1:], ours[:1])
    left, right = shift_pair("blk", ours[:, -1:], ours[:, :1])

    def plus(array, low0, high0, low1, high1):
        tall = jnp.concatenate([low0, array, high0], axis=0)
        around = [(1, 1), (0, 0), (0, 0)]
        return jnp.concatenate([jnp.pad(low1, around), tall, jnp.pad(high1, around)], axis=1)

    lag = tissue.astype(f32) * (voltage_lag - PHASE_REF)
    phase = jnp.stack(
        [plus(ours, below, above, left, right), plus(lag, lag_low, lag_high, lag_left, lag_right)]
    )
    charge = charges(pad_depth(phase), block)

    (gates_out,) = kernel_call(
        functools.partial(last_body, slots), [gates.shape], [SM, SM, VM, VM], [((CAP + 1) * 16, LANES)]
    )(arrived, par, returned, gates)
    return (v3, gates_out, charge)


def solution(mesh):
    in_specs = (
        P("slab", "blk", None),
        P("slab", "blk", None),
        P("slab", "blk", None),
        P("slab", "blk", None),
        P(),
        P("slab", "blk"),
        P(None, ("slab", "blk"), None),
        P(),
        P(),
        P(),
        P(),
        P(),
    )
    out_specs = (
        P("slab", "blk", None),
        P(None, ("slab", "blk"), None),
        P(None, "slab", "blk", None),
    )
    return jax.shard_map(on_device, mesh=mesh, in_specs=in_specs, out_specs=out_specs, check_vma=False)
```

```python
import functools

import jax
import jax.numpy as jnp
from jax import lax
from jax.experimental import pallas as pl
from jax.experimental.pallas import tpu as pltpu
from jax.sharding import PartitionSpec as P

FIB = 16
STEPS = 3
GATES = 12
CX, CY, CZ = 4, 8, 512
TILES = CX * CY
LANES = 128
CHUNKS = CZ // LANES
CAP = 16
NI, NJ = CX + 4, 16


STEP_DT = 0.1
PHASE_REF = -0.2
PHASE_SOFT = 0.5
COMPONENT = ((0, 3, 4), (3, 1, 5), (4, 5, 2))
HALF, STEEP, TMIN, TSPAN, CHANNEL = 0, 12, 24, 36, 48

f32 = jnp.float32
VM = pl.BlockSpec(memory_space=pltpu.VMEM)
SM = pl.BlockSpec(memory_space=pltpu.SMEM)
HB = pl.BlockSpec(memory_space=pltpu.HBM)


def kernel_call(body, outs, ins, scratch=(), flops=1_000_000, limit=6, specs=None):
    return pl.pallas_call(
        body,
        out_shape=[jax.ShapeDtypeStruct(shape, f32) for shape in outs],
        in_specs=ins,
        out_specs=specs or [VM] * len(outs),
        scratch_shapes=[pltpu.VMEM(s, f32) if isinstance(s, tuple) else s for s in scratch],
        cost_estimate=pl.CostEstimate(flops=flops, bytes_accessed=1_000_000, transcendentals=0),
        compiler_params=pltpu.CompilerParams(vmem_limit_bytes=limit * 1024 * 1024),
    )


def chunk(c):
    return pl.ds(c * LANES, LANES)


def to_dense(dense_ref, plane, i):
    for c in range(CHUNKS):
        dense_ref[pl.ds(i * CY * CHUNKS + c, CY, stride=CHUNKS), :] = plane[:, c * LANES : (c + 1) * LANES]


def from_dense(dense_ref, i, c):
    return dense_ref[pl.ds(i * CY * CHUNKS + c, CY, stride=CHUNKS), :]


def updated(level, state, par_ref, g):
    offset = level - par_ref[HALF + g]
    target = 1.0 / (1.0 + jnp.exp(-par_ref[STEEP + g] * offset))
    bell = 1.0 + 4.0 * (offset * offset)
    decay = jnp.exp((-STEP_DT * bell) / (par_ref[TMIN + g] * bell + par_ref[TSPAN + g]))
    return target + (state - target) * decay


def factors(s, par_ref):
    return (
        par_ref[CHANNEL] * s[0] * s[0] * s[0] * s[1] * s[2],
        par_ref[CHANNEL + 1] * s[3] * s[4] * s[5] * s[6],
        par_ref[CHANNEL + 2] * s[7] * s[8] + par_ref[CHANNEL + 3] * s[9] * s[10],
        par_ref[CHANNEL + 4] * s[11] * s[11],
    )


def current_from(level, parts, par_ref):
    inward = par_ref[CHANNEL + 5] * (level + 0.9) / (1.0 + jnp.exp(4.0 * (level + 0.6)))
    return (
        parts[0] * (level - 1.2)
        + parts[1] * (level - 1.0)
        + parts[2] * (level + 0.9)
        + parts[3] * (level + 0.8)
        + inward
    )


def start_body(voltage, lag, tissue, fiber, up_ref, down_ref):
    for ref, outer, pair in ((up_ref, CX - 1, (CX - 2, CX - 1)), (down_ref, 0, (0, 1))):
        w = tissue[outer].astype(f32)
        ref[0] = w * voltage[outer]
        ref[1] = w * (lag[outer] - PHASE_REF)
        for n, i in enumerate(pair):
            ref[2 + n] = fiber[i].astype(f32)
            ref[4 + n] = tissue[i].astype(f32)


def columns_body(voltage, lag, tissue, fiber, low, high, up_ref, down_ref):
    for ref, outer, pair in ((up_ref, CY - 1, (CY - 2, CY - 1)), (down_ref, 0, (0, 1))):
        one = slice(outer, outer + 1)
        ref[0:1] = low[0, one]
        ref[CX + 1 : CX + 2] = high[0, one]
        for i in range(CX):
            w = tissue[i, one].astype(f32)
            ref[1 + i : 2 + i] = w * voltage[i, one]
            ref[CX + 2 + i : CX + 3 + i] = w * (lag[i, one] - PHASE_REF)
        at = 2 * CX + 2
        for n, j in enumerate(pair):
            one = slice(j, j + 1)
            for m in range(2):
                for kind, base in ((2, at + n * NI), (4, at + (2 + n) * NI)):
                    ref[base + m : base + m + 1] = low[kind + m, one]
                    ref[base + CX + 2 + m : base + CX + 3 + m] = high[kind + m, one]
            for i in range(CX):
                ref[at + n * NI + 2 + i : at + n * NI + 3 + i] = fiber[i, one].astype(f32)
                ref[at + (2 + n) * NI + 2 + i : at + (2 + n) * NI + 3 + i] = tissue[i, one].astype(f32)


def by_row_body(gates, out_ref):
    for g in range(GATES):
        for c in range(CHUNKS):
            for k in range(0, CAP, 8):
                out_ref[pl.ds(k * GATES * CHUNKS + g * CHUNKS + c, 8, stride=GATES * CHUNKS), :] = gates[g, k : k + 8, chunk(c)]


def pack_body(slots, arrived, by_row, out_ref):
    for d in range(slots):
        k = jnp.maximum(arrived[d], 0)
        out_ref[d] = by_row[pl.ds(pl.multiple_of(k * GATES * CHUNKS, 8), GATES * CHUNKS), :]


def up_j(x):
    return pltpu.roll(x, NJ - 1, 0)


def down_j(x):
    return pltpu.roll(x, 1, 0)


def up_z(x):
    return pltpu.roll(x, CZ - 1, 1)


def down_z(x):
    return pltpu.roll(x, 1, 1)


def spread_of(f, face, first, last):
    z = lax.broadcasted_iota(jnp.int32, (NJ, CZ), 1)
    dy, dz = {}, {}
    for i in range(first - 1, last + 2):
        dy[i] = up_j(f[i]) - down_j(f[i])
        dz[i] = jnp.where(z == CZ - 1, 0.0, up_z(f[i])) - jnp.where(z == 0, 0.0, down_z(f[i]))
    along = {}
    for i in range(first - 1, last + 1):
        along[i] = (
            face(0, i) * (f[i + 1] - f[i])
            + face(1, i) * (0.25 * (dy[i] + dy[i + 1]))
            + face(2, i) * (0.25 * (dz[i] + dz[i + 1]))
        )
    total = {}
    for i in range(first, last + 1):
        dx = f[i + 1] - f[i - 1]
        flux_y = (
            face(4, i) * (up_j(f[i]) - f[i])
            + face(3, i) * (0.25 * (dx + up_j(dx)))
            + face(5, i) * (0.25 * (dz[i] + up_j(dz[i])))
        )
        flux_z = (
            face(8, i) * (up_z(f[i]) - f[i])
            + face(6, i) * (0.25 * (dx + up_z(dx)))
            + face(7, i) * (0.25 * (dy[i] + up_z(dy[i])))
        )
        total[i] = along[i] - along[i - 1] + flux_y - down_j(flux_y) + flux_z - down_z(flux_z)
    return total


def faces_body(voltage, tissue, fiber, low, high, left, right, cond, faces_out, weights_ref, base_ref, lag_ref, faces_ref, field_ref, fib_ref, stack_ref, sems):
    zero = jnp.zeros((NI, NJ, CZ), f32)
    field_ref[...] = zero
    fib_ref[...] = zero
    weights_ref[...] = zero
    own = slice(2, 2 + CY)
    for i in range(CX):
        w = tissue[i].astype(f32)
        field_ref[2 + i, own, :] = w * voltage[i]
        weights_ref[2 + i, own, :] = w
        fib_ref[2 + i, own, :] = fiber[i].astype(f32)
    for ref, base, at in ((low, 0, 1), (high, CX + 2, CX + 2)):
        field_ref[at, own, :] = ref[0]
        for m in range(2):
            fib_ref[base + m, own, :] = ref[2 + m]
            weights_ref[base + m, own, :] = ref[4 + m]
    at = 2 * CX + 2
    for ref, outer, cols in ((left, 1, (0, 1)), (right, 2 + CY, (2 + CY, 3 + CY))):
        for i in range(CX + 2):
            field_ref[1 + i, outer : outer + 1, :] = ref[i : i + 1, :]
        for n, j in enumerate(cols):
            for i in range(NI):
                fib_ref[i, j : j + 1, :] = ref[at + n * NI + i : at + n * NI + i + 1, :]
                weights_ref[i, j : j + 1, :] = ref[at + (2 + n) * NI + i : at + (2 + n) * NI + i + 1, :]

    def classes(i, carry):
        for c in range(CHUNKS):
            fib = fib_ref[i, :, chunk(c)]
            w = weights_ref[i, :, chunk(c)]
            found = [jnp.full((NJ, LANES), cond[n * FIB]) for n in range(6)]
            for k in range(1, FIB):
                here = fib == float(k)
                found = [jnp.where(here, cond[n * FIB + k], old) for n, old in enumerate(found)]
            for n in range(6):
                stack_ref[n, i, :, chunk(c)] = 0.5 * (w * found[n])
        return carry

    lax.fori_loop(0, NI, classes, 0)
    lag_ref[0:CY] = low[1]
    lag_ref[CY : 2 * CY] = high[1]
    lag_ref[2 * CY : 2 * CY + CX] = left[CX + 2 : 2 * CX + 2]
    lag_ref[2 * CY + CX : 2 * CY + 2 * CX] = right[CX + 2 : 2 * CX + 2]
    z = lax.broadcasted_iota(jnp.int32, (NJ, CZ), 1)
    copies = []
    for i in range(NI - 1):
        if i > 1:
            copies.append(pltpu.make_async_copy(faces_ref.at[i - 1], faces_out.at[i - 1], sems.at[i - 1]))
            copies[-1].start()
        w = weights_ref[i]
        both = w * weights_ref[i + 1]
        for n, comp in enumerate(COMPONENT[0]):
            faces_ref[i, n] = (stack_ref[comp, i] + stack_ref[comp, i + 1]) * both
        if i == 0:
            faces_ref[0, 3:] = jnp.zeros((6, NJ, CZ), f32)
            continue
        both = w * up_j(w)
        for n, comp in enumerate(COMPONENT[1]):
            here = stack_ref[comp, i]
            faces_ref[i, 3 + n] = (here + up_j(here)) * both
        both = w * jnp.where(z == CZ - 1, 0.0, up_z(w))
        for n, comp in enumerate(COMPONENT[2]):
            here = stack_ref[comp, i]
            faces_ref[i, 6 + n] = (here + up_z(here)) * both
    for i in (0, NI - 2):
        copies.append(pltpu.make_async_copy(faces_ref.at[i], faces_out.at[i], sems.at[i]))
        copies[-1].start()
    field = {i: field_ref[i] for i in range(1, NI - 1)}
    spread = spread_of(field, lambda n, i: faces_ref[i, n], 2, CX + 1)
    for i in range(CX):
        base_ref[i] = voltage[i] + tissue[i].astype(f32) * spread[2 + i][2 : 2 + CY]
    for copy in copies:
        copy.wait()


def react_body(holder, par, coming, voltage, base, tissue, live, v1_ref, current_ref, states_ref, v_d, base_d, w_d, live_d, out_d, cur_d):
    for i in range(CX):
        mask = jnp.concatenate([live[i]] * CHUNKS, axis=1)
        to_dense(v_d, voltage[i], i)
        to_dense(base_d, base[i], i)
        to_dense(w_d, tissue[i].astype(f32) * mask, i)
        to_dense(live_d, mask, i)

    def pair(p, carry):
        rows = pl.ds(pl.multiple_of(p * 8, 8), 8)
        first, second = holder[2 * p], holder[2 * p + 1]
        level = v_d[rows, :]
        states = [
            jnp.concatenate([coming[first, pl.ds(g * CHUNKS, CHUNKS), :], coming[second, pl.ds(g * CHUNKS, CHUNKS), :]], axis=0)
            for g in range(GATES)
        ]
        after = base_d[rows, :] - w_d[rows, :] * (STEP_DT * current_from(level, factors(states, par), par))
        states = [updated(level, s, par, g) for g, s in enumerate(states)]
        for g in range(GATES):
            states_ref[g, rows, :] = states[g]
        out_d[rows, :] = after
        cur_d[rows, :] = live_d[rows, :] * current_from(after, factors(states, par), par)
        return carry

    lax.fori_loop(0, TILES // 2, pair, 0)
    for i in range(CX):
        for c in range(CHUNKS):
            v1_ref[i, :, chunk(c)] = from_dense(out_d, i, c)
            current_ref[i, :, chunk(c)] = from_dense(cur_d, i, c)


def second_body(par, states_in, v1, parts_ref, v_d, parts_d):
    for i in range(CX):
        to_dense(v_d, v1[i], i)

    def pair(p, carry):
        rows = pl.ds(pl.multiple_of(p * 8, 8), 8)
        level = v_d[rows, :]
        states = [updated(level, states_in[g, rows, :], par, g) for g in range(GATES)]
        for n, part in enumerate(factors(states, par)):
            parts_d[n, rows, :] = part
        return carry

    lax.fori_loop(0, TILES // 2, pair, 0)
    for n in range(4):
        for i in range(CX):
            for c in range(CHUNKS):
                parts_ref[n, i, :, chunk(c)] = from_dense(parts_d.at[n], i, c)


def columns2_body(v1, current, low, high, up_ref, down_ref):
    for ref, pair in ((up_ref, (CY - 2, CY - 1)), (down_ref, (0, 1))):
        outer = CY - 1 if ref is up_ref else 0
        for n, j in enumerate(pair):
            one = slice(j, j + 1)
            for m in range(2):
                ref[n * NI + m : n * NI + m + 1] = low[m, one]
                ref[n * NI + CX + 2 + m : n * NI + CX + 3 + m] = high[m, one]
            for i in range(CX):
                ref[n * NI + 2 + i : n * NI + 3 + i] = v1[i, one]
        one = slice(outer, outer + 1)
        at = 2 * NI
        ref[at : at + 1] = low[2, one]
        ref[at + CX + 1 : at + CX + 2] = high[2, one]
        for i in range(CX):
            ref[at + 1 + i : at + 2 + i] = current[i, one]


def steps_body(slots, tile_of, par, v0, v1, current, low, high, left, right, weights, faces_in, parts, live, v3_ref, ours_ref, used_ref, faces, v_ref, cur_ref, next_ref, rows_ref, sem):
    fetch = pltpu.make_async_copy(faces_in, faces, sem)
    fetch.start()
    v_ref[...] = jnp.zeros((NI, NJ, CZ), f32)
    cur_ref[...] = jnp.zeros((NI, NJ, CZ), f32)
    own = slice(2, 2 + CY)
    for i in range(CX):
        v_ref[2 + i, own, :] = v1[i]
        cur_ref[2 + i, own, :] = current[i]
    for m in range(2):
        v_ref[m, own, :] = low[m]
        v_ref[CX + 2 + m, own, :] = high[m]
    cur_ref[1, own, :] = low[2]
    cur_ref[CX + 2, own, :] = high[2]
    for ref, cols, outer in ((left, (0, 1), 1), (right, (2 + CY, 3 + CY), 2 + CY)):
        for n, j in enumerate(cols):
            for i in range(NI):
                v_ref[i, j : j + 1, :] = ref[n * NI + i : n * NI + i + 1, :]
        for i in range(CX + 2):
            cur_ref[1 + i, outer : outer + 1, :] = ref[2 * NI + i : 2 * NI + i + 1, :]
    face = lambda n, i: faces[i, n]
    field = {i: weights[i] * v_ref[i] for i in range(NI)}
    fetch.wait()
    spread = spread_of(field, face, 1, NI - 2)
    for i in range(1, NI - 1):
        next_ref[i] = v_ref[i] + weights[i] * (spread[i] - STEP_DT * cur_ref[i])
    field = {i: weights[i] * next_ref[i] for i in range(1, NI - 1)}
    spread = spread_of(field, face, 2, CX + 1)
    for i in range(CX):
        v2 = next_ref[2 + i, own, :]
        w = weights[2 + i, own, :]
        mask = jnp.concatenate([live[i]] * CHUNKS, axis=1)
        found = mask * current_from(v2, [parts[n, i] for n in range(4)], par)
        v3 = v2 + w * (spread[2 + i][own] - STEP_DT * found)
        v3_ref[i] = v3
        ours_ref[i] = w * (v3 - PHASE_REF)
        for n, v in enumerate((v0[i], v1[i], v2)):
            for c in range(CHUNKS):
                rows_ref[pl.ds(i * CY * 16 + n * CHUNKS + c, CY, stride=16), :] = v[:, c * LANES : (c + 1) * LANES]
        for c in range(CHUNKS):
            rows_ref[pl.ds(i * CY * 16 + 3 * CHUNKS + c, CY, stride=16), :] = jnp.zeros((CY, LANES), f32)
    for d in range(slots):
        used_ref[d] = rows_ref[pl.ds(pl.multiple_of(tile_of[d] * 16, 16), 16), :]


def last_body(slots, arrived, par, returned, gates, out_ref, rows_ref):
    for d in range(slots):
        k = arrived[d]
        row = jnp.where(k >= 0, k, CAP)
        rows_ref[pl.ds(pl.multiple_of(row * 16, 16), 16), :] = returned[d]

    def one(g, carry):
        for k in range(0, CAP, 8):
            for c in range(CHUNKS):
                state = gates[g, k : k + 8, chunk(c)]
                for n in range(STEPS):
                    state = updated(rows_ref[pl.ds(k * 16 + n * CHUNKS + c, 8, stride=16), :], state, par, g)
                out_ref[g, k : k + 8, chunk(c)] = state
        return carry

    lax.fori_loop(0, GATES, one, 0)


def arctan_of(cross, den):
    size = jnp.abs(cross)
    big = size > 2.414213562373095 * den
    mid = size > 0.4142135623730950 * den
    num = jnp.where(big, -den, jnp.where(mid, size - den, size))
    x = num / jnp.where(big, size, jnp.where(mid, size + den, den))
    z = x * x
    tail = ((8.05374449538e-2 * z - 1.38776856032e-1) * z + 1.99777106478e-1) * z - 3.33329491539e-1
    found = jnp.where(big, 1.5707963267948966, jnp.where(mid, 0.7853981633974483, 0.0)) + (tail * z * x + x)
    return jnp.where(cross < 0.0, -found, found)


def edge_of(p, q):
    cross = p[0] * q[1] - p[1] * q[0]
    inner = p[0] * q[0] + p[1] * q[1]
    return arctan_of(cross, p[2] * q[2] + inner + PHASE_SOFT)


def charge_body(ours, below, above, left, right, lag, tissue, lag_rim, out_ref):
    row = lax.broadcasted_iota(jnp.int32, (CY, CZ), 0)
    z = lax.broadcasted_iota(jnp.int32, (CY, CZ), 1)

    def point(a, b):
        return (a, b, jnp.sqrt(a * a + b * b))

    a = {-1: below[0], CX: above[0]} | {i: ours[i] for i in range(CX)}
    b = {-1: lag_rim[0:CY], CX: lag_rim[CY : 2 * CY]} | {i: tissue[i].astype(f32) * (lag[i] - PHASE_REF) for i in range(CX)}
    plane = {i: point(a[i], b[i]) for i in range(-1, CX + 1)}
    for i in range(CX):
        at, beyond = 2 * CY + i, 2 * CY + CX + i

        def later(x, edge):
            return jnp.where(row == CY - 1, jnp.broadcast_to(edge, (CY, CZ)), pltpu.roll(x, CY - 1, 0))

        def earlier(x, edge):
            return jnp.where(row == 0, jnp.broadcast_to(edge, (CY, CZ)), pltpu.roll(x, 1, 0))

        y_up = point(later(a[i], right[i]), later(b[i], lag_rim[beyond : beyond + 1]))
        y_down = point(earlier(a[i], left[i]), earlier(b[i], lag_rim[at : at + 1]))
        z_up = tuple(jnp.where(z == CZ - 1, 0.0, up_z(x)) for x in plane[i])
        z_down = tuple(jnp.where(z == 0, 0.0, down_z(x)) for x in plane[i])
        x_up, x_down = plane[i + 1], plane[i - 1]
        for n, ring in enumerate(((x_up, y_up, x_down, y_down), (y_up, z_up, y_down, z_down), (x_up, z_up, x_down, z_down))):
            total = edge_of(ring[0], ring[1]) + edge_of(ring[1], ring[2]) + edge_of(ring[2], ring[3]) + edge_of(ring[3], ring[0])
            out_ref[n, i] = 2.0 * total


def shift_pair(axis, last, first):
    size = lax.axis_size(axis)
    up = [(i, i + 1) for i in range(size - 1)]
    return (lax.ppermute(last, axis, up), lax.ppermute(first, axis, [(b, a) for a, b in up]))


def swap_blocks(x):
    return lax.all_to_all(x, "blk", split_axis=0, concat_axis=0, tiled=True)


def on_device(
    voltage,
    voltage_lag,
    tissue,
    fiber,
    conductivity,
    worker,
    gates,
    gate_half,
    gate_steep,
    gate_tmin,
    gate_tspan,
    channel,
):
    block = voltage.shape
    slots = lax.axis_size("blk")
    par = jnp.concatenate([gate_half, gate_steep, gate_tmin, gate_tspan, channel])
    cond = conductivity.reshape(-1)

    live = worker >= 0
    holder = jnp.where(live, worker // CAP, -1)
    claimed = holder[None] == jnp.arange(slots, dtype=jnp.int32)[:, None, None]
    tiles = CY * jnp.arange(CX, dtype=jnp.int32)[:, None] + jnp.arange(CY, dtype=jnp.int32)[None, :]
    claims = jnp.sum(jnp.where(claimed, worker % CAP + 1, 0), axis=(1, 2)) - 1
    tile_of = jnp.sum(jnp.where(claimed, tiles[None], 0), axis=(1, 2))
    arrived = swap_blocks(jnp.broadcast_to(claims[:, None, None], (slots, 1, LANES)))[:, 0, 0]
    mask = jnp.broadcast_to(live.astype(f32)[:, :, None], (CX, CY, LANES))

    rim = (6, CY, CZ)
    up, down = kernel_call(start_body, [rim, rim], [VM] * 4)(voltage, voltage_lag, tissue, fiber)
    low, high = shift_pair("slab", up, down)
    (by_row,) = kernel_call(by_row_body, [(CAP * GATES * CHUNKS, LANES)], [VM])(gates)

    run = (slots, GATES * CHUNKS, LANES)
    (leaving,) = kernel_call(functools.partial(pack_body, slots), [run], [SM, VM])(arrived, by_row)
    coming = swap_blocks(leaving)

    side = (2 * CX + 2 + 4 * NI, CZ)
    up, down = kernel_call(columns_body, [side, side], [VM] * 6)(voltage, voltage_lag, tissue, fiber, low, high)
    left, right = shift_pair("blk", up, down)
    wide = (NI, NJ, CZ)
    sheets = (NI - 1, 9, NJ, CZ)
    faces, weights_e, base, lag_rim = kernel_call(
        faces_body,
        [sheets, wide, block, (2 * CY + 2 * CX, CZ)],
        [VM] * 7 + [SM],
        [sheets, wide, wide, (6, *wide), pltpu.SemaphoreType.DMA((NI - 1,))],
        specs=[HB, VM, VM, VM],
        limit=12,
    )(voltage, tissue, fiber, low, high, left, right, cond)

    dense = (TILES * CHUNKS, LANES)
    v1, current, states = kernel_call(
        react_body, [block, block, (GATES, *dense)], [SM, SM] + [VM] * 5, [dense] * 6
    )(jnp.maximum(holder, 0).reshape(-1), par, coming, voltage, base, tissue, mask)

    low, high = shift_pair(
        "slab", jnp.concatenate([v1[-2:], current[-1:]]), jnp.concatenate([v1[:2], current[:1]])
    )
    (parts,) = kernel_call(second_body, [(4, *block)], [SM, VM, VM], [dense, (4, *dense)])(par, states, v1)
    side = (2 * NI + CX + 2, CZ)
    up, down = kernel_call(columns2_body, [side, side], [VM] * 4)(v1, current, low, high)
    left, right = shift_pair("blk", up, down)

    v3, ours, used = kernel_call(
        functools.partial(steps_body, slots),
        [block, block, (slots, 16, LANES)],
        [SM, SM] + [VM] * 8 + [HB, VM, VM],
        [sheets, wide, wide, wide, (TILES * 16, LANES), pltpu.SemaphoreType.DMA],
        limit=12,
    )(tile_of, par, voltage, v1, current, low, high, left, right, weights_e, faces, parts, mask)
    returned = swap_blocks(used)

    below, above = shift_pair("slab", ours[-1:], ours[:1])
    left, right = shift_pair("blk", ours[:, -1:], ours[:, :1])

    (charge,) = kernel_call(charge_body, [(3, *block)], [VM] * 8)(
        ours, below, above, left, right, voltage_lag, tissue, lag_rim
    )

    (gates_out,) = kernel_call(
        functools.partial(last_body, slots), [gates.shape], [SM, SM, VM, VM], [((CAP + 1) * 16, LANES)]
    )(arrived, par, returned, gates)
    return (v3, gates_out, charge)


def solution(mesh):
    in_specs = (
        P("slab", "blk", None),
        P("slab", "blk", None),
        P("slab", "blk", None),
        P("slab", "blk", None),
        P(),
        P("slab", "blk"),
        P(None, ("slab", "blk"), None),
        P(),
        P(),
        P(),
        P(),
        P(),
    )
    out_specs = (
        P("slab", "blk", None),
        P(None, ("slab", "blk"), None),
        P(None, "slab", "blk", None),
    )
    return jax.shard_map(on_device, mesh=mesh, in_specs=in_specs, out_specs=out_specs, check_vma=False)
```

```python
import functools

import jax
import jax.numpy as jnp
from jax import lax
from jax.experimental import pallas as pl
from jax.experimental.pallas import tpu as pltpu
from jax.sharding import PartitionSpec as P

FIB = 16
STEPS = 3
GATES = 12
CX, CY, CZ = 4, 8, 512
TILES = CX * CY
LANES = 128
CHUNKS = CZ // LANES
CAP = 16
NI, NJ = CX + 4, 16


STEP_DT = 0.1
PHASE_REF = -0.2
PHASE_SOFT = 0.5
COMPONENT = ((0, 3, 4), (3, 1, 5), (4, 5, 2))
HALF, STEEP, TMIN, TSPAN, CHANNEL, COND, PARAMS = 0, 12, 24, 36, 48, 54, 256

f32 = jnp.float32
VM = pl.BlockSpec(memory_space=pltpu.VMEM)
SM = pl.BlockSpec(memory_space=pltpu.SMEM)
HB = pl.BlockSpec(memory_space=pltpu.HBM)


def kernel_call(body, outs, ins, scratch=(), flops=1_000_000, limit=6, specs=None):
    return pl.pallas_call(
        body,
        out_shape=[jax.ShapeDtypeStruct(shape, f32) for shape in outs],
        in_specs=ins,
        out_specs=specs or [VM] * len(outs),
        scratch_shapes=[pltpu.VMEM(s, f32) if isinstance(s, tuple) else s for s in scratch],
        cost_estimate=pl.CostEstimate(flops=flops, bytes_accessed=1_000_000, transcendentals=0),
        compiler_params=pltpu.CompilerParams(vmem_limit_bytes=limit * 1024 * 1024),
    )


def fetched(pairs, sems):
    copies = [pltpu.make_async_copy(a, b, sems.at[n]) for n, (a, b) in enumerate(pairs)]
    for copy in copies:
        copy.start()
    return copies


def live_plane(worker, i):
    row = lax.broadcasted_iota(jnp.int32, (CY, CZ), 0)
    mask = jnp.zeros((CY, CZ), f32)
    for j in range(CY):
        mask = jnp.where(row == j, jnp.where(worker[i, j] >= 0, 1.0, 0.0), mask)
    return mask


def chunk(c):
    return pl.ds(c * LANES, LANES)


def to_dense(dense_ref, plane, i):
    for c in range(CHUNKS):
        dense_ref[pl.ds(i * CY * CHUNKS + c, CY, stride=CHUNKS), :] = plane[:, c * LANES : (c + 1) * LANES]


def from_dense(dense_ref, i, c):
    return dense_ref[pl.ds(i * CY * CHUNKS + c, CY, stride=CHUNKS), :]


def updated(level, state, par_ref, g):
    offset = level - par_ref[HALF + g]
    target = 1.0 / (1.0 + jnp.exp(-par_ref[STEEP + g] * offset))
    bell = 1.0 + 4.0 * (offset * offset)
    decay = jnp.exp((-STEP_DT * bell) / (par_ref[TMIN + g] * bell + par_ref[TSPAN + g]))
    return target + (state - target) * decay


def factors(s, par_ref):
    return (
        par_ref[CHANNEL] * s[0] * s[0] * s[0] * s[1] * s[2],
        par_ref[CHANNEL + 1] * s[3] * s[4] * s[5] * s[6],
        par_ref[CHANNEL + 2] * s[7] * s[8] + par_ref[CHANNEL + 3] * s[9] * s[10],
        par_ref[CHANNEL + 4] * s[11] * s[11],
    )


def current_from(level, parts, par_ref):
    inward = par_ref[CHANNEL + 5] * (level + 0.9) / (1.0 + jnp.exp(4.0 * (level + 0.6)))
    return (
        parts[0] * (level - 1.2)
        + parts[1] * (level - 1.0)
        + parts[2] * (level + 0.9)
        + parts[3] * (level + 0.8)
        + inward
    )


def start_body(voltage_in, lag_in, tissue_in, fiber_in, up_ref, down_ref, right_ref, left_ref, voltage, lag, tissue, fiber, sems):
    for copy in fetched(((voltage_in, voltage), (lag_in, lag), (tissue_in, tissue), (fiber_in, fiber)), sems):
        copy.wait()
    for ref, outer, pair in ((up_ref, CX - 1, (CX - 2, CX - 1)), (down_ref, 0, (0, 1))):
        w = tissue[outer].astype(f32)
        ref[0] = w * voltage[outer]
        ref[1] = w * (lag[outer] - PHASE_REF)
        for n, i in enumerate(pair):
            ref[2 + n] = fiber[i].astype(f32)
            ref[4 + n] = tissue[i].astype(f32)
    for ref, outer, pair in ((right_ref, CY - 1, (CY - 2, CY - 1)), (left_ref, 0, (0, 1))):
        ref[...] = jnp.zeros(ref.shape, f32)
        one = slice(outer, outer + 1)
        for i in range(CX):
            w = tissue[i, one].astype(f32)
            ref[1 + i : 2 + i] = w * voltage[i, one]
            ref[CX + 2 + i : CX + 3 + i] = w * (lag[i, one] - PHASE_REF)
        at = 2 * CX + 2
        for n, j in enumerate(pair):
            one = slice(j, j + 1)
            for i in range(CX):
                ref[at + n * NI + 2 + i : at + n * NI + 3 + i] = fiber[i, one].astype(f32)
                ref[at + (2 + n) * NI + 2 + i : at + (2 + n) * NI + 3 + i] = tissue[i, one].astype(f32)


def columns_body(right_in, left_in, low, high, up_ref, down_ref):
    for ref, own, outer, pair in ((up_ref, right_in, CY - 1, (CY - 2, CY - 1)), (down_ref, left_in, 0, (0, 1))):
        ref[...] = own[...]
        one = slice(outer, outer + 1)
        ref[0:1] = low[0, one]
        ref[CX + 1 : CX + 2] = high[0, one]
        at = 2 * CX + 2
        for n, j in enumerate(pair):
            one = slice(j, j + 1)
            for m in range(2):
                for kind, base in ((2, at + n * NI), (4, at + (2 + n) * NI)):
                    ref[base + m : base + m + 1] = low[kind + m, one]
                    ref[base + CX + 2 + m : base + CX + 3 + m] = high[kind + m, one]


def by_row_body(gates, out_ref):
    for g in range(GATES):
        for c in range(CHUNKS):
            for k in range(0, CAP, 8):
                out_ref[pl.ds(k * GATES * CHUNKS + g * CHUNKS + c, 8, stride=GATES * CHUNKS), :] = gates[g, k : k + 8, chunk(c)]


def pack_body(slots, arrived, by_row, out_ref):
    for d in range(slots):
        k = jnp.maximum(arrived[d], 0)
        out_ref[d] = by_row[pl.ds(pl.multiple_of(k * GATES * CHUNKS, 8), GATES * CHUNKS), :]


def up_j(x):
    return pltpu.roll(x, NJ - 1, 0)


def down_j(x):
    return pltpu.roll(x, 1, 0)


def up_z(x):
    return pltpu.roll(x, CZ - 1, 1)


def down_z(x):
    return pltpu.roll(x, 1, 1)


def spread_of(f, face, first, last):
    z = lax.broadcasted_iota(jnp.int32, (NJ, CZ), 1)
    dy, dz = {}, {}
    for i in range(first - 1, last + 2):
        dy[i] = up_j(f[i]) - down_j(f[i])
        dz[i] = jnp.where(z == CZ - 1, 0.0, up_z(f[i])) - jnp.where(z == 0, 0.0, down_z(f[i]))
    along = {}
    for i in range(first - 1, last + 1):
        along[i] = (
            face(0, i) * (f[i + 1] - f[i])
            + face(1, i) * (0.25 * (dy[i] + dy[i + 1]))
            + face(2, i) * (0.25 * (dz[i] + dz[i + 1]))
        )
    total = {}
    for i in range(first, last + 1):
        dx = f[i + 1] - f[i - 1]
        flux_y = (
            face(4, i) * (up_j(f[i]) - f[i])
            + face(3, i) * (0.25 * (dx + up_j(dx)))
            + face(5, i) * (0.25 * (dz[i] + up_j(dz[i])))
        )
        flux_z = (
            face(8, i) * (up_z(f[i]) - f[i])
            + face(6, i) * (0.25 * (dx + up_z(dx)))
            + face(7, i) * (0.25 * (dy[i] + up_z(dy[i])))
        )
        total[i] = along[i] - along[i - 1] + flux_y - down_j(flux_y) + flux_z - down_z(flux_z)
    return total


def faces_body(
    voltage_in, tissue_in, fiber_in, par_in, low, high, left, right,
    faces_out, weights_out, base_out, lag_out,
    voltage, tissue, fiber, cond, faces_ref, weights_ref, base_ref, lag_ref, field_ref, fib_ref, stack_ref, sems, in_sems,
):
    coming = fetched(((voltage_in, voltage), (tissue_in, tissue), (fiber_in, fiber), (par_in, cond)), in_sems)
    zero = jnp.zeros((NI, NJ, CZ), f32)
    field_ref[...] = zero
    fib_ref[...] = zero
    weights_ref[...] = zero
    own = slice(2, 2 + CY)
    for copy in coming:
        copy.wait()
    for i in range(CX):
        w = tissue[i].astype(f32)
        field_ref[2 + i, own, :] = w * voltage[i]
        weights_ref[2 + i, own, :] = w
        fib_ref[2 + i, own, :] = fiber[i].astype(f32)
    for ref, base, at in ((low, 0, 1), (high, CX + 2, CX + 2)):
        field_ref[at, own, :] = ref[0]
        for m in range(2):
            fib_ref[base + m, own, :] = ref[2 + m]
            weights_ref[base + m, own, :] = ref[4 + m]
    at = 2 * CX + 2
    for ref, outer, cols in ((left, 1, (0, 1)), (right, 2 + CY, (2 + CY, 3 + CY))):
        for i in range(CX + 2):
            field_ref[1 + i, outer : outer + 1, :] = ref[i : i + 1, :]
        for n, j in enumerate(cols):
            for i in range(NI):
                fib_ref[i, j : j + 1, :] = ref[at + n * NI + i : at + n * NI + i + 1, :]
                weights_ref[i, j : j + 1, :] = ref[at + (2 + n) * NI + i : at + (2 + n) * NI + i + 1, :]

    def classes(i, carry):
        for c in range(CHUNKS):
            fib = fib_ref[i, :, chunk(c)]
            w = weights_ref[i, :, chunk(c)]
            found = [jnp.full((NJ, LANES), cond[COND + n * FIB]) for n in range(6)]
            for k in range(1, FIB):
                here = fib == float(k)
                found = [jnp.where(here, cond[COND + n * FIB + k], old) for n, old in enumerate(found)]
            for n in range(6):
                stack_ref[n, i, :, chunk(c)] = 0.5 * (w * found[n])
        return carry

    lax.fori_loop(0, NI, classes, 0)
    lag_ref[0:CY] = low[1]
    lag_ref[CY : 2 * CY] = high[1]
    lag_ref[2 * CY : 2 * CY + CX] = left[CX + 2 : 2 * CX + 2]
    lag_ref[2 * CY + CX : 2 * CY + 2 * CX] = right[CX + 2 : 2 * CX + 2]
    z = lax.broadcasted_iota(jnp.int32, (NJ, CZ), 1)
    copies = fetched(((weights_ref, weights_out), (lag_ref, lag_out)), sems)
    late = 2
    for i in range(NI - 1):
        if i > 1:
            copies.append(pltpu.make_async_copy(faces_ref.at[i - 1], faces_out.at[i - 1], sems.at[late + i - 1]))
            copies[-1].start()
        w = weights_ref[i]
        both = w * weights_ref[i + 1]
        for n, comp in enumerate(COMPONENT[0]):
            faces_ref[i, n] = (stack_ref[comp, i] + stack_ref[comp, i + 1]) * both
        if i == 0:
            faces_ref[0, 3:] = jnp.zeros((6, NJ, CZ), f32)
            continue
        both = w * up_j(w)
        for n, comp in enumerate(COMPONENT[1]):
            here = stack_ref[comp, i]
            faces_ref[i, 3 + n] = (here + up_j(here)) * both
        both = w * jnp.where(z == CZ - 1, 0.0, up_z(w))
        for n, comp in enumerate(COMPONENT[2]):
            here = stack_ref[comp, i]
            faces_ref[i, 6 + n] = (here + up_z(here)) * both
    for i in (0, NI - 2):
        copies.append(pltpu.make_async_copy(faces_ref.at[i], faces_out.at[i], sems.at[late + i]))
        copies[-1].start()
    field = {i: field_ref[i] for i in range(1, NI - 1)}
    spread = spread_of(field, lambda n, i: faces_ref[i, n], 2, CX + 1)
    for i in range(CX):
        base_ref[i] = voltage[i] + tissue[i].astype(f32) * spread[2 + i][2 : 2 + CY]
    copies.append(pltpu.make_async_copy(base_ref, base_out, sems.at[late + NI - 1]))
    copies[-1].start()
    for copy in copies:
        copy.wait()


def react_body(
    worker, voltage_in, base_in, tissue_in, par_in, coming,
    v1_ref, current_ref, states_ref, voltage, base, tissue, par, v_d, base_d, w_d, out_d, cur_d, sems,
):
    for copy in fetched(((voltage_in, voltage), (base_in, base), (tissue_in, tissue), (par_in, par)), sems):
        copy.wait()
    for i in range(CX):
        to_dense(v_d, voltage[i], i)
        to_dense(base_d, base[i], i)
        to_dense(w_d, tissue[i].astype(f32), i)
    low_half = lax.broadcasted_iota(jnp.int32, (8, LANES), 0) < CHUNKS

    def pair(p, carry):
        rows = pl.ds(pl.multiple_of(p * 8, 8), 8)
        owners = [worker[p // (CY // 2), 2 * (p % (CY // 2)) + m] for m in range(2)]
        first, second = [jnp.maximum(k, 0) // CAP for k in owners]
        live = jnp.where(low_half, *[jnp.where(k >= 0, 1.0, 0.0) for k in owners])
        level = v_d[rows, :]
        states = [
            jnp.concatenate([coming[first, pl.ds(g * CHUNKS, CHUNKS), :], coming[second, pl.ds(g * CHUNKS, CHUNKS), :]], axis=0)
            for g in range(GATES)
        ]
        after = base_d[rows, :] - w_d[rows, :] * (STEP_DT * (live * current_from(level, factors(states, par), par)))
        states = [updated(level, s, par, g) for g, s in enumerate(states)]
        for g in range(GATES):
            states_ref[g, rows, :] = states[g]
        out_d[rows, :] = after
        cur_d[rows, :] = live * current_from(after, factors(states, par), par)
        return carry

    lax.fori_loop(0, TILES // 2, pair, 0)
    for i in range(CX):
        for c in range(CHUNKS):
            v1_ref[i, :, chunk(c)] = from_dense(out_d, i, c)
            current_ref[i, :, chunk(c)] = from_dense(cur_d, i, c)


def second_body(par_in, states_in, v1, parts_ref, v_d, parts_d, par, sem):
    fetch = pltpu.make_async_copy(par_in, par, sem)
    fetch.start()
    fetch.wait()
    for i in range(CX):
        to_dense(v_d, v1[i], i)

    def pair(p, carry):
        rows = pl.ds(pl.multiple_of(p * 8, 8), 8)
        level = v_d[rows, :]
        states = [updated(level, states_in[g, rows, :], par, g) for g in range(GATES)]
        for n, part in enumerate(factors(states, par)):
            parts_d[n, rows, :] = part
        return carry

    lax.fori_loop(0, TILES // 2, pair, 0)
    for n in range(4):
        for i in range(CX):
            for c in range(CHUNKS):
                parts_ref[n, i, :, chunk(c)] = from_dense(parts_d.at[n], i, c)


def columns2_body(v1, current, low, high, up_ref, down_ref):
    for ref, pair in ((up_ref, (CY - 2, CY - 1)), (down_ref, (0, 1))):
        outer = CY - 1 if ref is up_ref else 0
        for n, j in enumerate(pair):
            one = slice(j, j + 1)
            for m in range(2):
                ref[n * NI + m : n * NI + m + 1] = low[m, one]
                ref[n * NI + CX + 2 + m : n * NI + CX + 3 + m] = high[m, one]
            for i in range(CX):
                ref[n * NI + 2 + i : n * NI + 3 + i] = v1[i, one]
        one = slice(outer, outer + 1)
        at = 2 * NI
        ref[at : at + 1] = low[2, one]
        ref[at + CX + 1 : at + CX + 2] = high[2, one]
        for i in range(CX):
            ref[at + 1 + i : at + 2 + i] = current[i, one]


def steps_body(
    slots, worker, tile_of_in, par_in, v0, weights, faces, v1, current, low, high, left, right, parts,
    v3_ref, ours_ref, used_ref, tile_of, par, v_ref, cur_ref, next_ref, rows_ref, sems,
):
    fetches = fetched(
        ((par_in, par), (tile_of_in, tile_of)), sems
    )
    v_ref[...] = jnp.zeros((NI, NJ, CZ), f32)
    cur_ref[...] = jnp.zeros((NI, NJ, CZ), f32)
    own = slice(2, 2 + CY)
    for i in range(CX):
        v_ref[2 + i, own, :] = v1[i]
        cur_ref[2 + i, own, :] = current[i]
    for m in range(2):
        v_ref[m, own, :] = low[m]
        v_ref[CX + 2 + m, own, :] = high[m]
    cur_ref[1, own, :] = low[2]
    cur_ref[CX + 2, own, :] = high[2]
    for ref, cols, outer in ((left, (0, 1), 1), (right, (2 + CY, 3 + CY), 2 + CY)):
        for n, j in enumerate(cols):
            for i in range(NI):
                v_ref[i, j : j + 1, :] = ref[n * NI + i : n * NI + i + 1, :]
        for i in range(CX + 2):
            cur_ref[1 + i, outer : outer + 1, :] = ref[2 * NI + i : 2 * NI + i + 1, :]
    face = lambda n, i: faces[i, n]
    for fetch in fetches:
        fetch.wait()
    field = {i: weights[i] * v_ref[i] for i in range(NI)}
    spread = spread_of(field, face, 1, NI - 2)
    for i in range(1, NI - 1):
        next_ref[i] = v_ref[i] + weights[i] * (spread[i] - STEP_DT * cur_ref[i])
    field = {i: weights[i] * next_ref[i] for i in range(1, NI - 1)}
    spread = spread_of(field, face, 2, CX + 1)
    for i in range(CX):
        v2 = next_ref[2 + i, own, :]
        w = weights[2 + i, own, :]
        found = live_plane(worker, i) * current_from(v2, [parts[n, i] for n in range(4)], par)
        v3 = v2 + w * (spread[2 + i][own] - STEP_DT * found)
        v3_ref[i] = v3
        ours_ref[i] = w * (v3 - PHASE_REF)
        for n, v in enumerate((v0[i], v1[i], v2)):
            for c in range(CHUNKS):
                rows_ref[pl.ds(i * CY * 16 + n * CHUNKS + c, CY, stride=16), :] = v[:, c * LANES : (c + 1) * LANES]
        for c in range(CHUNKS):
            rows_ref[pl.ds(i * CY * 16 + 3 * CHUNKS + c, CY, stride=16), :] = jnp.zeros((CY, LANES), f32)
    for d in range(slots):
        used_ref[d] = rows_ref[pl.ds(pl.multiple_of(tile_of[d] * 16, 16), 16), :]


def last_body(slots, arrived, par, returned, gates, out_ref, rows_ref, seen_ref):
    for d in range(slots):
        k = arrived[d]
        row = jnp.where(k >= 0, k, CAP)
        rows_ref[pl.ds(pl.multiple_of(row * 16, 16), 16), :] = returned[d]
    for n in range(STEPS):
        for k in range(0, CAP, 8):
            for c in range(CHUNKS):
                seen_ref[n, k : k + 8, chunk(c)] = rows_ref[pl.ds(k * 16 + n * CHUNKS + c, 8, stride=16), :]

    def one(g, carry):
        for k in range(0, CAP, 8):
            for c in range(CHUNKS):
                state = gates[g, k : k + 8, chunk(c)]
                for n in range(STEPS):
                    state = updated(seen_ref[n, k : k + 8, chunk(c)], state, par, g)
                out_ref[g, k : k + 8, chunk(c)] = state
        return carry

    lax.fori_loop(0, GATES, one, 0)


def arctan_of(cross, den):
    size = jnp.abs(cross)
    big = size > 2.414213562373095 * den
    mid = size > 0.4142135623730950 * den
    num = jnp.where(big, -den, jnp.where(mid, size - den, size))
    x = num / jnp.where(big, size, jnp.where(mid, size + den, den))
    z = x * x
    tail = ((8.05374449538e-2 * z - 1.38776856032e-1) * z + 1.99777106478e-1) * z - 3.33329491539e-1
    found = jnp.where(big, 1.5707963267948966, jnp.where(mid, 0.7853981633974483, 0.0)) + (tail * z * x + x)
    return jnp.where(cross < 0.0, -found, found)


def edge_of(p, q):
    cross = p[0] * q[1] - p[1] * q[0]
    inner = p[0] * q[0] + p[1] * q[1]
    return arctan_of(cross, p[2] * q[2] + inner + PHASE_SOFT)


def charge_body(ours, below, above, left, right, lag, tissue, lag_rim, out_ref):
    row = lax.broadcasted_iota(jnp.int32, (CY, CZ), 0)
    z = lax.broadcasted_iota(jnp.int32, (CY, CZ), 1)

    def point(a, b):
        return (a, b, jnp.sqrt(a * a + b * b))

    a = {-1: below[0], CX: above[0]} | {i: ours[i] for i in range(CX)}
    b = {-1: lag_rim[0:CY], CX: lag_rim[CY : 2 * CY]} | {i: tissue[i].astype(f32) * (lag[i] - PHASE_REF) for i in range(CX)}
    plane = {i: point(a[i], b[i]) for i in range(-1, CX + 1)}
    for i in range(CX):
        at, beyond = 2 * CY + i, 2 * CY + CX + i

        def later(x, edge):
            return jnp.where(row == CY - 1, jnp.broadcast_to(edge, (CY, CZ)), pltpu.roll(x, CY - 1, 0))

        def earlier(x, edge):
            return jnp.where(row == 0, jnp.broadcast_to(edge, (CY, CZ)), pltpu.roll(x, 1, 0))

        y_up = point(later(a[i], right[i]), later(b[i], lag_rim[beyond : beyond + 1]))
        y_down = point(earlier(a[i], left[i]), earlier(b[i], lag_rim[at : at + 1]))
        z_up = tuple(jnp.where(z == CZ - 1, 0.0, up_z(x)) for x in plane[i])
        z_down = tuple(jnp.where(z == 0, 0.0, down_z(x)) for x in plane[i])
        x_up, x_down = plane[i + 1], plane[i - 1]
        for n, ring in enumerate(((x_up, y_up, x_down, y_down), (y_up, z_up, y_down, z_down), (x_up, z_up, x_down, z_down))):
            total = edge_of(ring[0], ring[1]) + edge_of(ring[1], ring[2]) + edge_of(ring[2], ring[3]) + edge_of(ring[3], ring[0])
            out_ref[n, i] = 2.0 * total


def shift_pair(axis, last, first):
    size = lax.axis_size(axis)
    up = [(i, i + 1) for i in range(size - 1)]
    return (lax.ppermute(last, axis, up), lax.ppermute(first, axis, [(b, a) for a, b in up]))


def swap_blocks(x):
    return lax.all_to_all(x, "blk", split_axis=0, concat_axis=0, tiled=True)


def on_device(
    voltage,
    voltage_lag,
    tissue,
    fiber,
    conductivity,
    worker,
    gates,
    gate_half,
    gate_steep,
    gate_tmin,
    gate_tspan,
    channel,
):
    block = voltage.shape
    slots = lax.axis_size("blk")
    par = jnp.concatenate([gate_half, gate_steep, gate_tmin, gate_tspan, channel, *conductivity])
    par = jnp.pad(par, (0, PARAMS - par.shape[0]))
    smem = pltpu.SMEM((PARAMS,), f32)
    dma = lambda n: pltpu.SemaphoreType.DMA((n,))
    whole_i = pltpu.VMEM(block, jnp.int32)

    live = worker >= 0
    holder = jnp.where(live, worker // CAP, -1)
    claimed = holder[None] == jnp.arange(slots, dtype=jnp.int32)[:, None, None]
    tiles = CY * jnp.arange(CX, dtype=jnp.int32)[:, None] + jnp.arange(CY, dtype=jnp.int32)[None, :]
    claims = jnp.sum(jnp.where(claimed, worker % CAP + 1, 0), axis=(1, 2)) - 1
    tile_of = jnp.sum(jnp.where(claimed, tiles[None], 0), axis=(1, 2))
    arrived = swap_blocks(jnp.broadcast_to(claims[:, None, None], (slots, 1, LANES)))[:, 0, 0]
    rim = (6, CY, CZ)
    side = (2 * CX + 2 + 4 * NI, CZ)
    up, down, right, left = kernel_call(
        start_body, [rim, rim, side, side], [HB] * 4, [block, block, whole_i, whole_i, dma(4)]
    )(voltage, voltage_lag, tissue, fiber)
    low, high = shift_pair("slab", up, down)
    (by_row,) = kernel_call(by_row_body, [(CAP * GATES * CHUNKS, LANES)], [VM])(gates)

    run = (slots, GATES * CHUNKS, LANES)
    (leaving,) = kernel_call(functools.partial(pack_body, slots), [run], [SM, VM])(arrived, by_row)
    coming = swap_blocks(leaving)

    up, down = kernel_call(columns_body, [side, side], [VM] * 4)(right, left, low, high)
    left, right = shift_pair("blk", up, down)
    wide = (NI, NJ, CZ)
    sheets = (NI, 9, NJ, CZ)
    lags = (2 * CY + 2 * CX, CZ)
    faces, weights_e, base, lag_rim = kernel_call(
        faces_body,
        [sheets, wide, block, lags],
        [HB] * 4 + [VM] * 4,
        [block, whole_i, whole_i, smem, sheets, wide, block, lags, wide, wide, (6, *wide), dma(NI + 2), dma(4)],
        limit=61,
        specs=[HB] * 4,
    )(voltage, tissue, fiber, par, low, high, left, right)

    dense = (TILES * CHUNKS, LANES)
    v1, current, states = kernel_call(
        react_body,
        [block, block, (GATES, *dense)],
        [SM] + [HB] * 4 + [VM],
        [block, block, whole_i, smem] + [dense] * 5 + [dma(4)],
    )(worker, voltage, base, tissue, par, coming)

    low, high = shift_pair(
        "slab", jnp.concatenate([v1[-2:], current[-1:]]), jnp.concatenate([v1[:2], current[:1]])
    )
    (parts,) = kernel_call(second_body, [(4, *block)], [HB, VM, VM], [dense, (4, *dense), smem, pltpu.SemaphoreType.DMA])(par, states, v1)
    side = (2 * NI + CX + 2, CZ)
    up, down = kernel_call(columns2_body, [side, side], [VM] * 4)(v1, current, low, high)
    left, right = shift_pair("blk", up, down)

    v3, ours, used = kernel_call(
        functools.partial(steps_body, slots),
        [block, block, (slots, 16, LANES)],
        [SM] + [HB] * 2 + [VM] * 10,
        [pltpu.SMEM((LANES,), jnp.int32), smem, wide, wide, wide, (TILES * 16, LANES), dma(2)],
        limit=24,
    )(worker, jnp.pad(tile_of, (0, LANES - slots)), par, voltage, weights_e, faces, v1, current, low, high, left, right, parts)
    returned = swap_blocks(used)

    below, above = shift_pair("slab", ours[-1:], ours[:1])
    left, right = shift_pair("blk", ours[:, -1:], ours[:, :1])

    (charge,) = kernel_call(charge_body, [(3, *block)], [VM] * 8)(
        ours, below, above, left, right, voltage_lag, tissue, lag_rim
    )

    (gates_out,) = kernel_call(
        functools.partial(last_body, slots), [gates.shape], [SM, SM, VM, VM], [((CAP + 1) * 16, LANES), (STEPS, CAP, CZ)]
    )(arrived, par, returned, gates)
    return (v3, gates_out, charge)


def solution(mesh):
    in_specs = (
        P("slab", "blk", None),
        P("slab", "blk", None),
        P("slab", "blk", None),
        P("slab", "blk", None),
        P(),
        P("slab", "blk"),
        P(None, ("slab", "blk"), None),
        P(),
        P(),
        P(),
        P(),
        P(),
    )
    out_specs = (
        P("slab", "blk", None),
        P(None, ("slab", "blk"), None),
        P(None, "slab", "blk", None),
    )
    return jax.shard_map(on_device, mesh=mesh, in_specs=in_specs, out_specs=out_specs, check_vma=False)
```

```python
import functools

import jax
import jax.numpy as jnp
from jax import lax
from jax.experimental import pallas as pl
from jax.experimental.pallas import tpu as pltpu
from jax.sharding import PartitionSpec as P

FIB = 16
STEPS = 3
GATES = 12
CX, CY, CZ = 4, 8, 512
TILES = CX * CY
LANES = 128
CHUNKS = CZ // LANES
CAP = 16
NI, NJ = CX + 4, 16


STEP_DT = 0.1
PHASE_REF = -0.2
PHASE_SOFT = 0.5
COMPONENT = ((0, 3, 4), (3, 1, 5), (4, 5, 2))
HALF, STEEP, TMIN, TSPAN, CHANNEL, COND, PARAMS = 0, 12, 24, 36, 48, 54, 256

f32 = jnp.float32
VM = pl.BlockSpec(memory_space=pltpu.VMEM)
SM = pl.BlockSpec(memory_space=pltpu.SMEM)
HB = pl.BlockSpec(memory_space=pltpu.HBM)


def kernel_call(body, outs, ins, scratch=(), flops=1_000_000, limit=6, specs=None):
    return pl.pallas_call(
        body,
        out_shape=[jax.ShapeDtypeStruct(s, f32) if isinstance(s, tuple) else s for s in outs],
        in_specs=ins,
        out_specs=specs or [VM] * len(outs),
        scratch_shapes=[pltpu.VMEM(s, f32) if isinstance(s, tuple) else s for s in scratch],
        cost_estimate=pl.CostEstimate(flops=flops, bytes_accessed=1_000_000, transcendentals=0),
        compiler_params=pltpu.CompilerParams(vmem_limit_bytes=limit * 1024 * 1024),
    )


def fetched(pairs, sems):
    copies = [pltpu.make_async_copy(a, b, sems.at[n]) for n, (a, b) in enumerate(pairs)]
    for copy in copies:
        copy.start()
    return copies


def live_plane(worker, i):
    row = lax.broadcasted_iota(jnp.int32, (CY, CZ), 0)
    mask = jnp.zeros((CY, CZ), f32)
    for j in range(CY):
        mask = jnp.where(row == j, jnp.where(worker[i, j] >= 0, 1.0, 0.0), mask)
    return mask


def face_at(n, i):
    return 3 * i + n if n < 3 else 3 * (NI - 1) + 6 * (i - 1) + n - 3


def chunk(c):
    return pl.ds(c * LANES, LANES)


def to_dense(dense_ref, plane, i):
    for c in range(CHUNKS):
        dense_ref[pl.ds(i * CY * CHUNKS + c, CY, stride=CHUNKS), :] = plane[:, c * LANES : (c + 1) * LANES]


def from_dense(dense_ref, i, c):
    return dense_ref[pl.ds(i * CY * CHUNKS + c, CY, stride=CHUNKS), :]


def updated(level, state, par_ref, g):
    offset = level - par_ref[HALF + g]
    target = 1.0 / (1.0 + jnp.exp(-par_ref[STEEP + g] * offset))
    bell = 1.0 + 4.0 * (offset * offset)
    decay = jnp.exp((-STEP_DT * bell) / (par_ref[TMIN + g] * bell + par_ref[TSPAN + g]))
    return target + (state - target) * decay


def factors(s, par_ref):
    return (
        par_ref[CHANNEL] * s[0] * s[0] * s[0] * s[1] * s[2],
        par_ref[CHANNEL + 1] * s[3] * s[4] * s[5] * s[6],
        par_ref[CHANNEL + 2] * s[7] * s[8] + par_ref[CHANNEL + 3] * s[9] * s[10],
        par_ref[CHANNEL + 4] * s[11] * s[11],
    )


def current_from(level, parts, par_ref):
    inward = par_ref[CHANNEL + 5] * (level + 0.9) / (1.0 + jnp.exp(4.0 * (level + 0.6)))
    return (
        parts[0] * (level - 1.2)
        + parts[1] * (level - 1.0)
        + parts[2] * (level + 0.9)
        + parts[3] * (level + 0.8)
        + inward
    )


def start_body(voltage_in, lag_in, tissue_in, fiber_in, up_ref, down_ref, right_ref, left_ref, voltage, lag, tissue, fiber, sems):
    for copy in fetched(((voltage_in, voltage), (lag_in, lag), (tissue_in, tissue), (fiber_in, fiber)), sems):
        copy.wait()
    for ref, outer, pair in ((up_ref, CX - 1, (CX - 2, CX - 1)), (down_ref, 0, (0, 1))):
        w = tissue[outer].astype(f32)
        ref[0] = w * voltage[outer]
        ref[1] = w * (lag[outer] - PHASE_REF)
        for n, i in enumerate(pair):
            ref[2 + n] = fiber[i].astype(f32)
            ref[4 + n] = tissue[i].astype(f32)
    for ref, outer, pair in ((right_ref, CY - 1, (CY - 2, CY - 1)), (left_ref, 0, (0, 1))):
        ref[...] = jnp.zeros(ref.shape, f32)
        one = slice(outer, outer + 1)
        for i in range(CX):
            w = tissue[i, one].astype(f32)
            ref[1 + i : 2 + i] = w * voltage[i, one]
            ref[CX + 2 + i : CX + 3 + i] = w * (lag[i, one] - PHASE_REF)
        at = 2 * CX + 2
        for n, j in enumerate(pair):
            one = slice(j, j + 1)
            for i in range(CX):
                ref[at + n * NI + 2 + i : at + n * NI + 3 + i] = fiber[i, one].astype(f32)
                ref[at + (2 + n) * NI + 2 + i : at + (2 + n) * NI + 3 + i] = tissue[i, one].astype(f32)


def columns_body(right_in, left_in, low, high, up_ref, down_ref):
    for ref, own, outer, pair in ((up_ref, right_in, CY - 1, (CY - 2, CY - 1)), (down_ref, left_in, 0, (0, 1))):
        ref[...] = own[...]
        one = slice(outer, outer + 1)
        ref[0:1] = low[0, one]
        ref[CX + 1 : CX + 2] = high[0, one]
        at = 2 * CX + 2
        for n, j in enumerate(pair):
            one = slice(j, j + 1)
            for m in range(2):
                for kind, base in ((2, at + n * NI), (4, at + (2 + n) * NI)):
                    ref[base + m : base + m + 1] = low[kind + m, one]
                    ref[base + CX + 2 + m : base + CX + 3 + m] = high[kind + m, one]


def by_row_body(gates, out_ref):
    for g in range(GATES):
        for c in range(CHUNKS):
            for k in range(0, CAP, 8):
                out_ref[pl.ds(k * GATES * CHUNKS + g * CHUNKS + c, 8, stride=GATES * CHUNKS), :] = gates[g, k : k + 8, chunk(c)]


def pack_body(slots, arrived, by_row, out_ref):
    for d in range(slots):
        k = jnp.maximum(arrived[d], 0)
        out_ref[d] = by_row[pl.ds(pl.multiple_of(k * GATES * CHUNKS, 8), GATES * CHUNKS), :]


def up_j(x):
    return pltpu.roll(x, NJ - 1, 0)


def down_j(x):
    return pltpu.roll(x, 1, 0)


def up_z(x):
    return pltpu.roll(x, CZ - 1, 1)


def down_z(x):
    return pltpu.roll(x, 1, 1)


def spread_of(f, face, first, last):
    z = lax.broadcasted_iota(jnp.int32, (NJ, CZ), 1)
    dy, dz = {}, {}
    for i in range(first - 1, last + 2):
        dy[i] = up_j(f[i]) - down_j(f[i])
        dz[i] = jnp.where(z == CZ - 1, 0.0, up_z(f[i])) - jnp.where(z == 0, 0.0, down_z(f[i]))
    along = {}
    for i in range(first - 1, last + 1):
        along[i] = (
            face(0, i) * (f[i + 1] - f[i])
            + face(1, i) * (0.25 * (dy[i] + dy[i + 1]))
            + face(2, i) * (0.25 * (dz[i] + dz[i + 1]))
        )
    total = {}
    for i in range(first, last + 1):
        dx = f[i + 1] - f[i - 1]
        flux_y = (
            face(4, i) * (up_j(f[i]) - f[i])
            + face(3, i) * (0.25 * (dx + up_j(dx)))
            + face(5, i) * (0.25 * (dz[i] + up_j(dz[i])))
        )
        flux_z = (
            face(8, i) * (up_z(f[i]) - f[i])
            + face(6, i) * (0.25 * (dx + up_z(dx)))
            + face(7, i) * (0.25 * (dy[i] + up_z(dy[i])))
        )
        total[i] = along[i] - along[i - 1] + flux_y - down_j(flux_y) + flux_z - down_z(flux_z)
    return total


def faces_body(
    par, voltage, tissue, fiber, low, high, left, right,
    faces_ref, flags_ref, base_ref, lag_ref, weights_ref, field_ref, fib_ref, stack_ref,
):
    zero = jnp.zeros((NI, NJ, CZ), f32)
    field_ref[...] = zero
    fib_ref[...] = zero
    weights_ref[...] = zero
    own = slice(2, 2 + CY)
    for i in range(CX):
        w = tissue[i].astype(f32)
        field_ref[2 + i, own, :] = w * voltage[i]
        weights_ref[2 + i, own, :] = w
        fib_ref[2 + i, own, :] = fiber[i].astype(f32)
    for ref, base, at in ((low, 0, 1), (high, CX + 2, CX + 2)):
        field_ref[at, own, :] = ref[0]
        for m in range(2):
            fib_ref[base + m, own, :] = ref[2 + m]
            weights_ref[base + m, own, :] = ref[4 + m]
    at = 2 * CX + 2
    for ref, outer, cols in ((left, 1, (0, 1)), (right, 2 + CY, (2 + CY, 3 + CY))):
        for i in range(CX + 2):
            field_ref[1 + i, outer : outer + 1, :] = ref[i : i + 1, :]
        for n, j in enumerate(cols):
            for i in range(NI):
                fib_ref[i, j : j + 1, :] = ref[at + n * NI + i : at + n * NI + i + 1, :]
                weights_ref[i, j : j + 1, :] = ref[at + (2 + n) * NI + i : at + (2 + n) * NI + i + 1, :]

    def classes(i, carry):
        for c in range(CHUNKS):
            fib = fib_ref[i, :, chunk(c)]
            w = weights_ref[i, :, chunk(c)]
            found = [jnp.full((NJ, LANES), par[COND + n * FIB]) for n in range(6)]
            for k in range(1, FIB):
                here = fib == float(k)
                found = [jnp.where(here, par[COND + n * FIB + k], old) for n, old in enumerate(found)]
            for n in range(6):
                stack_ref[n, i, :, chunk(c)] = 0.5 * (w * found[n])
        return carry

    lax.fori_loop(0, NI, classes, 0)
    lag_ref[0:CY] = low[1]
    lag_ref[CY : 2 * CY] = high[1]
    lag_ref[2 * CY : 2 * CY + CX] = left[CX + 2 : 2 * CX + 2]
    lag_ref[2 * CY + CX : 2 * CY + 2 * CX] = right[CX + 2 : 2 * CX + 2]
    z = lax.broadcasted_iota(jnp.int32, (NJ, CZ), 1)
    for i in range(NI - 1):
        w = weights_ref[i]
        both = w * weights_ref[i + 1]
        for n, comp in enumerate(COMPONENT[0]):
            faces_ref[face_at(n, i)] = (stack_ref[comp, i] + stack_ref[comp, i + 1]) * both
        if i == 0:
            continue
        both = w * up_j(w)
        for n, comp in enumerate(COMPONENT[1]):
            here = stack_ref[comp, i]
            faces_ref[face_at(3 + n, i)] = (here + up_j(here)) * both
        both = w * jnp.where(z == CZ - 1, 0.0, up_z(w))
        for n, comp in enumerate(COMPONENT[2]):
            here = stack_ref[comp, i]
            faces_ref[face_at(6 + n, i)] = (here + up_z(here)) * both
    for i in range(NI):
        flags_ref[i] = weights_ref[i].astype(jnp.bfloat16)
    field = {i: field_ref[i] for i in range(1, NI - 1)}
    spread = spread_of(field, lambda n, i: faces_ref[face_at(n, i)], 2, CX + 1)
    for i in range(CX):
        base_ref[i] = voltage[i] + tissue[i].astype(f32) * spread[2 + i][2 : 2 + CY]


def react_body(worker, par, voltage, base, tissue, coming, v1_ref, current_ref, states_ref, v_d, base_d, w_d, out_d, cur_d):
    for i in range(CX):
        to_dense(v_d, voltage[i], i)
        to_dense(base_d, base[i], i)
        to_dense(w_d, tissue[i].astype(f32), i)
    low_half = lax.broadcasted_iota(jnp.int32, (8, LANES), 0) < CHUNKS

    def pair(p, carry):
        rows = pl.ds(pl.multiple_of(p * 8, 8), 8)
        owners = [worker[p // (CY // 2), 2 * (p % (CY // 2)) + m] for m in range(2)]
        first, second = [jnp.maximum(k, 0) // CAP for k in owners]
        live = jnp.where(low_half, *[jnp.where(k >= 0, 1.0, 0.0) for k in owners])
        level = v_d[rows, :]
        states = [
            jnp.concatenate([coming[first, pl.ds(g * CHUNKS, CHUNKS), :], coming[second, pl.ds(g * CHUNKS, CHUNKS), :]], axis=0)
            for g in range(GATES)
        ]
        after = base_d[rows, :] - w_d[rows, :] * (STEP_DT * (live * current_from(level, factors(states, par), par)))
        states = [updated(level, s, par, g) for g, s in enumerate(states)]
        for g in range(GATES):
            states_ref[g, rows, :] = states[g]
        out_d[rows, :] = after
        cur_d[rows, :] = live * current_from(after, factors(states, par), par)
        return carry

    lax.fori_loop(0, TILES // 2, pair, 0)
    for i in range(CX):
        for c in range(CHUNKS):
            v1_ref[i, :, chunk(c)] = from_dense(out_d, i, c)
            current_ref[i, :, chunk(c)] = from_dense(cur_d, i, c)


def second_body(par, states_in, v1, parts_ref, v_d, parts_d):
    for i in range(CX):
        to_dense(v_d, v1[i], i)

    def pair(p, carry):
        rows = pl.ds(pl.multiple_of(p * 8, 8), 8)
        level = v_d[rows, :]
        states = [updated(level, states_in[g, rows, :], par, g) for g in range(GATES)]
        for n, part in enumerate(factors(states, par)):
            parts_d[n, rows, :] = part
        return carry

    lax.fori_loop(0, TILES // 2, pair, 0)
    for n in range(4):
        for i in range(CX):
            for c in range(CHUNKS):
                parts_ref[n, i, :, chunk(c)] = from_dense(parts_d.at[n], i, c)


def columns2_body(v1, current, low, high, up_ref, down_ref):
    for ref, pair in ((up_ref, (CY - 2, CY - 1)), (down_ref, (0, 1))):
        outer = CY - 1 if ref is up_ref else 0
        for n, j in enumerate(pair):
            one = slice(j, j + 1)
            for m in range(2):
                ref[n * NI + m : n * NI + m + 1] = low[m, one]
                ref[n * NI + CX + 2 + m : n * NI + CX + 3 + m] = high[m, one]
            for i in range(CX):
                ref[n * NI + 2 + i : n * NI + 3 + i] = v1[i, one]
        one = slice(outer, outer + 1)
        at = 2 * NI
        ref[at : at + 1] = low[2, one]
        ref[at + CX + 1 : at + CX + 2] = high[2, one]
        for i in range(CX):
            ref[at + 1 + i : at + 2 + i] = current[i, one]


def steps_body(
    slots, worker, tile_of, par, v0, flags, faces, v1, current, low, high, left, right, parts,
    v3_ref, ours_ref, used_ref, v_ref, cur_ref, next_ref, rows_ref,
):
    v_ref[...] = jnp.zeros((NI, NJ, CZ), f32)
    cur_ref[...] = jnp.zeros((NI, NJ, CZ), f32)
    own = slice(2, 2 + CY)
    for i in range(CX):
        v_ref[2 + i, own, :] = v1[i]
        cur_ref[2 + i, own, :] = current[i]
    for m in range(2):
        v_ref[m, own, :] = low[m]
        v_ref[CX + 2 + m, own, :] = high[m]
    cur_ref[1, own, :] = low[2]
    cur_ref[CX + 2, own, :] = high[2]
    for ref, cols, outer in ((left, (0, 1), 1), (right, (2 + CY, 3 + CY), 2 + CY)):
        for n, j in enumerate(cols):
            for i in range(NI):
                v_ref[i, j : j + 1, :] = ref[n * NI + i : n * NI + i + 1, :]
        for i in range(CX + 2):
            cur_ref[1 + i, outer : outer + 1, :] = ref[2 * NI + i : 2 * NI + i + 1, :]
    face = lambda n, i: faces[face_at(n, i)]
    weights = {i: flags[i].astype(f32) for i in range(NI)}
    field = {i: weights[i] * v_ref[i] for i in range(NI)}
    spread = spread_of(field, face, 1, NI - 2)
    for i in range(1, NI - 1):
        next_ref[i] = v_ref[i] + weights[i] * (spread[i] - STEP_DT * cur_ref[i])
    field = {i: weights[i] * next_ref[i] for i in range(1, NI - 1)}
    spread = spread_of(field, face, 2, CX + 1)
    for i in range(CX):
        v2 = next_ref[2 + i, own, :]
        w = weights[2 + i][own]
        found = live_plane(worker, i) * current_from(v2, [parts[n, i] for n in range(4)], par)
        v3 = v2 + w * (spread[2 + i][own] - STEP_DT * found)
        v3_ref[i] = v3
        ours_ref[i] = w * (v3 - PHASE_REF)
        for n, v in enumerate((v0[i], v1[i], v2)):
            for c in range(CHUNKS):
                rows_ref[pl.ds(i * CY * 16 + n * CHUNKS + c, CY, stride=16), :] = v[:, c * LANES : (c + 1) * LANES]
        for c in range(CHUNKS):
            rows_ref[pl.ds(i * CY * 16 + 3 * CHUNKS + c, CY, stride=16), :] = jnp.zeros((CY, LANES), f32)
    for d in range(slots):
        used_ref[d] = rows_ref[pl.ds(pl.multiple_of(tile_of[d] * 16, 16), 16), :]


def last_body(slots, arrived, par, returned, gates, out_ref, rows_ref, seen_ref):
    for d in range(slots):
        k = arrived[d]
        row = jnp.where(k >= 0, k, CAP)
        rows_ref[pl.ds(pl.multiple_of(row * 16, 16), 16), :] = returned[d]
    for n in range(STEPS):
        for k in range(0, CAP, 8):
            for c in range(CHUNKS):
                seen_ref[n, k : k + 8, chunk(c)] = rows_ref[pl.ds(k * 16 + n * CHUNKS + c, 8, stride=16), :]

    def one(g, carry):
        for k in range(0, CAP, 8):
            for c in range(CHUNKS):
                state = gates[g, k : k + 8, chunk(c)]
                for n in range(STEPS):
                    state = updated(seen_ref[n, k : k + 8, chunk(c)], state, par, g)
                out_ref[g, k : k + 8, chunk(c)] = state
        return carry

    lax.fori_loop(0, GATES, one, 0)


def arctan_of(cross, den):
    size = jnp.abs(cross)
    big = size > 2.414213562373095 * den
    mid = size > 0.4142135623730950 * den
    num = jnp.where(big, -den, jnp.where(mid, size - den, size))
    x = num / jnp.where(big, size, jnp.where(mid, size + den, den))
    z = x * x
    tail = ((8.05374449538e-2 * z - 1.38776856032e-1) * z + 1.99777106478e-1) * z - 3.33329491539e-1
    found = jnp.where(big, 1.5707963267948966, jnp.where(mid, 0.7853981633974483, 0.0)) + (tail * z * x + x)
    return jnp.where(cross < 0.0, -found, found)


def edge_of(p, q):
    cross = p[0] * q[1] - p[1] * q[0]
    inner = p[0] * q[0] + p[1] * q[1]
    return arctan_of(cross, p[2] * q[2] + inner + PHASE_SOFT)


def charge_body(ours, below, above, left, right, lag, tissue, lag_rim, out_ref):
    row = lax.broadcasted_iota(jnp.int32, (CY, CZ), 0)
    z = lax.broadcasted_iota(jnp.int32, (CY, CZ), 1)

    def point(a, b):
        return (a, b, jnp.sqrt(a * a + b * b))

    a = {-1: below[0], CX: above[0]} | {i: ours[i] for i in range(CX)}
    b = {-1: lag_rim[0:CY], CX: lag_rim[CY : 2 * CY]} | {i: tissue[i].astype(f32) * (lag[i] - PHASE_REF) for i in range(CX)}
    plane = {i: point(a[i], b[i]) for i in range(-1, CX + 1)}
    for i in range(CX):
        at, beyond = 2 * CY + i, 2 * CY + CX + i

        def later(x, edge):
            return jnp.where(row == CY - 1, jnp.broadcast_to(edge, (CY, CZ)), pltpu.roll(x, CY - 1, 0))

        def earlier(x, edge):
            return jnp.where(row == 0, jnp.broadcast_to(edge, (CY, CZ)), pltpu.roll(x, 1, 0))

        y_up = point(later(a[i], right[i]), later(b[i], lag_rim[beyond : beyond + 1]))
        y_down = point(earlier(a[i], left[i]), earlier(b[i], lag_rim[at : at + 1]))
        z_up = tuple(jnp.where(z == CZ - 1, 0.0, up_z(x)) for x in plane[i])
        z_down = tuple(jnp.where(z == 0, 0.0, down_z(x)) for x in plane[i])
        x_up, x_down = plane[i + 1], plane[i - 1]
        for n, ring in enumerate(((x_up, y_up, x_down, y_down), (y_up, z_up, y_down, z_down), (x_up, z_up, x_down, z_down))):
            total = edge_of(ring[0], ring[1]) + edge_of(ring[1], ring[2]) + edge_of(ring[2], ring[3]) + edge_of(ring[3], ring[0])
            out_ref[n, i] = 2.0 * total


def shift_pair(axis, last, first):
    size = lax.axis_size(axis)
    up = [(i, i + 1) for i in range(size - 1)]
    return (lax.ppermute(last, axis, up), lax.ppermute(first, axis, [(b, a) for a, b in up]))


def swap_blocks(x):
    return lax.all_to_all(x, "blk", split_axis=0, concat_axis=0, tiled=True)


def on_device(
    voltage,
    voltage_lag,
    tissue,
    fiber,
    conductivity,
    worker,
    gates,
    gate_half,
    gate_steep,
    gate_tmin,
    gate_tspan,
    channel,
):
    block = voltage.shape
    slots = lax.axis_size("blk")
    par = jnp.concatenate([gate_half, gate_steep, gate_tmin, gate_tspan, channel, *conductivity])
    par = jnp.pad(par, (0, PARAMS - par.shape[0]))
    dma = lambda n: pltpu.SemaphoreType.DMA((n,))
    whole_i = pltpu.VMEM(block, jnp.int32)

    live = worker >= 0
    holder = jnp.where(live, worker // CAP, -1)
    claimed = holder[None] == jnp.arange(slots, dtype=jnp.int32)[:, None, None]
    tiles = CY * jnp.arange(CX, dtype=jnp.int32)[:, None] + jnp.arange(CY, dtype=jnp.int32)[None, :]
    claims = jnp.sum(jnp.where(claimed, worker % CAP + 1, 0), axis=(1, 2)) - 1
    tile_of = jnp.sum(jnp.where(claimed, tiles[None], 0), axis=(1, 2))
    arrived = swap_blocks(jnp.broadcast_to(claims[:, None, None], (slots, 1, LANES)))[:, 0, 0]
    rim = (6, CY, CZ)
    side = (2 * CX + 2 + 4 * NI, CZ)
    up, down, right, left = kernel_call(
        start_body, [rim, rim, side, side], [HB] * 4, [block, block, whole_i, whole_i, dma(4)]
    )(voltage, voltage_lag, tissue, fiber)
    low, high = shift_pair("slab", up, down)
    (by_row,) = kernel_call(by_row_body, [(CAP * GATES * CHUNKS, LANES)], [VM])(gates)

    run = (slots, GATES * CHUNKS, LANES)
    (leaving,) = kernel_call(functools.partial(pack_body, slots), [run], [SM, VM])(arrived, by_row)
    coming = swap_blocks(leaving)

    up, down = kernel_call(columns_body, [side, side], [VM] * 4)(right, left, low, high)
    left, right = shift_pair("blk", up, down)
    wide = (NI, NJ, CZ)
    sheets = (3 * (NI - 1) + 6 * (NI - 2), NJ, CZ)
    lags = (2 * CY + 2 * CX, CZ)
    faces, flags, base, lag_rim = kernel_call(
        faces_body,
        [sheets, jax.ShapeDtypeStruct(wide, jnp.bfloat16), block, lags],
        [SM] + [VM] * 7,
        [wide, wide, wide, (6, *wide)],
        limit=12,
    )(par, voltage, tissue, fiber, low, high, left, right)

    dense = (TILES * CHUNKS, LANES)
    v1, current, states = kernel_call(
        react_body, [block, block, (GATES, *dense)], [SM, SM] + [VM] * 4, [dense] * 5
    )(worker, par, voltage, base, tissue, coming)

    low, high = shift_pair(
        "slab", jnp.concatenate([v1[-2:], current[-1:]]), jnp.concatenate([v1[:2], current[:1]])
    )
    (parts,) = kernel_call(second_body, [(4, *block)], [SM, VM, VM], [dense, (4, *dense)])(par, states, v1)
    side = (2 * NI + CX + 2, CZ)
    up, down = kernel_call(columns2_body, [side, side], [VM] * 4)(v1, current, low, high)
    left, right = shift_pair("blk", up, down)

    v3, ours, used = kernel_call(
        functools.partial(steps_body, slots),
        [block, block, (slots, 16, LANES)],
        [SM] * 3 + [VM] * 10,
        [wide, wide, wide, (TILES * 16, LANES)],
        limit=12,
    )(worker, tile_of, par, voltage, flags, faces, v1, current, low, high, left, right, parts)
    returned = swap_blocks(used)

    below, above = shift_pair("slab", ours[-1:], ours[:1])
    left, right = shift_pair("blk", ours[:, -1:], ours[:, :1])

    (charge,) = kernel_call(charge_body, [(3, *block)], [VM] * 8)(
        ours, below, above, left, right, voltage_lag, tissue, lag_rim
    )

    (gates_out,) = kernel_call(
        functools.partial(last_body, slots), [gates.shape], [SM, SM, VM, VM], [((CAP + 1) * 16, LANES), (STEPS, CAP, CZ)]
    )(arrived, par, returned, gates)
    return (v3, gates_out, charge)


def solution(mesh):
    in_specs = (
        P("slab", "blk", None),
        P("slab", "blk", None),
        P("slab", "blk", None),
        P("slab", "blk", None),
        P(),
        P("slab", "blk"),
        P(None, ("slab", "blk"), None),
        P(),
        P(),
        P(),
        P(),
        P(),
    )
    out_specs = (
        P("slab", "blk", None),
        P(None, ("slab", "blk"), None),
        P(None, "slab", "blk", None),
    )
    return jax.shard_map(on_device, mesh=mesh, in_specs=in_specs, out_specs=out_specs, check_vma=False)
```

```python
import functools

import jax
import jax.numpy as jnp
from jax import lax
from jax.experimental import pallas as pl
from jax.experimental.pallas import tpu as pltpu
from jax.sharding import PartitionSpec as P

FIB = 16
STEPS = 3
GATES = 12
CX, CY, CZ = 4, 8, 512
TILES = CX * CY
LANES = 128
CHUNKS = CZ // LANES
CAP = 16
NI, NJ = CX + 4, 16


STEP_DT = 0.1
PHASE_REF = -0.2
PHASE_SOFT = 0.5
COMPONENT = ((0, 3, 4), (3, 1, 5), (4, 5, 2))
HALF, STEEP, TMIN, TSPAN, CHANNEL, COND, PARAMS = 0, 12, 24, 36, 48, 54, 256

f32 = jnp.float32
VM = pl.BlockSpec(memory_space=pltpu.VMEM)
SM = pl.BlockSpec(memory_space=pltpu.SMEM)
HB = pl.BlockSpec(memory_space=pltpu.HBM)


def kernel_call(body, outs, ins, scratch=(), flops=1_000_000, limit=6, specs=None):
    return pl.pallas_call(
        body,
        out_shape=[jax.ShapeDtypeStruct(s, f32) if isinstance(s, tuple) else s for s in outs],
        in_specs=ins,
        out_specs=specs or [VM] * len(outs),
        scratch_shapes=[pltpu.VMEM(s, f32) if isinstance(s, tuple) else s for s in scratch],
        cost_estimate=pl.CostEstimate(flops=flops, bytes_accessed=1_000_000, transcendentals=0),
        compiler_params=pltpu.CompilerParams(vmem_limit_bytes=limit * 1024 * 1024),
    )


def fetched(pairs, sems):
    copies = [pltpu.make_async_copy(a, b, sems.at[n]) for n, (a, b) in enumerate(pairs)]
    for copy in copies:
        copy.start()
    return copies


def live_plane(worker, i):
    row = lax.broadcasted_iota(jnp.int32, (CY, CZ), 0)
    mask = jnp.zeros((CY, CZ), f32)
    for j in range(CY):
        mask = jnp.where(row == j, jnp.where(worker[i, j] >= 0, 1.0, 0.0), mask)
    return mask


def face_at(n, i):
    return 3 * i + n if n < 3 else 3 * (NI - 1) + 6 * (i - 1) + n - 3


def chunk(c):
    return pl.ds(c * LANES, LANES)


def to_dense(dense_ref, plane, i):
    for c in range(CHUNKS):
        dense_ref[pl.ds(i * CY * CHUNKS + c, CY, stride=CHUNKS), :] = plane[:, c * LANES : (c + 1) * LANES]


def from_dense(dense_ref, i, c):
    return dense_ref[pl.ds(i * CY * CHUNKS + c, CY, stride=CHUNKS), :]


def updated(level, state, par_ref, g):
    offset = level - par_ref[HALF + g]
    target = 1.0 / (1.0 + jnp.exp(-par_ref[STEEP + g] * offset))
    bell = 1.0 + 4.0 * (offset * offset)
    decay = jnp.exp((-STEP_DT * bell) / (par_ref[TMIN + g] * bell + par_ref[TSPAN + g]))
    return target + (state - target) * decay


def factors(s, par_ref):
    return (
        par_ref[CHANNEL] * s[0] * s[0] * s[0] * s[1] * s[2],
        par_ref[CHANNEL + 1] * s[3] * s[4] * s[5] * s[6],
        par_ref[CHANNEL + 2] * s[7] * s[8] + par_ref[CHANNEL + 3] * s[9] * s[10],
        par_ref[CHANNEL + 4] * s[11] * s[11],
    )


def current_from(level, parts, par_ref):
    inward = par_ref[CHANNEL + 5] * (level + 0.9) / (1.0 + jnp.exp(4.0 * (level + 0.6)))
    return (
        parts[0] * (level - 1.2)
        + parts[1] * (level - 1.0)
        + parts[2] * (level + 0.9)
        + parts[3] * (level + 0.8)
        + inward
    )


def start_body(voltage_in, lag_in, tissue_in, fiber_in, up_ref, down_ref, right_ref, left_ref, voltage, lag, tissue, fiber, sems):
    for copy in fetched(((voltage_in, voltage), (lag_in, lag), (tissue_in, tissue), (fiber_in, fiber)), sems):
        copy.wait()
    for ref, outer, pair in ((up_ref, CX - 1, (CX - 2, CX - 1)), (down_ref, 0, (0, 1))):
        w = tissue[outer].astype(f32)
        ref[0] = w * voltage[outer]
        ref[1] = w * (lag[outer] - PHASE_REF)
        for n, i in enumerate(pair):
            ref[2 + n] = fiber[i].astype(f32)
            ref[4 + n] = tissue[i].astype(f32)
    for ref, outer, pair in ((right_ref, CY - 1, (CY - 2, CY - 1)), (left_ref, 0, (0, 1))):
        ref[...] = jnp.zeros(ref.shape, f32)
        one = slice(outer, outer + 1)
        for i in range(CX):
            w = tissue[i, one].astype(f32)
            ref[1 + i : 2 + i] = w * voltage[i, one]
            ref[CX + 2 + i : CX + 3 + i] = w * (lag[i, one] - PHASE_REF)
        at = 2 * CX + 2
        for n, j in enumerate(pair):
            one = slice(j, j + 1)
            for i in range(CX):
                ref[at + n * NI + 2 + i : at + n * NI + 3 + i] = fiber[i, one].astype(f32)
                ref[at + (2 + n) * NI + 2 + i : at + (2 + n) * NI + 3 + i] = tissue[i, one].astype(f32)


def columns_body(right_in, left_in, low, high, up_ref, down_ref):
    for ref, own, outer, pair in ((up_ref, right_in, CY - 1, (CY - 2, CY - 1)), (down_ref, left_in, 0, (0, 1))):
        ref[...] = own[...]
        one = slice(outer, outer + 1)
        ref[0:1] = low[0, one]
        ref[CX + 1 : CX + 2] = high[0, one]
        at = 2 * CX + 2
        for n, j in enumerate(pair):
            one = slice(j, j + 1)
            for m in range(2):
                for kind, base in ((2, at + n * NI), (4, at + (2 + n) * NI)):
                    ref[base + m : base + m + 1] = low[kind + m, one]
                    ref[base + CX + 2 + m : base + CX + 3 + m] = high[kind + m, one]


def claims_body(slots, worker, claims_ref, held_ref):
    held_ref[...] = jnp.full(held_ref.shape, -1, jnp.int32)
    for t in range(TILES):
        k = worker[t // CY, t % CY]
        at = jnp.where(k >= 0, jnp.maximum(k, 0) // CAP, slots)
        held_ref[at] = jnp.full((1, LANES), jnp.maximum(k, 0) % CAP, jnp.int32)
    claims_ref[...] = held_ref[0:slots]


def by_row_body(gates, out_ref):
    for g in range(GATES):
        for c in range(CHUNKS):
            for k in range(0, CAP, 8):
                out_ref[pl.ds(k * GATES * CHUNKS + g * CHUNKS + c, 8, stride=GATES * CHUNKS), :] = gates[g, k : k + 8, chunk(c)]


def pack_body(slots, arrived, by_row, out_ref):
    for d in range(slots):
        k = jnp.maximum(arrived[d, 0, 0], 0)
        out_ref[d] = by_row[pl.ds(pl.multiple_of(k * GATES * CHUNKS, 8), GATES * CHUNKS), :]


def up_j(x):
    return pltpu.roll(x, NJ - 1, 0)


def down_j(x):
    return pltpu.roll(x, 1, 0)


def up_z(x):
    return pltpu.roll(x, CZ - 1, 1)


def down_z(x):
    return pltpu.roll(x, 1, 1)


def spread_of(f, face, first, last):
    z = lax.broadcasted_iota(jnp.int32, (NJ, CZ), 1)
    dy, dz = {}, {}
    for i in range(first - 1, last + 2):
        dy[i] = up_j(f[i]) - down_j(f[i])
        dz[i] = jnp.where(z == CZ - 1, 0.0, up_z(f[i])) - jnp.where(z == 0, 0.0, down_z(f[i]))
    along = {}
    for i in range(first - 1, last + 1):
        along[i] = (
            face(0, i) * (f[i + 1] - f[i])
            + face(1, i) * (0.25 * (dy[i] + dy[i + 1]))
            + face(2, i) * (0.25 * (dz[i] + dz[i + 1]))
        )
    total = {}
    for i in range(first, last + 1):
        dx = f[i + 1] - f[i - 1]
        flux_y = (
            face(4, i) * (up_j(f[i]) - f[i])
            + face(3, i) * (0.25 * (dx + up_j(dx)))
            + face(5, i) * (0.25 * (dz[i] + up_j(dz[i])))
        )
        flux_z = (
            face(8, i) * (up_z(f[i]) - f[i])
            + face(6, i) * (0.25 * (dx + up_z(dx)))
            + face(7, i) * (0.25 * (dy[i] + up_z(dy[i])))
        )
        total[i] = along[i] - along[i - 1] + flux_y - down_j(flux_y) + flux_z - down_z(flux_z)
    return total


def faces_body(
    par, voltage, tissue, fiber, low, high, left, right,
    faces_ref, flags_ref, base_ref, lag_ref, weights_ref, field_ref, fib_ref, stack_ref,
):
    zero = jnp.zeros((NI, NJ, CZ), f32)
    field_ref[...] = zero
    fib_ref[...] = zero
    weights_ref[...] = zero
    own = slice(2, 2 + CY)
    for i in range(CX):
        w = tissue[i].astype(f32)
        field_ref[2 + i, own, :] = w * voltage[i]
        weights_ref[2 + i, own, :] = w
        fib_ref[2 + i, own, :] = fiber[i].astype(f32)
    for ref, base, at in ((low, 0, 1), (high, CX + 2, CX + 2)):
        field_ref[at, own, :] = ref[0]
        for m in range(2):
            fib_ref[base + m, own, :] = ref[2 + m]
            weights_ref[base + m, own, :] = ref[4 + m]
    at = 2 * CX + 2
    for ref, outer, cols in ((left, 1, (0, 1)), (right, 2 + CY, (2 + CY, 3 + CY))):
        for i in range(CX + 2):
            field_ref[1 + i, outer : outer + 1, :] = ref[i : i + 1, :]
        for n, j in enumerate(cols):
            for i in range(NI):
                fib_ref[i, j : j + 1, :] = ref[at + n * NI + i : at + n * NI + i + 1, :]
                weights_ref[i, j : j + 1, :] = ref[at + (2 + n) * NI + i : at + (2 + n) * NI + i + 1, :]

    def classes(i, carry):
        for c in range(CHUNKS):
            fib = fib_ref[i, :, chunk(c)]
            w = weights_ref[i, :, chunk(c)]
            found = [jnp.full((NJ, LANES), par[COND + n * FIB]) for n in range(6)]
            for k in range(1, FIB):
                here = fib == float(k)
                found = [jnp.where(here, par[COND + n * FIB + k], old) for n, old in enumerate(found)]
            for n in range(6):
                stack_ref[n, i, :, chunk(c)] = 0.5 * (w * found[n])
        return carry

    lax.fori_loop(0, NI, classes, 0)
    lag_ref[0:CY] = low[1]
    lag_ref[CY : 2 * CY] = high[1]
    lag_ref[2 * CY : 2 * CY + CX] = left[CX + 2 : 2 * CX + 2]
    lag_ref[2 * CY + CX : 2 * CY + 2 * CX] = right[CX + 2 : 2 * CX + 2]
    z = lax.broadcasted_iota(jnp.int32, (NJ, CZ), 1)
    for i in range(NI - 1):
        w = weights_ref[i]
        both = w * weights_ref[i + 1]
        for n, comp in enumerate(COMPONENT[0]):
            faces_ref[face_at(n, i)] = (stack_ref[comp, i] + stack_ref[comp, i + 1]) * both
        if i == 0:
            continue
        both = w * up_j(w)
        for n, comp in enumerate(COMPONENT[1]):
            here = stack_ref[comp, i]
            faces_ref[face_at(3 + n, i)] = (here + up_j(here)) * both
        both = w * jnp.where(z == CZ - 1, 0.0, up_z(w))
        for n, comp in enumerate(COMPONENT[2]):
            here = stack_ref[comp, i]
            faces_ref[face_at(6 + n, i)] = (here + up_z(here)) * both
    for i in range(NI):
        flags_ref[i] = weights_ref[i].astype(jnp.bfloat16)
    field = {i: field_ref[i] for i in range(1, NI - 1)}
    spread = spread_of(field, lambda n, i: faces_ref[face_at(n, i)], 2, CX + 1)
    for i in range(CX):
        base_ref[i] = voltage[i] + tissue[i].astype(f32) * spread[2 + i][2 : 2 + CY]


def react_body(worker, par, voltage, base, flags, coming, v1_ref, current_ref, states_ref, v_d, base_d, w_d, out_d, cur_d):
    for i in range(CX):
        to_dense(v_d, voltage[i], i)
        to_dense(base_d, base[i], i)
        to_dense(w_d, flags[2 + i].astype(f32)[2 : 2 + CY], i)
    low_half = lax.broadcasted_iota(jnp.int32, (8, LANES), 0) < CHUNKS

    def pair(p, carry):
        rows = pl.ds(pl.multiple_of(p * 8, 8), 8)
        owners = [worker[p // (CY // 2), 2 * (p % (CY // 2)) + m] for m in range(2)]
        first, second = [jnp.maximum(k, 0) // CAP for k in owners]
        live = jnp.where(low_half, *[jnp.where(k >= 0, 1.0, 0.0) for k in owners])
        level = v_d[rows, :]
        states = [
            jnp.concatenate([coming[first, pl.ds(g * CHUNKS, CHUNKS), :], coming[second, pl.ds(g * CHUNKS, CHUNKS), :]], axis=0)
            for g in range(GATES)
        ]
        after = base_d[rows, :] - w_d[rows, :] * (STEP_DT * (live * current_from(level, factors(states, par), par)))
        states = [updated(level, s, par, g) for g, s in enumerate(states)]
        for g in range(GATES):
            states_ref[g, rows, :] = states[g]
        out_d[rows, :] = after
        cur_d[rows, :] = live * current_from(after, factors(states, par), par)
        return carry

    lax.fori_loop(0, TILES // 2, pair, 0)
    for i in range(CX):
        for c in range(CHUNKS):
            v1_ref[i, :, chunk(c)] = from_dense(out_d, i, c)
            current_ref[i, :, chunk(c)] = from_dense(cur_d, i, c)


def second_body(par, states_in, v1, parts_ref, v_d, parts_d):
    for i in range(CX):
        to_dense(v_d, v1[i], i)

    def pair(p, carry):
        rows = pl.ds(pl.multiple_of(p * 8, 8), 8)
        level = v_d[rows, :]
        states = [updated(level, states_in[g, rows, :], par, g) for g in range(GATES)]
        for n, part in enumerate(factors(states, par)):
            parts_d[n, rows, :] = part
        return carry

    lax.fori_loop(0, TILES // 2, pair, 0)
    for n in range(4):
        for i in range(CX):
            for c in range(CHUNKS):
                parts_ref[n, i, :, chunk(c)] = from_dense(parts_d.at[n], i, c)


def columns2_body(v1, current, low, high, up_ref, down_ref):
    for ref, pair in ((up_ref, (CY - 2, CY - 1)), (down_ref, (0, 1))):
        outer = CY - 1 if ref is up_ref else 0
        for n, j in enumerate(pair):
            one = slice(j, j + 1)
            for m in range(2):
                ref[n * NI + m : n * NI + m + 1] = low[m, one]
                ref[n * NI + CX + 2 + m : n * NI + CX + 3 + m] = high[m, one]
            for i in range(CX):
                ref[n * NI + 2 + i : n * NI + 3 + i] = v1[i, one]
        one = slice(outer, outer + 1)
        at = 2 * NI
        ref[at : at + 1] = low[2, one]
        ref[at + CX + 1 : at + CX + 2] = high[2, one]
        for i in range(CX):
            ref[at + 1 + i : at + 2 + i] = current[i, one]


def steps_body(
    slots, worker, par, v0, flags, faces, v1, current, low, high, left, right, parts,
    v3_ref, ours_ref, used_ref, v_ref, cur_ref, next_ref, rows_ref, tile_of,
):
    v_ref[...] = jnp.zeros((NI, NJ, CZ), f32)
    cur_ref[...] = jnp.zeros((NI, NJ, CZ), f32)
    own = slice(2, 2 + CY)
    for i in range(CX):
        v_ref[2 + i, own, :] = v1[i]
        cur_ref[2 + i, own, :] = current[i]
    for m in range(2):
        v_ref[m, own, :] = low[m]
        v_ref[CX + 2 + m, own, :] = high[m]
    cur_ref[1, own, :] = low[2]
    cur_ref[CX + 2, own, :] = high[2]
    for ref, cols, outer in ((left, (0, 1), 1), (right, (2 + CY, 3 + CY), 2 + CY)):
        for n, j in enumerate(cols):
            for i in range(NI):
                v_ref[i, j : j + 1, :] = ref[n * NI + i : n * NI + i + 1, :]
        for i in range(CX + 2):
            cur_ref[1 + i, outer : outer + 1, :] = ref[2 * NI + i : 2 * NI + i + 1, :]
    for d in range(slots):
        tile_of[d] = 0
    for t in range(TILES):
        k = worker[t // CY, t % CY]
        tile_of[jnp.where(k >= 0, jnp.maximum(k, 0) // CAP, slots)] = t
    face = lambda n, i: faces[face_at(n, i)]
    weights = {i: flags[i].astype(f32) for i in range(NI)}
    field = {i: weights[i] * v_ref[i] for i in range(NI)}
    spread = spread_of(field, face, 1, NI - 2)
    for i in range(1, NI - 1):
        next_ref[i] = v_ref[i] + weights[i] * (spread[i] - STEP_DT * cur_ref[i])
    field = {i: weights[i] * next_ref[i] for i in range(1, NI - 1)}
    spread = spread_of(field, face, 2, CX + 1)
    for i in range(CX):
        v2 = next_ref[2 + i, own, :]
        w = weights[2 + i][own]
        found = live_plane(worker, i) * current_from(v2, [parts[n, i] for n in range(4)], par)
        v3 = v2 + w * (spread[2 + i][own] - STEP_DT * found)
        v3_ref[i] = v3
        ours_ref[i] = w * (v3 - PHASE_REF)
        for n, v in enumerate((v0[i], v1[i], v2)):
            for c in range(CHUNKS):
                rows_ref[pl.ds(i * CY * 16 + n * CHUNKS + c, CY, stride=16), :] = v[:, c * LANES : (c + 1) * LANES]
        for c in range(CHUNKS):
            rows_ref[pl.ds(i * CY * 16 + 3 * CHUNKS + c, CY, stride=16), :] = jnp.zeros((CY, LANES), f32)
    for d in range(slots):
        used_ref[d] = rows_ref[pl.ds(pl.multiple_of(tile_of[d] * 16, 16), 16), :]


def last_body(slots, arrived, par, returned, gates, out_ref, rows_ref, seen_ref):
    for d in range(slots):
        k = arrived[d, 0, 0]
        row = jnp.where(k >= 0, k, CAP)
        rows_ref[pl.ds(pl.multiple_of(row * 16, 16), 16), :] = returned[d]
    for n in range(STEPS):
        for k in range(0, CAP, 8):
            for c in range(CHUNKS):
                seen_ref[n, k : k + 8, chunk(c)] = rows_ref[pl.ds(k * 16 + n * CHUNKS + c, 8, stride=16), :]

    def one(g, carry):
        for k in range(0, CAP, 8):
            for c in range(CHUNKS):
                state = gates[g, k : k + 8, chunk(c)]
                for n in range(STEPS):
                    state = updated(seen_ref[n, k : k + 8, chunk(c)], state, par, g)
                out_ref[g, k : k + 8, chunk(c)] = state
        return carry

    lax.fori_loop(0, GATES, one, 0)


def arctan_of(cross, den):
    size = jnp.abs(cross)
    big = size > 2.414213562373095 * den
    mid = size > 0.4142135623730950 * den
    num = jnp.where(big, -den, jnp.where(mid, size - den, size))
    x = num / jnp.where(big, size, jnp.where(mid, size + den, den))
    z = x * x
    tail = ((8.05374449538e-2 * z - 1.38776856032e-1) * z + 1.99777106478e-1) * z - 3.33329491539e-1
    found = jnp.where(big, 1.5707963267948966, jnp.where(mid, 0.7853981633974483, 0.0)) + (tail * z * x + x)
    return jnp.where(cross < 0.0, -found, found)


def edge_of(p, q):
    cross = p[0] * q[1] - p[1] * q[0]
    inner = p[0] * q[0] + p[1] * q[1]
    return arctan_of(cross, p[2] * q[2] + inner + PHASE_SOFT)


def charge_body(ours, below, above, left, right, lag, tissue, lag_rim, out_ref):
    row = lax.broadcasted_iota(jnp.int32, (CY, CZ), 0)
    z = lax.broadcasted_iota(jnp.int32, (CY, CZ), 1)

    def point(a, b):
        return (a, b, jnp.sqrt(a * a + b * b))

    a = {-1: below[0], CX: above[0]} | {i: ours[i] for i in range(CX)}
    b = {-1: lag_rim[0:CY], CX: lag_rim[CY : 2 * CY]} | {i: tissue[i].astype(f32) * (lag[i] - PHASE_REF) for i in range(CX)}
    plane = {i: point(a[i], b[i]) for i in range(-1, CX + 1)}
    for i in range(CX):
        at, beyond = 2 * CY + i, 2 * CY + CX + i

        def later(x, edge):
            return jnp.where(row == CY - 1, jnp.broadcast_to(edge, (CY, CZ)), pltpu.roll(x, CY - 1, 0))

        def earlier(x, edge):
            return jnp.where(row == 0, jnp.broadcast_to(edge, (CY, CZ)), pltpu.roll(x, 1, 0))

        y_up = point(later(a[i], right[i]), later(b[i], lag_rim[beyond : beyond + 1]))
        y_down = point(earlier(a[i], left[i]), earlier(b[i], lag_rim[at : at + 1]))
        z_up = tuple(jnp.where(z == CZ - 1, 0.0, up_z(x)) for x in plane[i])
        z_down = tuple(jnp.where(z == 0, 0.0, down_z(x)) for x in plane[i])
        x_up, x_down = plane[i + 1], plane[i - 1]
        for n, ring in enumerate(((x_up, y_up, x_down, y_down), (y_up, z_up, y_down, z_down), (x_up, z_up, x_down, z_down))):
            total = edge_of(ring[0], ring[1]) + edge_of(ring[1], ring[2]) + edge_of(ring[2], ring[3]) + edge_of(ring[3], ring[0])
            out_ref[n, i] = 2.0 * total


def shift_pair(axis, last, first):
    size = lax.axis_size(axis)
    up = [(i, i + 1) for i in range(size - 1)]
    return (lax.ppermute(last, axis, up), lax.ppermute(first, axis, [(b, a) for a, b in up]))


def swap_blocks(x):
    return lax.all_to_all(x, "blk", split_axis=0, concat_axis=0, tiled=True)


def on_device(
    voltage,
    voltage_lag,
    tissue,
    fiber,
    conductivity,
    worker,
    gates,
    gate_half,
    gate_steep,
    gate_tmin,
    gate_tspan,
    channel,
):
    block = voltage.shape
    slots = lax.axis_size("blk")
    par = jnp.concatenate([gate_half, gate_steep, gate_tmin, gate_tspan, channel, *conductivity])
    par = jnp.pad(par, (0, PARAMS - par.shape[0]))
    dma = lambda n: pltpu.SemaphoreType.DMA((n,))
    whole_i = pltpu.VMEM(block, jnp.int32)

    slip = (slots, 1, LANES)
    (claims,) = kernel_call(
        functools.partial(claims_body, slots),
        [jax.ShapeDtypeStruct(slip, jnp.int32)],
        [SM],
        [pltpu.VMEM((slots + 1, 1, LANES), jnp.int32)],
    )(worker)
    arrived = swap_blocks(claims)

    rim = (6, CY, CZ)
    side = (2 * CX + 2 + 4 * NI, CZ)
    up, down, right, left = kernel_call(
        start_body, [rim, rim, side, side], [HB] * 4, [block, block, whole_i, whole_i, dma(4)], limit=62
    )(voltage, voltage_lag, tissue, fiber)
    low, high = shift_pair("slab", up, down)
    (by_row,) = kernel_call(by_row_body, [(CAP * GATES * CHUNKS, LANES)], [VM])(gates)

    run = (slots, GATES * CHUNKS, LANES)
    (leaving,) = kernel_call(functools.partial(pack_body, slots), [run], [SM, VM])(arrived, by_row)
    coming = swap_blocks(leaving)

    up, down = kernel_call(columns_body, [side, side], [VM] * 4)(right, left, low, high)
    left, right = shift_pair("blk", up, down)
    wide = (NI, NJ, CZ)
    sheets = (3 * (NI - 1) + 6 * (NI - 2), NJ, CZ)
    lags = (2 * CY + 2 * CX, CZ)
    faces, flags, base, lag_rim = kernel_call(
        faces_body,
        [sheets, jax.ShapeDtypeStruct(wide, jnp.bfloat16), block, lags],
        [SM] + [VM] * 7,
        [wide, wide, wide, (6, *wide)],
        limit=12,
    )(par, voltage, tissue, fiber, low, high, left, right)

    dense = (TILES * CHUNKS, LANES)
    v1, current, states = kernel_call(
        react_body, [block, block, (GATES, *dense)], [SM, SM] + [VM] * 4, [dense] * 5
    )(worker, par, voltage, base, flags, coming)

    low, high = shift_pair(
        "slab", jnp.concatenate([v1[-2:], current[-1:]]), jnp.concatenate([v1[:2], current[:1]])
    )
    (parts,) = kernel_call(second_body, [(4, *block)], [SM, VM, VM], [dense, (4, *dense)])(par, states, v1)
    side = (2 * NI + CX + 2, CZ)
    up, down = kernel_call(columns2_body, [side, side], [VM] * 4)(v1, current, low, high)
    left, right = shift_pair("blk", up, down)

    v3, ours, used = kernel_call(
        functools.partial(steps_body, slots),
        [block, block, (slots, 16, LANES)],
        [SM] * 2 + [VM] * 10,
        [wide, wide, wide, (TILES * 16, LANES), pltpu.SMEM((slots + 1,), jnp.int32)],
        limit=12,
    )(worker, par, voltage, flags, faces, v1, current, low, high, left, right, parts)
    returned = swap_blocks(used)

    below, above = shift_pair("slab", ours[-1:], ours[:1])
    left, right = shift_pair("blk", ours[:, -1:], ours[:, :1])

    (charge,) = kernel_call(charge_body, [(3, *block)], [VM] * 8)(
        ours, below, above, left, right, voltage_lag, tissue, lag_rim
    )

    (gates_out,) = kernel_call(
        functools.partial(last_body, slots), [gates.shape], [SM, SM, VM, VM], [((CAP + 1) * 16, LANES), (STEPS, CAP, CZ)]
    )(arrived, par, returned, gates)
    return (v3, gates_out, charge)


def solution(mesh):
    in_specs = (
        P("slab", "blk", None),
        P("slab", "blk", None),
        P("slab", "blk", None),
        P("slab", "blk", None),
        P(),
        P("slab", "blk"),
        P(None, ("slab", "blk"), None),
        P(),
        P(),
        P(),
        P(),
        P(),
    )
    out_specs = (
        P("slab", "blk", None),
        P(None, ("slab", "blk"), None),
        P(None, "slab", "blk", None),
    )
    return jax.shard_map(on_device, mesh=mesh, in_specs=in_specs, out_specs=out_specs, check_vma=False)
```

```python
import functools

import jax
import jax.numpy as jnp
from jax import lax
from jax.experimental import pallas as pl
from jax.experimental.pallas import tpu as pltpu
from jax.sharding import PartitionSpec as P

FIB = 16
STEPS = 3
GATES = 12
CX, CY, CZ = 4, 8, 512
TILES = CX * CY
LANES = 128
CHUNKS = CZ // LANES
CAP = 16
NI, NJ = CX + 4, 16


STEP_DT = 0.1
PHASE_REF = -0.2
PHASE_SOFT = 0.5
COMPONENT = ((0, 3, 4), (3, 1, 5), (4, 5, 2))
HALF, STEEP, TMIN, TSPAN, CHANNEL, COND, PARAMS = 0, 12, 24, 36, 48, 54, 256

f32 = jnp.float32
VM = pl.BlockSpec(memory_space=pltpu.VMEM)
SM = pl.BlockSpec(memory_space=pltpu.SMEM)
HB = pl.BlockSpec(memory_space=pltpu.HBM)


def kernel_call(body, outs, ins, scratch=(), flops=1_000_000, limit=6, specs=None):
    return pl.pallas_call(
        body,
        out_shape=[jax.ShapeDtypeStruct(s, f32) if isinstance(s, tuple) else s for s in outs],
        in_specs=ins,
        out_specs=specs or [VM] * len(outs),
        scratch_shapes=[pltpu.VMEM(s, f32) if isinstance(s, tuple) else s for s in scratch],
        cost_estimate=pl.CostEstimate(flops=flops, bytes_accessed=1_000_000, transcendentals=0),
        compiler_params=pltpu.CompilerParams(vmem_limit_bytes=limit * 1024 * 1024),
    )


def fetched(pairs, sems):
    copies = [pltpu.make_async_copy(a, b, sems.at[n]) for n, (a, b) in enumerate(pairs)]
    for copy in copies:
        copy.start()
    return copies


def live_plane(worker, i):
    row = lax.broadcasted_iota(jnp.int32, (CY, CZ), 0)
    mask = jnp.zeros((CY, CZ), f32)
    for j in range(CY):
        mask = jnp.where(row == j, jnp.where(worker[i, j] >= 0, 1.0, 0.0), mask)
    return mask


def face_at(n, i):
    return 3 * i + n if n < 3 else 3 * (NI - 1) + 6 * (i - 1) + n - 3


def chunk(c):
    return pl.ds(c * LANES, LANES)


def to_dense(dense_ref, plane, i):
    for c in range(CHUNKS):
        dense_ref[pl.ds(i * CY * CHUNKS + c, CY, stride=CHUNKS), :] = plane[:, c * LANES : (c + 1) * LANES]


def from_dense(dense_ref, i, c):
    return dense_ref[pl.ds(i * CY * CHUNKS + c, CY, stride=CHUNKS), :]


def updated(level, state, par_ref, g):
    offset = level - par_ref[HALF + g]
    target = 1.0 / (1.0 + jnp.exp(-par_ref[STEEP + g] * offset))
    bell = 1.0 + 4.0 * (offset * offset)
    decay = jnp.exp((-STEP_DT * bell) / (par_ref[TMIN + g] * bell + par_ref[TSPAN + g]))
    return target + (state - target) * decay


def factors(s, par_ref):
    return (
        par_ref[CHANNEL] * s[0] * s[0] * s[0] * s[1] * s[2],
        par_ref[CHANNEL + 1] * s[3] * s[4] * s[5] * s[6],
        par_ref[CHANNEL + 2] * s[7] * s[8] + par_ref[CHANNEL + 3] * s[9] * s[10],
        par_ref[CHANNEL + 4] * s[11] * s[11],
    )


def current_from(level, parts, par_ref):
    inward = par_ref[CHANNEL + 5] * (level + 0.9) / (1.0 + jnp.exp(4.0 * (level + 0.6)))
    return (
        parts[0] * (level - 1.2)
        + parts[1] * (level - 1.0)
        + parts[2] * (level + 0.9)
        + parts[3] * (level + 0.8)
        + inward
    )


def start_body(voltage_in, lag_in, tissue_in, fiber_in, up_ref, down_ref, right_ref, left_ref, voltage, lag, tissue, fiber, sems):
    for copy in fetched(((voltage_in, voltage), (lag_in, lag), (tissue_in, tissue), (fiber_in, fiber)), sems):
        copy.wait()
    for ref, outer, pair in ((up_ref, CX - 1, (CX - 2, CX - 1)), (down_ref, 0, (0, 1))):
        w = tissue[outer].astype(f32)
        ref[0] = w * voltage[outer]
        ref[1] = w * (lag[outer] - PHASE_REF)
        for n, i in enumerate(pair):
            ref[2 + n] = fiber[i].astype(f32)
            ref[4 + n] = tissue[i].astype(f32)
    for ref, outer, pair in ((right_ref, CY - 1, (CY - 2, CY - 1)), (left_ref, 0, (0, 1))):
        ref[...] = jnp.zeros(ref.shape, f32)
        one = slice(outer, outer + 1)
        for i in range(CX):
            w = tissue[i, one].astype(f32)
            ref[1 + i : 2 + i] = w * voltage[i, one]
            ref[CX + 2 + i : CX + 3 + i] = w * (lag[i, one] - PHASE_REF)
        at = 2 * CX + 2
        for n, j in enumerate(pair):
            one = slice(j, j + 1)
            for i in range(CX):
                ref[at + n * NI + 2 + i : at + n * NI + 3 + i] = fiber[i, one].astype(f32)
                ref[at + (2 + n) * NI + 2 + i : at + (2 + n) * NI + 3 + i] = tissue[i, one].astype(f32)


def columns_body(right_in, left_in, low, high, up_ref, down_ref):
    for ref, own, outer, pair in ((up_ref, right_in, CY - 1, (CY - 2, CY - 1)), (down_ref, left_in, 0, (0, 1))):
        ref[...] = own[...]
        one = slice(outer, outer + 1)
        ref[0:1] = low[0, one]
        ref[CX + 1 : CX + 2] = high[0, one]
        at = 2 * CX + 2
        for n, j in enumerate(pair):
            one = slice(j, j + 1)
            for m in range(2):
                for kind, base in ((2, at + n * NI), (4, at + (2 + n) * NI)):
                    ref[base + m : base + m + 1] = low[kind + m, one]
                    ref[base + CX + 2 + m : base + CX + 3 + m] = high[kind + m, one]


def claims_body(slots, worker, claims_ref, held_ref):
    held_ref[...] = jnp.full(held_ref.shape, -1, jnp.int32)
    for t in range(TILES):
        k = worker[t // CY, t % CY]
        at = jnp.where(k >= 0, jnp.maximum(k, 0) // CAP, slots)
        held_ref[at] = jnp.full((1, LANES), jnp.maximum(k, 0) % CAP, jnp.int32)
    claims_ref[...] = held_ref[0:slots]


def by_row_body(gates, out_ref):
    for g in range(GATES):
        for c in range(CHUNKS):
            for k in range(0, CAP, 8):
                out_ref[pl.ds(k * GATES * CHUNKS + g * CHUNKS + c, 8, stride=GATES * CHUNKS), :] = gates[g, k : k + 8, chunk(c)]


def pack_body(slots, arrived, by_row, out_ref, sems):
    copies = []
    for d in range(slots):
        k = jnp.maximum(arrived[d, 0, 0], 0)
        rows = pl.ds(pl.multiple_of(k * GATES * CHUNKS, 8), GATES * CHUNKS)
        copies.append(pltpu.make_async_copy(by_row.at[rows, :], out_ref.at[d], sems.at[d]))
        copies[-1].start()
    for copy in copies:
        copy.wait()


def up_j(x):
    return pltpu.roll(x, NJ - 1, 0)


def down_j(x):
    return pltpu.roll(x, 1, 0)


def up_z(x):
    return pltpu.roll(x, CZ - 1, 1)


def down_z(x):
    return pltpu.roll(x, 1, 1)


def spread_of(f, face, first, last):
    z = lax.broadcasted_iota(jnp.int32, (NJ, CZ), 1)
    dy, dz = {}, {}
    for i in range(first - 1, last + 2):
        dy[i] = up_j(f[i]) - down_j(f[i])
        dz[i] = jnp.where(z == CZ - 1, 0.0, up_z(f[i])) - jnp.where(z == 0, 0.0, down_z(f[i]))
    along = {}
    for i in range(first - 1, last + 1):
        along[i] = (
            face(0, i) * (f[i + 1] - f[i])
            + face(1, i) * (0.25 * (dy[i] + dy[i + 1]))
            + face(2, i) * (0.25 * (dz[i] + dz[i + 1]))
        )
    total = {}
    for i in range(first, last + 1):
        dx = f[i + 1] - f[i - 1]
        flux_y = (
            face(4, i) * (up_j(f[i]) - f[i])
            + face(3, i) * (0.25 * (dx + up_j(dx)))
            + face(5, i) * (0.25 * (dz[i] + up_j(dz[i])))
        )
        flux_z = (
            face(8, i) * (up_z(f[i]) - f[i])
            + face(6, i) * (0.25 * (dx + up_z(dx)))
            + face(7, i) * (0.25 * (dy[i] + up_z(dy[i])))
        )
        total[i] = along[i] - along[i - 1] + flux_y - down_j(flux_y) + flux_z - down_z(flux_z)
    return total


def faces_body(
    par, voltage, tissue, fiber, low, high, left, right,
    faces_ref, flags_ref, base_ref, lag_ref, weights_ref, field_ref, fib_ref, stack_ref,
):
    zero = jnp.zeros((NI, NJ, CZ), f32)
    field_ref[...] = zero
    fib_ref[...] = zero
    weights_ref[...] = zero
    own = slice(2, 2 + CY)
    for i in range(CX):
        w = tissue[i].astype(f32)
        field_ref[2 + i, own, :] = w * voltage[i]
        weights_ref[2 + i, own, :] = w
        fib_ref[2 + i, own, :] = fiber[i].astype(f32)
    for ref, base, at in ((low, 0, 1), (high, CX + 2, CX + 2)):
        field_ref[at, own, :] = ref[0]
        for m in range(2):
            fib_ref[base + m, own, :] = ref[2 + m]
            weights_ref[base + m, own, :] = ref[4 + m]
    at = 2 * CX + 2
    for ref, outer, cols in ((left, 1, (0, 1)), (right, 2 + CY, (2 + CY, 3 + CY))):
        for i in range(CX + 2):
            field_ref[1 + i, outer : outer + 1, :] = ref[i : i + 1, :]
        for n, j in enumerate(cols):
            for i in range(NI):
                fib_ref[i, j : j + 1, :] = ref[at + n * NI + i : at + n * NI + i + 1, :]
                weights_ref[i, j : j + 1, :] = ref[at + (2 + n) * NI + i : at + (2 + n) * NI + i + 1, :]

    def classes(i, carry):
        for c in range(CHUNKS):
            fib = fib_ref[i, :, chunk(c)]
            w = weights_ref[i, :, chunk(c)]
            found = [jnp.full((NJ, LANES), par[COND + n * FIB]) for n in range(6)]
            for k in range(1, FIB):
                here = fib == float(k)
                found = [jnp.where(here, par[COND + n * FIB + k], old) for n, old in enumerate(found)]
            for n in range(6):
                stack_ref[n, i, :, chunk(c)] = 0.5 * (w * found[n])
        return carry

    lax.fori_loop(0, NI, classes, 0)
    lag_ref[0:CY] = low[1]
    lag_ref[CY : 2 * CY] = high[1]
    lag_ref[2 * CY : 2 * CY + CX] = left[CX + 2 : 2 * CX + 2]
    lag_ref[2 * CY + CX : 2 * CY + 2 * CX] = right[CX + 2 : 2 * CX + 2]
    z = lax.broadcasted_iota(jnp.int32, (NJ, CZ), 1)
    for i in range(NI - 1):
        w = weights_ref[i]
        both = w * weights_ref[i + 1]
        for n, comp in enumerate(COMPONENT[0]):
            faces_ref[face_at(n, i)] = (stack_ref[comp, i] + stack_ref[comp, i + 1]) * both
        if i == 0:
            continue
        both = w * up_j(w)
        for n, comp in enumerate(COMPONENT[1]):
            here = stack_ref[comp, i]
            faces_ref[face_at(3 + n, i)] = (here + up_j(here)) * both
        both = w * jnp.where(z == CZ - 1, 0.0, up_z(w))
        for n, comp in enumerate(COMPONENT[2]):
            here = stack_ref[comp, i]
            faces_ref[face_at(6 + n, i)] = (here + up_z(here)) * both
    for i in range(NI):
        flags_ref[i] = weights_ref[i].astype(jnp.bfloat16)
    field = {i: field_ref[i] for i in range(1, NI - 1)}
    spread = spread_of(field, lambda n, i: faces_ref[face_at(n, i)], 2, CX + 1)
    for i in range(CX):
        base_ref[i] = voltage[i] + tissue[i].astype(f32) * spread[2 + i][2 : 2 + CY]


def react_body(worker, par, voltage, base, flags, coming, v1_ref, current_ref, states_ref, v_d, base_d, w_d, out_d, cur_d):
    for i in range(CX):
        to_dense(v_d, voltage[i], i)
        to_dense(base_d, base[i], i)
        to_dense(w_d, flags[2 + i].astype(f32)[2 : 2 + CY], i)
    low_half = lax.broadcasted_iota(jnp.int32, (8, LANES), 0) < CHUNKS

    def pair(p, carry):
        rows = pl.ds(pl.multiple_of(p * 8, 8), 8)
        owners = [worker[p // (CY // 2), 2 * (p % (CY // 2)) + m] for m in range(2)]
        first, second = [jnp.maximum(k, 0) // CAP for k in owners]
        live = jnp.where(low_half, *[jnp.where(k >= 0, 1.0, 0.0) for k in owners])
        level = v_d[rows, :]
        states = [
            jnp.concatenate([coming[first, pl.ds(g * CHUNKS, CHUNKS), :], coming[second, pl.ds(g * CHUNKS, CHUNKS), :]], axis=0)
            for g in range(GATES)
        ]
        after = base_d[rows, :] - w_d[rows, :] * (STEP_DT * (live * current_from(level, factors(states, par), par)))
        states = [updated(level, s, par, g) for g, s in enumerate(states)]
        for g in range(GATES):
            states_ref[g, rows, :] = states[g]
        out_d[rows, :] = after
        cur_d[rows, :] = live * current_from(after, factors(states, par), par)
        return carry

    lax.fori_loop(0, TILES // 2, pair, 0)
    for i in range(CX):
        for c in range(CHUNKS):
            v1_ref[i, :, chunk(c)] = from_dense(out_d, i, c)
            current_ref[i, :, chunk(c)] = from_dense(cur_d, i, c)


def second_body(par, states_in, v1, parts_ref, v_d, parts_d):
    for i in range(CX):
        to_dense(v_d, v1[i], i)

    def pair(p, carry):
        rows = pl.ds(pl.multiple_of(p * 8, 8), 8)
        level = v_d[rows, :]
        states = [updated(level, states_in[g, rows, :], par, g) for g in range(GATES)]
        for n, part in enumerate(factors(states, par)):
            parts_d[n, rows, :] = part
        return carry

    lax.fori_loop(0, TILES // 2, pair, 0)
    for n in range(4):
        for i in range(CX):
            for c in range(CHUNKS):
                parts_ref[n, i, :, chunk(c)] = from_dense(parts_d.at[n], i, c)


def columns2_body(v1, current, low, high, up_ref, down_ref):
    for ref, pair in ((up_ref, (CY - 2, CY - 1)), (down_ref, (0, 1))):
        outer = CY - 1 if ref is up_ref else 0
        for n, j in enumerate(pair):
            one = slice(j, j + 1)
            for m in range(2):
                ref[n * NI + m : n * NI + m + 1] = low[m, one]
                ref[n * NI + CX + 2 + m : n * NI + CX + 3 + m] = high[m, one]
            for i in range(CX):
                ref[n * NI + 2 + i : n * NI + 3 + i] = v1[i, one]
        one = slice(outer, outer + 1)
        at = 2 * NI
        ref[at : at + 1] = low[2, one]
        ref[at + CX + 1 : at + CX + 2] = high[2, one]
        for i in range(CX):
            ref[at + 1 + i : at + 2 + i] = current[i, one]


def steps_body(
    slots, worker, par, v0, flags, faces, v1, current, low, high, left, right, parts,
    v3_ref, ours_ref, used_ref, v_ref, cur_ref, next_ref, rows_ref, tile_of,
):
    v_ref[...] = jnp.zeros((NI, NJ, CZ), f32)
    cur_ref[...] = jnp.zeros((NI, NJ, CZ), f32)
    own = slice(2, 2 + CY)
    for i in range(CX):
        v_ref[2 + i, own, :] = v1[i]
        cur_ref[2 + i, own, :] = current[i]
    for m in range(2):
        v_ref[m, own, :] = low[m]
        v_ref[CX + 2 + m, own, :] = high[m]
    cur_ref[1, own, :] = low[2]
    cur_ref[CX + 2, own, :] = high[2]
    for ref, cols, outer in ((left, (0, 1), 1), (right, (2 + CY, 3 + CY), 2 + CY)):
        for n, j in enumerate(cols):
            for i in range(NI):
                v_ref[i, j : j + 1, :] = ref[n * NI + i : n * NI + i + 1, :]
        for i in range(CX + 2):
            cur_ref[1 + i, outer : outer + 1, :] = ref[2 * NI + i : 2 * NI + i + 1, :]
    for d in range(slots):
        tile_of[d] = 0
    for t in range(TILES):
        k = worker[t // CY, t % CY]
        tile_of[jnp.where(k >= 0, jnp.maximum(k, 0) // CAP, slots)] = t
    face = lambda n, i: faces[face_at(n, i)]
    weights = {i: flags[i].astype(f32) for i in range(NI)}
    field = {i: weights[i] * v_ref[i] for i in range(NI)}
    spread = spread_of(field, face, 1, NI - 2)
    for i in range(1, NI - 1):
        next_ref[i] = v_ref[i] + weights[i] * (spread[i] - STEP_DT * cur_ref[i])
    field = {i: weights[i] * next_ref[i] for i in range(1, NI - 1)}
    spread = spread_of(field, face, 2, CX + 1)
    for i in range(CX):
        v2 = next_ref[2 + i, own, :]
        w = weights[2 + i][own]
        found = live_plane(worker, i) * current_from(v2, [parts[n, i] for n in range(4)], par)
        v3 = v2 + w * (spread[2 + i][own] - STEP_DT * found)
        v3_ref[i] = v3
        ours_ref[i] = w * (v3 - PHASE_REF)
        for n, v in enumerate((v0[i], v1[i], v2)):
            for c in range(CHUNKS):
                rows_ref[pl.ds(i * CY * 16 + n * CHUNKS + c, CY, stride=16), :] = v[:, c * LANES : (c + 1) * LANES]
        for c in range(CHUNKS):
            rows_ref[pl.ds(i * CY * 16 + 3 * CHUNKS + c, CY, stride=16), :] = jnp.zeros((CY, LANES), f32)
    for d in range(slots):
        used_ref[d] = rows_ref[pl.ds(pl.multiple_of(tile_of[d] * 16, 16), 16), :]


def last_body(slots, arrived, par, returned, gates, out_ref, rows_ref, seen_ref):
    for d in range(slots):
        k = arrived[d, 0, 0]
        row = jnp.where(k >= 0, k, CAP)
        rows_ref[pl.ds(pl.multiple_of(row * 16, 16), 16), :] = returned[d]
    for n in range(STEPS):
        for k in range(0, CAP, 8):
            for c in range(CHUNKS):
                seen_ref[n, k : k + 8, chunk(c)] = rows_ref[pl.ds(k * 16 + n * CHUNKS + c, 8, stride=16), :]

    def one(g, carry):
        for k in range(0, CAP, 8):
            for c in range(CHUNKS):
                state = gates[g, k : k + 8, chunk(c)]
                for n in range(STEPS):
                    state = updated(seen_ref[n, k : k + 8, chunk(c)], state, par, g)
                out_ref[g, k : k + 8, chunk(c)] = state
        return carry

    lax.fori_loop(0, GATES, one, 0)


def arctan_of(cross, den):
    size = jnp.abs(cross)
    big = size > 2.414213562373095 * den
    mid = size > 0.4142135623730950 * den
    num = jnp.where(big, -den, jnp.where(mid, size - den, size))
    x = num / jnp.where(big, size, jnp.where(mid, size + den, den))
    z = x * x
    tail = ((8.05374449538e-2 * z - 1.38776856032e-1) * z + 1.99777106478e-1) * z - 3.33329491539e-1
    found = jnp.where(big, 1.5707963267948966, jnp.where(mid, 0.7853981633974483, 0.0)) + (tail * z * x + x)
    return jnp.where(cross < 0.0, -found, found)


def edge_of(p, q):
    cross = p[0] * q[1] - p[1] * q[0]
    inner = p[0] * q[0] + p[1] * q[1]
    return arctan_of(cross, p[2] * q[2] + inner + PHASE_SOFT)


def charge_body(ours, below, above, left, right, lag, tissue, lag_rim, out_ref):
    row = lax.broadcasted_iota(jnp.int32, (CY, CZ), 0)
    z = lax.broadcasted_iota(jnp.int32, (CY, CZ), 1)

    def point(a, b):
        return (a, b, jnp.sqrt(a * a + b * b))

    a = {-1: below[0], CX: above[0]} | {i: ours[i] for i in range(CX)}
    b = {-1: lag_rim[0:CY], CX: lag_rim[CY : 2 * CY]} | {i: tissue[i].astype(f32) * (lag[i] - PHASE_REF) for i in range(CX)}
    plane = {i: point(a[i], b[i]) for i in range(-1, CX + 1)}
    for i in range(CX):
        at, beyond = 2 * CY + i, 2 * CY + CX + i

        def later(x, edge):
            return jnp.where(row == CY - 1, jnp.broadcast_to(edge, (CY, CZ)), pltpu.roll(x, CY - 1, 0))

        def earlier(x, edge):
            return jnp.where(row == 0, jnp.broadcast_to(edge, (CY, CZ)), pltpu.roll(x, 1, 0))

        y_up = point(later(a[i], right[i]), later(b[i], lag_rim[beyond : beyond + 1]))
        y_down = point(earlier(a[i], left[i]), earlier(b[i], lag_rim[at : at + 1]))
        z_up = tuple(jnp.where(z == CZ - 1, 0.0, up_z(x)) for x in plane[i])
        z_down = tuple(jnp.where(z == 0, 0.0, down_z(x)) for x in plane[i])
        x_up, x_down = plane[i + 1], plane[i - 1]
        for n, ring in enumerate(((x_up, y_up, x_down, y_down), (y_up, z_up, y_down, z_down), (x_up, z_up, x_down, z_down))):
            total = edge_of(ring[0], ring[1]) + edge_of(ring[1], ring[2]) + edge_of(ring[2], ring[3]) + edge_of(ring[3], ring[0])
            out_ref[n, i] = 2.0 * total


def shift_pair(axis, last, first):
    size = lax.axis_size(axis)
    up = [(i, i + 1) for i in range(size - 1)]
    return (lax.ppermute(last, axis, up), lax.ppermute(first, axis, [(b, a) for a, b in up]))


def swap_blocks(x):
    return lax.all_to_all(x, "blk", split_axis=0, concat_axis=0, tiled=True)


def on_device(
    voltage,
    voltage_lag,
    tissue,
    fiber,
    conductivity,
    worker,
    gates,
    gate_half,
    gate_steep,
    gate_tmin,
    gate_tspan,
    channel,
):
    block = voltage.shape
    slots = lax.axis_size("blk")
    par = jnp.concatenate([gate_half, gate_steep, gate_tmin, gate_tspan, channel, *conductivity])
    par = jnp.pad(par, (0, PARAMS - par.shape[0]))
    dma = lambda n: pltpu.SemaphoreType.DMA((n,))
    whole_i = pltpu.VMEM(block, jnp.int32)

    slip = (slots, 1, LANES)
    (claims,) = kernel_call(
        functools.partial(claims_body, slots),
        [jax.ShapeDtypeStruct(slip, jnp.int32)],
        [SM],
        [pltpu.VMEM((slots + 1, 1, LANES), jnp.int32)],
        limit=62,
    )(worker)
    arrived = swap_blocks(claims)

    rim = (6, CY, CZ)
    side = (2 * CX + 2 + 4 * NI, CZ)
    up, down, right, left = kernel_call(
        start_body, [rim, rim, side, side], [HB] * 4, [block, block, whole_i, whole_i, dma(4)]
    )(voltage, voltage_lag, tissue, fiber)
    low, high = shift_pair("slab", up, down)
    (by_row,) = kernel_call(by_row_body, [(CAP * GATES * CHUNKS, LANES)], [VM])(gates)

    run = (slots, GATES * CHUNKS, LANES)
    (leaving,) = kernel_call(functools.partial(pack_body, slots), [run], [SM, VM], [dma(slots)], specs=[HB])(arrived, by_row)
    coming = swap_blocks(leaving)

    up, down = kernel_call(columns_body, [side, side], [VM] * 4)(right, left, low, high)
    left, right = shift_pair("blk", up, down)
    wide = (NI, NJ, CZ)
    sheets = (3 * (NI - 1) + 6 * (NI - 2), NJ, CZ)
    lags = (2 * CY + 2 * CX, CZ)
    faces, flags, base, lag_rim = kernel_call(
        faces_body,
        [sheets, jax.ShapeDtypeStruct(wide, jnp.bfloat16), block, lags],
        [SM] + [VM] * 7,
        [wide, wide, wide, (6, *wide)],
        limit=12,
    )(par, voltage, tissue, fiber, low, high, left, right)

    dense = (TILES * CHUNKS, LANES)
    v1, current, states = kernel_call(
        react_body, [block, block, (GATES, *dense)], [SM, SM] + [VM] * 4, [dense] * 5
    )(worker, par, voltage, base, flags, coming)

    low, high = shift_pair(
        "slab", jnp.concatenate([v1[-2:], current[-1:]]), jnp.concatenate([v1[:2], current[:1]])
    )
    (parts,) = kernel_call(second_body, [(4, *block)], [SM, VM, VM], [dense, (4, *dense)])(par, states, v1)
    side = (2 * NI + CX + 2, CZ)
    up, down = kernel_call(columns2_body, [side, side], [VM] * 4)(v1, current, low, high)
    left, right = shift_pair("blk", up, down)

    v3, ours, used = kernel_call(
        functools.partial(steps_body, slots),
        [block, block, (slots, 16, LANES)],
        [SM] * 2 + [VM] * 10,
        [wide, wide, wide, (TILES * 16, LANES), pltpu.SMEM((slots + 1,), jnp.int32)],
        limit=12,
    )(worker, par, voltage, flags, faces, v1, current, low, high, left, right, parts)
    returned = swap_blocks(used)

    left, right = shift_pair("blk", ours[:, -1:], ours[:, :1])
    below, above = shift_pair("slab", ours[-1:], ours[:1])

    (charge,) = kernel_call(charge_body, [(3, *block)], [VM] * 8)(
        ours, below, above, left, right, voltage_lag, tissue, lag_rim
    )

    (gates_out,) = kernel_call(
        functools.partial(last_body, slots), [gates.shape], [SM, SM, VM, VM], [((CAP + 1) * 16, LANES), (STEPS, CAP, CZ)]
    )(arrived, par, returned, gates)
    return (v3, gates_out, charge)


def solution(mesh):
    in_specs = (
        P("slab", "blk", None),
        P("slab", "blk", None),
        P("slab", "blk", None),
        P("slab", "blk", None),
        P(),
        P("slab", "blk"),
        P(None, ("slab", "blk"), None),
        P(),
        P(),
        P(),
        P(),
        P(),
    )
    out_specs = (
        P("slab", "blk", None),
        P(None, ("slab", "blk"), None),
        P(None, "slab", "blk", None),
    )
    return jax.shard_map(on_device, mesh=mesh, in_specs=in_specs, out_specs=out_specs, check_vma=False)
```

```python
import functools

import jax
import jax.numpy as jnp
from jax import lax
from jax.experimental import pallas as pl
from jax.experimental.pallas import tpu as pltpu
from jax.sharding import PartitionSpec as P

FIB = 16
STEPS = 3
GATES = 12
CX, CY, CZ = 4, 8, 512
TILES = CX * CY
LANES = 128
CHUNKS = CZ // LANES
CAP = 16
NI, NJ = CX + 4, 16


STEP_DT = 0.1
PHASE_REF = -0.2
PHASE_SOFT = 0.5
COMPONENT = ((0, 3, 4), (3, 1, 5), (4, 5, 2))
HALF, STEEP, TMIN, TSPAN, CHANNEL, COND, PARAMS = 0, 12, 24, 36, 48, 54, 256

f32 = jnp.float32
VM = pl.BlockSpec(memory_space=pltpu.VMEM)
SM = pl.BlockSpec(memory_space=pltpu.SMEM)
HB = pl.BlockSpec(memory_space=pltpu.HBM)


def kernel_call(body, outs, ins, scratch=(), flops=1_000_000, limit=6, specs=None):
    return pl.pallas_call(
        body,
        out_shape=[jax.ShapeDtypeStruct(s, f32) if isinstance(s, tuple) else s for s in outs],
        in_specs=ins,
        out_specs=specs or [VM] * len(outs),
        scratch_shapes=[pltpu.VMEM(s, f32) if isinstance(s, tuple) else s for s in scratch],
        cost_estimate=pl.CostEstimate(flops=flops, bytes_accessed=1_000_000, transcendentals=0),
        compiler_params=pltpu.CompilerParams(vmem_limit_bytes=limit * 1024 * 1024),
    )


def fetched(pairs, sems):
    copies = [pltpu.make_async_copy(a, b, sems.at[n]) for n, (a, b) in enumerate(pairs)]
    for copy in copies:
        copy.start()
    return copies


def live_plane(worker, i):
    row = lax.broadcasted_iota(jnp.int32, (CY, CZ), 0)
    mask = jnp.zeros((CY, CZ), f32)
    for j in range(CY):
        mask = jnp.where(row == j, jnp.where(worker[i, j] >= 0, 1.0, 0.0), mask)
    return mask


def face_at(n, i):
    return 3 * i + n if n < 3 else 3 * (NI - 1) + 6 * (i - 1) + n - 3


def chunk(c):
    return pl.ds(c * LANES, LANES)


def to_dense(dense_ref, plane, i):
    for c in range(CHUNKS):
        dense_ref[pl.ds(i * CY * CHUNKS + c, CY, stride=CHUNKS), :] = plane[:, c * LANES : (c + 1) * LANES]


def from_dense(dense_ref, i, c):
    return dense_ref[pl.ds(i * CY * CHUNKS + c, CY, stride=CHUNKS), :]


def updated(level, state, par_ref, g):
    offset = level - par_ref[HALF + g]
    target = 1.0 / (1.0 + jnp.exp(-par_ref[STEEP + g] * offset))
    bell = 1.0 + 4.0 * (offset * offset)
    decay = jnp.exp((-STEP_DT * bell) / (par_ref[TMIN + g] * bell + par_ref[TSPAN + g]))
    return target + (state - target) * decay


def factors(s, par_ref):
    return (
        par_ref[CHANNEL] * s[0] * s[0] * s[0] * s[1] * s[2],
        par_ref[CHANNEL + 1] * s[3] * s[4] * s[5] * s[6],
        par_ref[CHANNEL + 2] * s[7] * s[8] + par_ref[CHANNEL + 3] * s[9] * s[10],
        par_ref[CHANNEL + 4] * s[11] * s[11],
    )


def current_from(level, parts, par_ref):
    inward = par_ref[CHANNEL + 5] * (level + 0.9) / (1.0 + jnp.exp(4.0 * (level + 0.6)))
    return (
        parts[0] * (level - 1.2)
        + parts[1] * (level - 1.0)
        + parts[2] * (level + 0.9)
        + parts[3] * (level + 0.8)
        + inward
    )


def start_body(voltage_in, lag_in, tissue_in, fiber_in, up_ref, down_ref, right_ref, left_ref, voltage, lag, tissue, fiber, sems):
    for copy in fetched(((voltage_in, voltage), (lag_in, lag), (tissue_in, tissue), (fiber_in, fiber)), sems):
        copy.wait()
    for ref, outer, pair in ((up_ref, CX - 1, (CX - 2, CX - 1)), (down_ref, 0, (0, 1))):
        w = tissue[outer].astype(f32)
        ref[0] = w * voltage[outer]
        ref[1] = w * (lag[outer] - PHASE_REF)
        for n, i in enumerate(pair):
            ref[2 + n] = fiber[i].astype(f32)
            ref[4 + n] = tissue[i].astype(f32)
    for ref, outer, pair in ((right_ref, CY - 1, (CY - 2, CY - 1)), (left_ref, 0, (0, 1))):
        ref[...] = jnp.zeros(ref.shape, f32)
        one = slice(outer, outer + 1)
        for i in range(CX):
            w = tissue[i, one].astype(f32)
            ref[1 + i : 2 + i] = w * voltage[i, one]
            ref[CX + 2 + i : CX + 3 + i] = w * (lag[i, one] - PHASE_REF)
        at = 2 * CX + 2
        for n, j in enumerate(pair):
            one = slice(j, j + 1)
            for i in range(CX):
                ref[at + n * NI + 2 + i : at + n * NI + 3 + i] = fiber[i, one].astype(f32)
                ref[at + (2 + n) * NI + 2 + i : at + (2 + n) * NI + 3 + i] = tissue[i, one].astype(f32)


def columns_body(right_in, left_in, low, high, up_ref, down_ref):
    for ref, own, outer, pair in ((up_ref, right_in, CY - 1, (CY - 2, CY - 1)), (down_ref, left_in, 0, (0, 1))):
        ref[...] = own[...]
        one = slice(outer, outer + 1)
        ref[0:1] = low[0, one]
        ref[CX + 1 : CX + 2] = high[0, one]
        at = 2 * CX + 2
        for n, j in enumerate(pair):
            one = slice(j, j + 1)
            for m in range(2):
                for kind, base in ((2, at + n * NI), (4, at + (2 + n) * NI)):
                    ref[base + m : base + m + 1] = low[kind + m, one]
                    ref[base + CX + 2 + m : base + CX + 3 + m] = high[kind + m, one]


def claims_body(slots, worker, claims_ref, held_ref):
    held_ref[...] = jnp.full(held_ref.shape, -1, jnp.int32)
    for t in range(TILES):
        k = worker[t // CY, t % CY]
        at = jnp.where(k >= 0, jnp.maximum(k, 0) // CAP, slots)
        held_ref[at] = jnp.full((1, LANES), jnp.maximum(k, 0) % CAP, jnp.int32)
    claims_ref[...] = held_ref[0:slots]


def by_row_body(gates, out_ref):
    for g in range(GATES):
        for c in range(CHUNKS):
            for k in range(0, CAP, 8):
                out_ref[pl.ds(k * GATES * CHUNKS + g * CHUNKS + c, 8, stride=GATES * CHUNKS), :] = gates[g, k : k + 8, chunk(c)]


def pack_body(slots, arrived, by_row, out_ref):
    for d in range(slots):
        k = jnp.maximum(arrived[d, 0, 0], 0)
        out_ref[d] = by_row[pl.ds(pl.multiple_of(k * GATES * CHUNKS, 8), GATES * CHUNKS), :]


def up_j(x):
    return pltpu.roll(x, NJ - 1, 0)


def down_j(x):
    return pltpu.roll(x, 1, 0)


def up_z(x):
    return pltpu.roll(x, CZ - 1, 1)


def down_z(x):
    return pltpu.roll(x, 1, 1)


def spread_of(f, face, first, last):
    z = lax.broadcasted_iota(jnp.int32, (NJ, CZ), 1)
    dy, dz = {}, {}
    for i in range(first - 1, last + 2):
        dy[i] = up_j(f[i]) - down_j(f[i])
        dz[i] = jnp.where(z == CZ - 1, 0.0, up_z(f[i])) - jnp.where(z == 0, 0.0, down_z(f[i]))
    along = {}
    for i in range(first - 1, last + 1):
        along[i] = (
            face(0, i) * (f[i + 1] - f[i])
            + face(1, i) * (0.25 * (dy[i] + dy[i + 1]))
            + face(2, i) * (0.25 * (dz[i] + dz[i + 1]))
        )
    total = {}
    for i in range(first, last + 1):
        dx = f[i + 1] - f[i - 1]
        flux_y = (
            face(4, i) * (up_j(f[i]) - f[i])
            + face(3, i) * (0.25 * (dx + up_j(dx)))
            + face(5, i) * (0.25 * (dz[i] + up_j(dz[i])))
        )
        flux_z = (
            face(8, i) * (up_z(f[i]) - f[i])
            + face(6, i) * (0.25 * (dx + up_z(dx)))
            + face(7, i) * (0.25 * (dy[i] + up_z(dy[i])))
        )
        total[i] = along[i] - along[i - 1] + flux_y - down_j(flux_y) + flux_z - down_z(flux_z)
    return total


def faces_body(
    par, voltage, tissue, fiber, low, high, left, right,
    faces_ref, flags_ref, base_ref, lag_ref, weights_ref, field_ref, fib_ref, stack_ref,
):
    zero = jnp.zeros((NI, NJ, CZ), f32)
    field_ref[...] = zero
    fib_ref[...] = zero
    weights_ref[...] = zero
    own = slice(2, 2 + CY)
    for i in range(CX):
        w = tissue[i].astype(f32)
        field_ref[2 + i, own, :] = w * voltage[i]
        weights_ref[2 + i, own, :] = w
        fib_ref[2 + i, own, :] = fiber[i].astype(f32)
    for ref, base, at in ((low, 0, 1), (high, CX + 2, CX + 2)):
        field_ref[at, own, :] = ref[0]
        for m in range(2):
            fib_ref[base + m, own, :] = ref[2 + m]
            weights_ref[base + m, own, :] = ref[4 + m]
    at = 2 * CX + 2
    for ref, outer, cols in ((left, 1, (0, 1)), (right, 2 + CY, (2 + CY, 3 + CY))):
        for i in range(CX + 2):
            field_ref[1 + i, outer : outer + 1, :] = ref[i : i + 1, :]
        for n, j in enumerate(cols):
            for i in range(NI):
                fib_ref[i, j : j + 1, :] = ref[at + n * NI + i : at + n * NI + i + 1, :]
                weights_ref[i, j : j + 1, :] = ref[at + (2 + n) * NI + i : at + (2 + n) * NI + i + 1, :]

    def classes(i, carry):
        for c in range(CHUNKS):
            fib = fib_ref[i, :, chunk(c)]
            w = weights_ref[i, :, chunk(c)]
            found = [jnp.full((NJ, LANES), par[COND + n * FIB]) for n in range(6)]
            for k in range(1, FIB):
                here = fib == float(k)
                found = [jnp.where(here, par[COND + n * FIB + k], old) for n, old in enumerate(found)]
            for n in range(6):
                stack_ref[n, i, :, chunk(c)] = 0.5 * (w * found[n])
        return carry

    lax.fori_loop(0, NI, classes, 0)
    lag_ref[0:CY] = low[1]
    lag_ref[CY : 2 * CY] = high[1]
    lag_ref[2 * CY : 2 * CY + CX] = left[CX + 2 : 2 * CX + 2]
    lag_ref[2 * CY + CX : 2 * CY + 2 * CX] = right[CX + 2 : 2 * CX + 2]
    z = lax.broadcasted_iota(jnp.int32, (NJ, CZ), 1)
    for i in range(NI - 1):
        w = weights_ref[i]
        both = w * weights_ref[i + 1]
        for n, comp in enumerate(COMPONENT[0]):
            faces_ref[face_at(n, i)] = (stack_ref[comp, i] + stack_ref[comp, i + 1]) * both
        if i == 0:
            continue
        both = w * up_j(w)
        for n, comp in enumerate(COMPONENT[1]):
            here = stack_ref[comp, i]
            faces_ref[face_at(3 + n, i)] = (here + up_j(here)) * both
        both = w * jnp.where(z == CZ - 1, 0.0, up_z(w))
        for n, comp in enumerate(COMPONENT[2]):
            here = stack_ref[comp, i]
            faces_ref[face_at(6 + n, i)] = (here + up_z(here)) * both
    for i in range(NI):
        flags_ref[i] = weights_ref[i].astype(jnp.bfloat16)
    field = {i: field_ref[i] for i in range(1, NI - 1)}
    spread = spread_of(field, lambda n, i: faces_ref[face_at(n, i)], 2, CX + 1)
    for i in range(CX):
        base_ref[i] = voltage[i] + tissue[i].astype(f32) * spread[2 + i][2 : 2 + CY]


def react_body(worker, par, voltage, base, flags, coming, v1_ref, current_ref, states_ref, v_d, base_d, w_d, out_d, cur_d):
    for i in range(CX):
        to_dense(v_d, voltage[i], i)
        to_dense(base_d, base[i], i)
        to_dense(w_d, flags[2 + i].astype(f32)[2 : 2 + CY], i)
    low_half = lax.broadcasted_iota(jnp.int32, (8, LANES), 0) < CHUNKS

    def pair(p, carry):
        rows = pl.ds(pl.multiple_of(p * 8, 8), 8)
        owners = [worker[p // (CY // 2), 2 * (p % (CY // 2)) + m] for m in range(2)]
        first, second = [jnp.maximum(k, 0) // CAP for k in owners]
        live = jnp.where(low_half, *[jnp.where(k >= 0, 1.0, 0.0) for k in owners])
        level = v_d[rows, :]
        states = [
            jnp.concatenate([coming[first, pl.ds(g * CHUNKS, CHUNKS), :], coming[second, pl.ds(g * CHUNKS, CHUNKS), :]], axis=0)
            for g in range(GATES)
        ]
        after = base_d[rows, :] - w_d[rows, :] * (STEP_DT * (live * current_from(level, factors(states, par), par)))
        states = [updated(level, s, par, g) for g, s in enumerate(states)]
        for g in range(GATES):
            states_ref[g, rows, :] = states[g]
        out_d[rows, :] = after
        cur_d[rows, :] = live * current_from(after, factors(states, par), par)
        return carry

    lax.fori_loop(0, TILES // 2, pair, 0)
    for i in range(CX):
        for c in range(CHUNKS):
            v1_ref[i, :, chunk(c)] = from_dense(out_d, i, c)
            current_ref[i, :, chunk(c)] = from_dense(cur_d, i, c)


def second_body(par, states_in, v1, parts_ref, v_d, parts_d):
    for i in range(CX):
        to_dense(v_d, v1[i], i)

    def pair(p, carry):
        rows = pl.ds(pl.multiple_of(p * 8, 8), 8)
        level = v_d[rows, :]
        states = [updated(level, states_in[g, rows, :], par, g) for g in range(GATES)]
        for n, part in enumerate(factors(states, par)):
            parts_d[n, rows, :] = part
        return carry

    lax.fori_loop(0, TILES // 2, pair, 0)
    for n in range(4):
        for i in range(CX):
            for c in range(CHUNKS):
                parts_ref[n, i, :, chunk(c)] = from_dense(parts_d.at[n], i, c)


def columns2_body(v1, current, low, high, up_ref, down_ref):
    for ref, pair in ((up_ref, (CY - 2, CY - 1)), (down_ref, (0, 1))):
        outer = CY - 1 if ref is up_ref else 0
        for n, j in enumerate(pair):
            one = slice(j, j + 1)
            for m in range(2):
                ref[n * NI + m : n * NI + m + 1] = low[m, one]
                ref[n * NI + CX + 2 + m : n * NI + CX + 3 + m] = high[m, one]
            for i in range(CX):
                ref[n * NI + 2 + i : n * NI + 3 + i] = v1[i, one]
        one = slice(outer, outer + 1)
        at = 2 * NI
        ref[at : at + 1] = low[2, one]
        ref[at + CX + 1 : at + CX + 2] = high[2, one]
        for i in range(CX):
            ref[at + 1 + i : at + 2 + i] = current[i, one]


def steps_body(
    slots, worker, par, v0, flags, faces, v1, current, low, high, left, right, parts,
    v3_ref, ours_ref, used_ref, v_ref, cur_ref, next_ref, rows_ref, tile_of,
):
    v_ref[...] = jnp.zeros((NI, NJ, CZ), f32)
    cur_ref[...] = jnp.zeros((NI, NJ, CZ), f32)
    own = slice(2, 2 + CY)
    for i in range(CX):
        v_ref[2 + i, own, :] = v1[i]
        cur_ref[2 + i, own, :] = current[i]
    for m in range(2):
        v_ref[m, own, :] = low[m]
        v_ref[CX + 2 + m, own, :] = high[m]
    cur_ref[1, own, :] = low[2]
    cur_ref[CX + 2, own, :] = high[2]
    for ref, cols, outer in ((left, (0, 1), 1), (right, (2 + CY, 3 + CY), 2 + CY)):
        for n, j in enumerate(cols):
            for i in range(NI):
                v_ref[i, j : j + 1, :] = ref[n * NI + i : n * NI + i + 1, :]
        for i in range(CX + 2):
            cur_ref[1 + i, outer : outer + 1, :] = ref[2 * NI + i : 2 * NI + i + 1, :]
    for d in range(slots):
        tile_of[d] = 0
    for t in range(TILES):
        k = worker[t // CY, t % CY]
        tile_of[jnp.where(k >= 0, jnp.maximum(k, 0) // CAP, slots)] = t
    face = lambda n, i: faces[face_at(n, i)]
    weights = {i: flags[i].astype(f32) for i in range(NI)}
    field = {i: weights[i] * v_ref[i] for i in range(NI)}
    spread = spread_of(field, face, 1, NI - 2)
    for i in range(1, NI - 1):
        next_ref[i] = v_ref[i] + weights[i] * (spread[i] - STEP_DT * cur_ref[i])
    field = {i: weights[i] * next_ref[i] for i in range(1, NI - 1)}
    spread = spread_of(field, face, 2, CX + 1)
    for i in range(CX):
        v2 = next_ref[2 + i, own, :]
        w = weights[2 + i][own]
        found = live_plane(worker, i) * current_from(v2, [parts[n, i] for n in range(4)], par)
        v3 = v2 + w * (spread[2 + i][own] - STEP_DT * found)
        v3_ref[i] = v3
        ours_ref[i] = w * (v3 - PHASE_REF)
        for n, v in enumerate((v0[i], v1[i], v2)):
            for c in range(CHUNKS):
                rows_ref[pl.ds(i * CY * 16 + n * CHUNKS + c, CY, stride=16), :] = v[:, c * LANES : (c + 1) * LANES]
        for c in range(CHUNKS):
            rows_ref[pl.ds(i * CY * 16 + 3 * CHUNKS + c, CY, stride=16), :] = jnp.zeros((CY, LANES), f32)
    for d in range(slots):
        used_ref[d] = rows_ref[pl.ds(pl.multiple_of(tile_of[d] * 16, 16), 16), :]


def last_body(slots, arrived, par, returned, gates, gates_out, rows_ref, seen_ref, out_ref, sems):
    for d in range(slots):
        k = arrived[d, 0, 0]
        row = jnp.where(k >= 0, k, CAP)
        rows_ref[pl.ds(pl.multiple_of(row * 16, 16), 16), :] = returned[d]
    for n in range(STEPS):
        for k in range(0, CAP, 8):
            for c in range(CHUNKS):
                seen_ref[n, k : k + 8, chunk(c)] = rows_ref[pl.ds(k * 16 + n * CHUNKS + c, 8, stride=16), :]

    def one(g, carry):
        for k in range(0, CAP, 8):
            for c in range(CHUNKS):
                state = gates[g, k : k + 8, chunk(c)]
                for n in range(STEPS):
                    state = updated(seen_ref[n, k : k + 8, chunk(c)], state, par, g)
                out_ref[g, k : k + 8, chunk(c)] = state
        pltpu.make_async_copy(out_ref.at[g], gates_out.at[g], sems.at[g]).start()
        return carry

    lax.fori_loop(0, GATES, one, 0)
    for g in range(GATES):
        pltpu.make_async_copy(out_ref.at[g], gates_out.at[g], sems.at[g]).wait()


def arctan_of(cross, den):
    size = jnp.abs(cross)
    big = size > 2.414213562373095 * den
    mid = size > 0.4142135623730950 * den
    num = jnp.where(big, -den, jnp.where(mid, size - den, size))
    x = num / jnp.where(big, size, jnp.where(mid, size + den, den))
    z = x * x
    tail = ((8.05374449538e-2 * z - 1.38776856032e-1) * z + 1.99777106478e-1) * z - 3.33329491539e-1
    found = jnp.where(big, 1.5707963267948966, jnp.where(mid, 0.7853981633974483, 0.0)) + (tail * z * x + x)
    return jnp.where(cross < 0.0, -found, found)


def edge_of(p, q):
    cross = p[0] * q[1] - p[1] * q[0]
    inner = p[0] * q[0] + p[1] * q[1]
    return arctan_of(cross, p[2] * q[2] + inner + PHASE_SOFT)


def charge_body(ours, below, above, left, right, lag, tissue, lag_rim, out_ref):
    row = lax.broadcasted_iota(jnp.int32, (CY, CZ), 0)
    z = lax.broadcasted_iota(jnp.int32, (CY, CZ), 1)

    def point(a, b):
        return (a, b, jnp.sqrt(a * a + b * b))

    a = {-1: below[0], CX: above[0]} | {i: ours[i] for i in range(CX)}
    b = {-1: lag_rim[0:CY], CX: lag_rim[CY : 2 * CY]} | {i: tissue[i].astype(f32) * (lag[i] - PHASE_REF) for i in range(CX)}
    plane = {i: point(a[i], b[i]) for i in range(-1, CX + 1)}
    for i in range(CX):
        at, beyond = 2 * CY + i, 2 * CY + CX + i

        def later(x, edge):
            return jnp.where(row == CY - 1, jnp.broadcast_to(edge, (CY, CZ)), pltpu.roll(x, CY - 1, 0))

        def earlier(x, edge):
            return jnp.where(row == 0, jnp.broadcast_to(edge, (CY, CZ)), pltpu.roll(x, 1, 0))

        y_up = point(later(a[i], right[i]), later(b[i], lag_rim[beyond : beyond + 1]))
        y_down = point(earlier(a[i], left[i]), earlier(b[i], lag_rim[at : at + 1]))
        z_up = tuple(jnp.where(z == CZ - 1, 0.0, up_z(x)) for x in plane[i])
        z_down = tuple(jnp.where(z == 0, 0.0, down_z(x)) for x in plane[i])
        x_up, x_down = plane[i + 1], plane[i - 1]
        for n, ring in enumerate(((x_up, y_up, x_down, y_down), (y_up, z_up, y_down, z_down), (x_up, z_up, x_down, z_down))):
            total = edge_of(ring[0], ring[1]) + edge_of(ring[1], ring[2]) + edge_of(ring[2], ring[3]) + edge_of(ring[3], ring[0])
            out_ref[n, i] = 2.0 * total


def shift_pair(axis, last, first):
    size = lax.axis_size(axis)
    up = [(i, i + 1) for i in range(size - 1)]
    return (lax.ppermute(last, axis, up), lax.ppermute(first, axis, [(b, a) for a, b in up]))


def swap_blocks(x):
    return lax.all_to_all(x, "blk", split_axis=0, concat_axis=0, tiled=True)


def on_device(
    voltage,
    voltage_lag,
    tissue,
    fiber,
    conductivity,
    worker,
    gates,
    gate_half,
    gate_steep,
    gate_tmin,
    gate_tspan,
    channel,
):
    block = voltage.shape
    slots = lax.axis_size("blk")
    par = jnp.concatenate([gate_half, gate_steep, gate_tmin, gate_tspan, channel, *conductivity])
    par = jnp.pad(par, (0, PARAMS - par.shape[0]))
    dma = lambda n: pltpu.SemaphoreType.DMA((n,))
    whole_i = pltpu.VMEM(block, jnp.int32)

    slip = (slots, 1, LANES)
    (claims,) = kernel_call(
        functools.partial(claims_body, slots),
        [jax.ShapeDtypeStruct(slip, jnp.int32)],
        [SM],
        [pltpu.VMEM((slots + 1, 1, LANES), jnp.int32)],
        limit=62,
    )(worker)
    arrived = swap_blocks(claims)

    rim = (6, CY, CZ)
    side = (2 * CX + 2 + 4 * NI, CZ)
    up, down, right, left = kernel_call(
        start_body, [rim, rim, side, side], [HB] * 4, [block, block, whole_i, whole_i, dma(4)]
    )(voltage, voltage_lag, tissue, fiber)
    low, high = shift_pair("slab", up, down)
    (by_row,) = kernel_call(by_row_body, [(CAP * GATES * CHUNKS, LANES)], [VM])(gates)

    run = (slots, GATES * CHUNKS, LANES)
    (leaving,) = kernel_call(functools.partial(pack_body, slots), [run], [SM, VM])(arrived, by_row)
    coming = swap_blocks(leaving)

    up, down = kernel_call(columns_body, [side, side], [VM] * 4)(right, left, low, high)
    left, right = shift_pair("blk", up, down)
    wide = (NI, NJ, CZ)
    sheets = (3 * (NI - 1) + 6 * (NI - 2), NJ, CZ)
    lags = (2 * CY + 2 * CX, CZ)
    faces, flags, base, lag_rim = kernel_call(
        faces_body,
        [sheets, jax.ShapeDtypeStruct(wide, jnp.bfloat16), block, lags],
        [SM] + [VM] * 7,
        [wide, wide, wide, (6, *wide)],
        limit=12,
    )(par, voltage, tissue, fiber, low, high, left, right)

    dense = (TILES * CHUNKS, LANES)
    v1, current, states = kernel_call(
        react_body, [block, block, (GATES, *dense)], [SM, SM] + [VM] * 4, [dense] * 5
    )(worker, par, voltage, base, flags, coming)

    low, high = shift_pair(
        "slab", jnp.concatenate([v1[-2:], current[-1:]]), jnp.concatenate([v1[:2], current[:1]])
    )
    (parts,) = kernel_call(second_body, [(4, *block)], [SM, VM, VM], [dense, (4, *dense)])(par, states, v1)
    side = (2 * NI + CX + 2, CZ)
    up, down = kernel_call(columns2_body, [side, side], [VM] * 4)(v1, current, low, high)
    left, right = shift_pair("blk", up, down)

    v3, ours, used = kernel_call(
        functools.partial(steps_body, slots),
        [block, block, (slots, 16, LANES)],
        [SM] * 2 + [VM] * 10,
        [wide, wide, wide, (TILES * 16, LANES), pltpu.SMEM((slots + 1,), jnp.int32)],
        limit=12,
    )(worker, par, voltage, flags, faces, v1, current, low, high, left, right, parts)
    returned = swap_blocks(used)

    left, right = shift_pair("blk", ours[:, -1:], ours[:, :1])
    below, above = shift_pair("slab", ours[-1:], ours[:1])

    (charge,) = kernel_call(charge_body, [(3, *block)], [VM] * 8)(
        ours, below, above, left, right, voltage_lag, tissue, lag_rim
    )

    (gates_out,) = kernel_call(
        functools.partial(last_body, slots), [gates.shape], [SM, SM, VM, VM], [((CAP + 1) * 16, LANES), (STEPS, CAP, CZ), gates.shape, dma(GATES)], specs=[HB]
    )(arrived, par, returned, gates)
    return (v3, gates_out, charge)


def solution(mesh):
    in_specs = (
        P("slab", "blk", None),
        P("slab", "blk", None),
        P("slab", "blk", None),
        P("slab", "blk", None),
        P(),
        P("slab", "blk"),
        P(None, ("slab", "blk"), None),
        P(),
        P(),
        P(),
        P(),
        P(),
    )
    out_specs = (
        P("slab", "blk", None),
        P(None, ("slab", "blk"), None),
        P(None, "slab", "blk", None),
    )
    return jax.shard_map(on_device, mesh=mesh, in_specs=in_specs, out_specs=out_specs, check_vma=False)
```
